32 devices in a mesh: gx: 8 (over z, y), gy: 2 (over core), gz: 2 (over x).
Axes of the slice: x: 2, y: 2, z: 4, core: 2. Of those that a mesh axis runs over, the one named last changes fastest.
Arguments:
- adjoint_in: float32 [19, 64, 16, 256], P(None, 'gx', 'gy', 'gz'), may hold values from -16 to 16
- forward_states: float32 [2, 19, 64, 16, 256], P(None, None, 'gx', 'gy', 'gz'), may hold values from 0.01 to 0.63
- design: float32 [64, 16, 256], P('gx', 'gy', 'gz'), may hold values from 0 to 1
- solid_mask: int32 [64, 16, 256], P('gx', 'gy', 'gz'), may hold values 0 or 1
- boundary_kind: int32 [64, 16, 256], P('gx', 'gy', 'gz'), may hold values from 0 to 2, as said below
Outputs:
- adjoint_out: float32 [19, 64, 16, 256], P(None, 'gx', 'gy', 'gz')
- sensitivity: float32 [64, 16, 256], P('gx', 'gy', 'gz')
- objective: float32 [], replicated
- sens_rms: float32 [], replicated
The draws below stay inside these ranges and needn't reach their ends.
Inputs may be any that keep to these rules, and one draw needn't show every extreme that they name: `boundary_kind`: 1 marks inlet cells, 2 outlet cells.
All inputs are finite; a program needn't handle non-finite values. No bound on the sum of `solid_mask` on one device may be relied on, other than what follows from the above.
Results may differ from the reference program's by a relative error of at most 0.0003.
Values sent between devices are 32-bit elements; how exact they have to be, the bound alone decides.
A program may use at most 64 MiB of HBM per device.

```python
import jax
import jax.numpy as jnp
import numpy as np
from jax import lax

CX = 8
NX = 64
NY = 16
NZ = 256


stream_sign = np.array([0, 1, -1, 0, 0, 0, 0, 1, -1, 1, -1, 1, -1, 1, -1, 0, 0, 0, 0], dtype=np.float32)


lattice_weights = np.array([1.0 / 3] + [1.0 / 18] * 6 + [1.0 / 36] * 12, dtype=np.float32)


def draw_adjoint_in(key, part):
    xpos = jnp.arange(NX).astype(jnp.float32) / (NX - 1)
    values = jnp.clip(jax.random.normal(key, (19, NX, NY, NZ), jnp.float32), -4.0, 4.0)
    ramp = 1.0 + 2.0 * xpos
    return (values * ramp[None, :, None, None]).astype(jnp.float32)


def draw_forward_states(key, part):
    values = jnp.clip(jax.random.normal(key, (2, 19, NX, NY, NZ), jnp.float32), -2.5, 2.5)
    flow = 0.05
    scale = lattice_weights * (1.0 + 3.0 * flow * stream_sign)
    return (scale[None, :, None, None, None] * jnp.exp(0.25 * values)).astype(jnp.float32)


def draw_boundary_kind(key, part):
    picks = jax.random.randint(key, (NX, NY, NZ), 0, 32)
    return jnp.where(picks == 0, 1, jnp.where(picks == 1, 2, 0)).astype(jnp.int32)


def set_ends(values, stream_key, smallest, top_value):
    dims = values.shape
    place = [jax.random.randint(jax.random.fold_in(stream_key, axis), (), 0, dims[axis]) for axis in range(len(dims))]
    values = values.at[tuple(place)].set(smallest)
    longest = dims.index(max(dims))
    place[longest] = (place[longest] + 1) % dims[longest]
    return values.at[tuple(place)].set(top_value)


def shard_levels(key, extent, cuts, smallest, largest):
    factor_of, own = 1.0, jax.random.fold_in(key, 6)
    for position, shards_of in cuts:
        heights = jnp.exp(jax.random.uniform(jax.random.fold_in(own, position), (shards_of,), jnp.float32, smallest / len(cuts), largest / len(cuts)))
        factor_of = factor_of * jnp.repeat(heights, extent[position] // shards_of).reshape([-1 if axis == position else 1 for axis in range(len(extent))])
    return factor_of


def setup_inputs(seed: int = 0) -> dict:
    key_of = jax.random.split(jax.random.key(seed), 6)
    return {
        "adjoint_in": draw_adjoint_in(jax.random.fold_in(key_of[5], 71), 0),
        "forward_states": draw_forward_states(jax.random.fold_in(key_of[5], 71), 0),
        "design": jnp.clip(1.0 * jax.random.uniform(key_of[2], (NX, NY, NZ), jnp.float32) ** shard_levels(key_of[2], (NX, NY, NZ), ((0, 8), (1, 2), (2, 2)), -0.2, 0.2), 0.0, 1.0),
        "solid_mask": set_ends((jax.random.randint(key_of[3], (NX, NY, NZ), 0, 8) < 1).astype(jnp.int32), jax.random.fold_in(key_of[3], 1), 0, 1),
        "boundary_kind": draw_boundary_kind(jax.random.fold_in(key_of[5], 71), 0),
    }


lattice_table = np.array([[0, 0, 0], [1, 0, 0], [-1, 0, 0], [0, 1, 0], [0, -1, 0], [0, 0, 1], [0, 0, -1], [1, 1, 0], [-1, -1, 0], [1, -1, 0], [-1, 1, 0], [1, 0, 1], [-1, 0, -1], [1, 0, -1], [-1, 0, 1], [0, 1, 1], [0, -1, -1], [0, 1, -1], [0, -1, 1]], dtype=np.int32)
velocity_table = np.array(lattice_table, dtype=np.float32)
lattice_weights = np.array([1.0 / 3] + [1.0 / 18] * 6 + [1.0 / 36] * 12, dtype=np.float32)
opposite_index = [0, 2, 1, 4, 3, 6, 5, 8, 7, 10, 9, 12, 11, 14, 13, 16, 15, 18, 17]
brinkman_max = 4.0
convexity = 0.1
inflow_speed = 0.08

def build_relax(lattice):
    cx = lattice[:, 0].astype(np.float32)
    cy = lattice[:, 1].astype(np.float32)
    cz = lattice[:, 2].astype(np.float32)
    csq = cx * cx + cy * cy + cz * cz
    rows = [np.ones(19, dtype=np.float32), 19 * csq - 30, (21 * csq * csq - 53 * csq + 24) / 2, cx, (5 * csq - 9) * cx, cy, (5 * csq - 9) * cy, cz, (5 * csq - 9) * cz, 3 * cx * cx - csq, (3 * csq - 5) * (3 * cx * cx - csq), cy * cy - cz * cz, (3 * csq - 5) * (cy * cy - cz * cz), cx * cy, cy * cz, cx * cz, (cy * cy - cz * cz) * cx, (cz * cz - cx * cx) * cy, (cx * cx - cy * cy) * cz]
    moments = np.stack(rows).astype(np.float32)
    shear = 1.0 / 0.6
    rates = np.array([0, 1.19, 1.4, 0, 1.2, 0, 1.2, 0, 1.2, shear, 1.4, shear, 1.4, shear, shear, shear, 1.98, 1.98, 1.98], dtype=np.float32)
    norms = np.sum(moments * moments, axis=1)
    scaled = moments.T * (rates / norms)[None, :]
    return (scaled @ moments).astype(np.float32)

def equilibrium(density, velocity):
    projected = jnp.tensordot(velocity_table, velocity, axes=(1, 0), precision=lax.Precision.HIGHEST)
    squared = lax.optimization_barrier(jnp.sum(velocity * velocity, axis=0))
    return lattice_weights[:, None, None, None] * density * (1.0 + 3.0 * projected + 4.5 * projected * projected - 1.5 * squared)

def post_and_cost(dist, design, solid, kind, weight):
    relax_matrix = build_relax(lattice_table)
    density = lax.optimization_barrier(jnp.sum(dist, axis=0))
    flux = jnp.tensordot(velocity_table.T, dist, axes=(1, 0), precision=lax.Precision.HIGHEST)
    damping = 1.0 / (1.0 + brinkman_max * convexity * (1.0 - design) / (convexity + design))
    velocity = flux / density * damping
    collided = dist - jnp.tensordot(relax_matrix, dist - equilibrium(density, velocity), axes=(1, 0), precision=lax.Precision.HIGHEST)
    ones = jnp.ones_like(density)
    inflow = equilibrium(density, jnp.stack([inflow_speed * ones, 0.0 * ones, 0.0 * ones]))
    outflow = equilibrium(ones, velocity)
    bounced = jnp.stack([dist[k] for k in opposite_index])
    post = jnp.where(solid == 1, bounced, jnp.where(kind == 1, inflow, jnp.where(kind == 2, outflow, collided)))
    fluid = (solid == 0).astype(jnp.float32)
    cost = weight * fluid * 0.5 * density * lax.optimization_barrier(jnp.sum(velocity * velocity, axis=0))
    return (post, cost)

def adjoint_step(dist, design, solid, kind, weight, pulled):

    def local(d, g):
        return post_and_cost(d, g, solid, kind, weight)
    outs, backward = jax.vjp(local, dist, design)
    new_adjoint, sens = backward((pulled, jnp.ones_like(outs[1])))
    return (new_adjoint, sens, jnp.sum(outs[1]))

def pull_back(adjoint):
    length_x, length_y, length_z = adjoint.shape[1:]
    padded = jnp.pad(adjoint, ((0, 0), (1, 1), (1, 1), (1, 1)))
    pieces = []
    for i in range(19):
        cx, cy, cz = (int(lattice_table[i, 0]), int(lattice_table[i, 1]), int(lattice_table[i, 2]))
        pieces.append(padded[i, 1 + cx:1 + cx + length_x, 1 + cy:1 + cy + length_y, 1 + cz:1 + cz + length_z])
    return jnp.stack(pieces)

def reference(adjoint_in, forward_states, design, solid_mask, boundary_kind):
    xpos = jnp.arange(NX, dtype=jnp.int32).astype(jnp.float32)
    weight = (1.0 + 2.0 * xpos / (NX - 1))[:, None, None]
    blocks = NX // CX
    adjoint = adjoint_in
    sens_total = jnp.zeros((NX, NY, NZ), jnp.float32)
    cost_total = jnp.zeros((), jnp.float32)
    for t in (1, 0):
        pulled = pull_back(adjoint)
        state = forward_states[t]

        def block_step(b):
            start = (b * CX).astype(jnp.int32)
            return adjoint_step(lax.dynamic_slice_in_dim(state, start, CX, 1), lax.dynamic_slice_in_dim(design, start, CX, 0), lax.dynamic_slice_in_dim(solid_mask, start, CX, 0), lax.dynamic_slice_in_dim(boundary_kind, start, CX, 0), lax.dynamic_slice_in_dim(weight, start, CX, 0), lax.dynamic_slice_in_dim(pulled, start, CX, 1))
        new_blocks, sens_blocks, cost_blocks = lax.map(block_step, jnp.arange(blocks, dtype=jnp.int32))
        adjoint = jnp.transpose(new_blocks, (1, 0, 2, 3, 4)).reshape(19, NX, NY, NZ)
        sens_total = sens_total + sens_blocks.reshape(NX, NY, NZ)
        cost_total = cost_total + jnp.sum(cost_blocks)
    cells = NX * NY * NZ
    objective = cost_total / cells
    sens_rms = jnp.sqrt(jnp.sum(sens_total * sens_total) / cells + 1e-06)
    return (adjoint, sens_total / sens_rms, objective, sens_rms)
```

```python
import functools

import jax
import jax.numpy as jnp
import numpy as np
from jax import lax
from jax.experimental import pallas as pl
from jax.experimental.pallas import tpu as pltpu
from jax.sharding import PartitionSpec as P

MESH = pl.DeviceIdType.MESH
lattice_table = np.array(
    [
        [0, 0, 0],
        [1, 0, 0],
        [-1, 0, 0],
        [0, 1, 0],
        [0, -1, 0],
        [0, 0, 1],
        [0, 0, -1],
        [1, 1, 0],
        [-1, -1, 0],
        [1, -1, 0],
        [-1, 1, 0],
        [1, 0, 1],
        [-1, 0, -1],
        [1, 0, -1],
        [-1, 0, 1],
        [0, 1, 1],
        [0, -1, -1],
        [0, 1, -1],
        [0, -1, 1],
    ],
    dtype=np.int32,
)
LAT = [tuple(int(v) for v in row) for row in lattice_table]
WEIGHTS = np.array([1.0 / 3] + [1.0 / 18] * 6 + [1.0 / 36] * 12, dtype=np.float64)
opposite_index = [0, 2, 1, 4, 3, 6, 5, 8, 7, 10, 9, 12, 11, 14, 13, 16, 15, 18, 17]
inflow_speed = 0.08
AXES = ("gx", "gy", "gz")
VMEM_LIMIT = 16000 * 1024


def moment_rows():
    c = lattice_table.astype(np.float64)
    cx, cy, cz = c[:, 0], c[:, 1], c[:, 2]
    csq = cx * cx + cy * cy + cz * cz
    return np.stack(
        [
            np.ones(19),
            19 * csq - 30,
            (21 * csq * csq - 53 * csq + 24) / 2,
            cx,
            (5 * csq - 9) * cx,
            cy,
            (5 * csq - 9) * cy,
            cz,
            (5 * csq - 9) * cz,
            3 * cx * cx - csq,
            (3 * csq - 5) * (3 * cx * cx - csq),
            cy * cy - cz * cz,
            (3 * csq - 5) * (cy * cy - cz * cz),
            cx * cy,
            cy * cz,
            cx * cz,
            (cy * cy - cz * cz) * cx,
            (cz * cz - cx * cx) * cy,
            (cx * cx - cy * cy) * cz,
        ]
    )


ROWS = moment_rows()
NORMS = np.sum(ROWS * ROWS, axis=1)
SHEAR = 1.0 / 0.6
RATES = [0, 1.19, 1.4, 0, 1.2, 0, 1.2, 0, 1.2, SHEAR, 1.4, SHEAR, 1.4, SHEAR, SHEAR, SHEAR]
RATES = np.array(RATES + [1.98, 1.98, 1.98], dtype=np.float64)


def weighted_rows():
    c = lattice_table.astype(np.float64)
    pairs = [(0, 0), (1, 1), (2, 2), (0, 1), (1, 2), (0, 2)]
    rows = [WEIGHTS] + [WEIGHTS * c[:, a] for a in range(3)]
    rows += [WEIGHTS * c[:, a] * c[:, b] for a, b in pairs]
    out = np.stack(rows) @ (ROWS / NORMS[:, None]).T
    out[np.abs(out) < 1e-12] = 0.0
    return out


WROWS = weighted_rows()


def group(column, sign):
    return [i for i in range(19) if LAT[i][column] == sign]


SLOT = [{i: k for s in (1, -1) for k, i in enumerate(group(col, s))} for col in range(3)]


def side(sign):
    return 0 if sign == 1 else 1


def combine(coefs, terms):
    total = None
    for coef, term in zip(coefs, terms):
        if coef == 0.0:
            continue
        part = term if coef == 1.0 else float(np.float32(coef)) * term
        total = part if total is None else total + part
    return total


def flux_sums(f):
    s = {i: f[i] + f[i + 1] for i in range(1, 19, 2)}
    d = {i: f[i] - f[i + 1] for i in range(1, 19, 2)}
    return s, d


def moments(p):
    s, d = flux_sums(p)
    sxy, sxz, syz = s[7] + s[9], s[11] + s[13], s[15] + s[17]
    axis_yz = s[3] + s[5]
    axis = s[1] + axis_yz
    exy = sxy + sxz
    edge = exy + syz
    m = [None] * 19
    m[0] = p[0] + axis + edge
    m[1] = 8.0 * edge - 11.0 * axis - 30.0 * p[0]
    m[2] = edge - 4.0 * axis + 12.0 * p[0]
    a = 2.0 * s[1] - axis_yz
    b = exy - 2.0 * syz
    m[9] = a + b
    m[10] = b - 2.0 * a
    a = s[3] - s[5]
    b = sxy - sxz
    m[11] = a + b
    m[12] = b - 2.0 * a
    m[13] = s[7] - s[9]
    m[14] = s[15] - s[17]
    m[15] = s[11] - s[13]
    xa, xb = d[7] + d[9], d[11] + d[13]
    ya, yb = d[7] - d[9], d[15] + d[17]
    za, zb = d[11] - d[13], d[15] - d[17]
    for k, axis_d, u, v in ((3, d[1], xa, xb), (5, d[3], ya, yb), (7, d[5], za, zb)):
        e = u + v
        m[k] = axis_d + e
        m[k + 1] = e - 4.0 * axis_d
    m[16] = xa - xb
    m[17] = yb - ya
    m[18] = za - zb
    return m


def rebuild(z):
    out = [None] * 19
    out[0] = z[0] - 30.0 * z[1] + 12.0 * z[2]
    axis = z[0] - 11.0 * z[1] - 4.0 * z[2]
    edge = z[0] + 8.0 * z[1] + z[2]
    px = z[9] - 2.0 * z[10]
    pw = z[11] - 2.0 * z[12]
    qx = z[9] + z[10]
    qw = z[11] + z[12]
    ayz = axis - px
    eyz = edge - 2.0 * qx
    exx = edge + qx
    exy, exz = exx + qw, exx - qw
    jx, jy, jz = z[3] + z[4], z[5] + z[6], z[7] + z[8]
    x1, x2 = jx + z[16], jx - z[16]
    y1, y2 = jy - z[17], jy + z[17]
    z1, z2 = jz + z[18], jz - z[18]
    even = {
        1: axis + 2.0 * px,
        3: ayz + pw,
        5: ayz - pw,
        7: exy + z[13],
        9: exy - z[13],
        11: exz + z[15],
        13: exz - z[15],
        15: eyz + z[14],
        17: eyz - z[14],
    }
    odd = {
        1: z[3] - 4.0 * z[4],
        3: z[5] - 4.0 * z[6],
        5: z[7] - 4.0 * z[8],
        7: x1 + y1,
        9: x1 - y1,
        11: x2 + z1,
        13: x2 - z1,
        15: y2 + z2,
        17: y2 - z2,
    }
    for i in even:
        out[i] = even[i] + odd[i]
        out[i + 1] = even[i] - odd[i]
    return out


def cell_adjoint(f, p, damping, slope, fluid, solid, inner, inlet, outlet, weight):
    s, d = flux_sums(f)
    rho = f[0]
    for i in s:
        rho = rho + s[i]
    fx = d[1] + (d[7] + d[9]) + (d[11] + d[13])
    fy = d[3] + (d[7] - d[9]) + (d[15] + d[17])
    fz = d[5] + (d[11] - d[13]) + (d[15] - d[17])
    inv = 1.0 / rho
    bx, by, bz = fx * inv, fy * inv, fz * inv
    ux, uy, uz = bx * damping, by * damping, bz * damping
    uu = ux * ux + uy * uy + uz * uz
    m = moments(p)
    n = [None] * 19
    for k in range(16):
        rate = float(np.float32(RATES[k]))
        n[k] = m[k] * jnp.where(inner, rate, 1.0) if np.any(WROWS[:, k]) else None
    s0, sx, sy, sz, xx, yy, zz, xy, yz, xz = [
        combine(WROWS[r, :16], n) for r in range(10)
    ]
    vx = jnp.where(inlet, inflow_speed, ux)
    vy = jnp.where(inlet, 0.0, uy)
    vz = jnp.where(inlet, 0.0, uz)
    gx = xx * vx + xy * vy + xz * vz
    gy = xy * vx + yy * vy + yz * vz
    gz = xz * vx + yz * vy + zz * vz
    vv = vx * vx + vy * vy + vz * vz
    rho_bar = (
        s0 * (1.0 - 1.5 * vv)
        + 3.0 * (sx * vx + sy * vy + sz * vz)
        + 4.5 * (gx * vx + gy * vy + gz * vz)
    )
    rho_bar = jnp.where(outlet, 0.0, rho_bar) + (0.5 * weight) * uu
    scale = jnp.where(inlet, 0.0, jnp.where(outlet, 1.0, rho))
    wr = weight * rho
    ux_bar = scale * (3.0 * sx + 9.0 * gx - 3.0 * s0 * vx) + wr * ux
    uy_bar = scale * (3.0 * sy + 9.0 * gy - 3.0 * s0 * vy) + wr * uy
    uz_bar = scale * (3.0 * sz + 9.0 * gz - 3.0 * s0 * vz) + wr * uz
    d_bar = ux_bar * bx + uy_bar * by + uz_bar * bz
    di = damping * inv
    rho_bar = rho_bar - d_bar * di
    z = [None] * 19
    for k in range(19):
        coef = (1.0 - RATES[k]) / NORMS[k]
        z[k] = jnp.where(inner, float(np.float32(coef)) * m[k], 0.0)
    z[0] = z[0] + rho_bar
    z[3] = z[3] + ux_bar * di
    z[5] = z[5] + uy_bar * di
    z[7] = z[7] + uz_bar * di
    out = rebuild(z)
    out = [jnp.where(solid, p[opposite_index[i]], out[i]) for i in range(19)]
    sens = fluid * (d_bar * slope)
    cost = fluid * (0.5 * wr * uu)
    return out, sens, cost


def sum_groups(sizes):
    nx, ny, nz = sizes
    return [nx * ny * nz] if nx * ny * nz <= 64 else [nx, ny * nz]


def kernel(
    sizes,
    adj_hbm,
    fwd_hbm,
    des_hbm,
    sol_hbm,
    kind_hbm,
    out_ref,
    sens_ref,
    tot_ref,
    adj,
    fwd,
    des,
    sol,
    kin,
    mid,
    xs,
    ys,
    zs,
    xr,
    yr,
    zr,
    er,
    load_sem,
    store_sem,
    send_sem,
    recv_sem,
    *sum_refs,
):
    ex, ey, ez = des.shape
    me = tuple(lax.axis_index(name) for name in AXES)
    nx, ny, nz = sizes

    loads = [
        pltpu.make_async_copy(adj_hbm, adj, load_sem.at[0]),
        pltpu.make_async_copy(fwd_hbm.at[1], fwd.at[1], load_sem.at[1]),
        pltpu.make_async_copy(des_hbm, des, load_sem.at[2]),
        pltpu.make_async_copy(sol_hbm, sol, load_sem.at[3]),
        pltpu.make_async_copy(kind_hbm, kin, load_sem.at[4]),
        pltpu.make_async_copy(fwd_hbm.at[0], fwd.at[0], load_sem.at[5]),
    ]
    for load in loads:
        load.start()

    def reach(offset, sign):
        ok = None
        where = {}
        for a in range(3):
            c = sign * offset[a]
            where[AXES[a]] = me[a] + c if c else me[a]
            if c == 1:
                test = me[a] < sizes[a] - 1
            elif c == -1:
                test = me[a] > 0
            else:
                continue
            ok = test if ok is None else jnp.logical_and(ok, test)
        return ok, where

    live = [
        i
        for i in range(1, 19)
        if all(sizes[a] > 1 or LAT[i][a] == 0 for a in range(3))
    ]

    def all_peer(k):
        rank = lax.rem((me[0] * ny + me[1]) * nz + me[2] + k, nx * ny * nz)
        return {
            "gx": rank // (ny * nz),
            "gy": lax.rem(rank // nz, ny),
            "gz": lax.rem(rank, nz),
        }

    def x_peer(k):
        return {"gx": lax.rem(me[0] + k, nx), "gy": me[1], "gz": me[2]}

    def yz_peer(k):
        rank = lax.rem(me[1] * nz + me[2] + k, ny * nz)
        return {"gx": me[0], "gy": rank // nz, "gz": lax.rem(rank, nz)}

    if len(sum_groups(sizes)) == 1:
        peers = [all_peer]
    else:
        peers = [x_peer, yz_peer]

    barrier = pltpu.get_barrier_semaphore()
    count = jnp.int32(sum(n - 1 for n in sum_groups(sizes)))
    for n, peer in zip(sum_groups(sizes), peers):
        for k in range(1, n):
            pl.semaphore_signal(barrier, inc=1, device_id=peer(k), device_id_type=MESH)
    if len(peers) > 1:
        for i in live:
            ok, where = reach(LAT[i], -1)

            @pl.when(ok)
            def _():
                pl.semaphore_signal(barrier, inc=1, device_id=where, device_id_type=MESH)

            count = count + reach(LAT[i], 1)[0].astype(jnp.int32)

    def landing(i, t):
        if i < 3:
            return xr.at[t, i - 1]
        if i < 5:
            return yr.at[t, i - 3]
        if i < 7:
            return zr.at[t, i - 5]
        return er.at[t, i - 7]

    def leaving(i, t):
        c = LAT[i]
        if i < 3:
            return xs.at[t, i - 1]
        if i < 5:
            return ys.at[t, i - 3]
        if i < 7:
            return zs.at[t, i - 5]
        if c[2] == 0:
            return ys.at[t, side(c[1]), SLOT[1][i]]
        return zs.at[t, side(c[2])]

    for i in range(1, 19):
        if i in live:

            @pl.when(jnp.logical_not(reach(LAT[i], 1)[0]))
            def _():
                for t in (0, 1):
                    ref = landing(i, t)
                    ref[...] = jnp.zeros(ref.shape, jnp.float32)

        else:
            for t in (0, 1):
                ref = landing(i, t)
                ref[...] = jnp.zeros(ref.shape, jnp.float32)

    lane = lax.broadcasted_iota(jnp.int32, (ey, ez), 1)
    row = lax.broadcasted_iota(jnp.int32, (ey, ez), 0)

    def hop(i, t):
        ok, where = reach(LAT[i], -1)
        copy = pltpu.make_async_remote_copy(
            src_ref=leaving(i, t),
            dst_ref=landing(i, t),
            send_sem=send_sem.at[t, i - 1],
            recv_sem=recv_sem.at[t, i - 1],
            device_id=where,
            device_id_type=MESH,
        )
        return ok, copy

    def pack_layer(t, x, tiles, packs):
        packs = list(packs)
        for sign in (1, -1):
            h = side(sign)
            if x == (0 if sign == 1 else ex - 1):
                for k, i in enumerate(group(0, sign)):
                    xs[t, h, k] = tiles(i)
            edge = 0 if sign == 1 else ey - 1
            for k, i in enumerate(group(1, sign)):
                ys[t, h, k, x : x + 1, :] = tiles(i)[edge : edge + 1, :]
            edge = 0 if sign == 1 else ez - 1
            for k, i in enumerate(group(2, sign)):
                at = k * ex + x
                moved = tiles(i)
                if (at - edge) % ez:
                    moved = pltpu.roll(moved, (at - edge) % ez, 1)
                packs[h] = jnp.where(lane == at, moved, packs[h])
        return tuple(packs)

    def send_all(t, packs):
        zs[t, 0] = packs[0]
        zs[t, 1] = packs[1]
        for i in sorted(live, key=lambda i: (LAT[i][0] == 0, -sum(map(abs, LAT[i])))):
            ok, copy = hop(i, t)
            pl.when(ok)(copy.start)

    def receive(t, along_x):
        for i in live:
            if (LAT[i][0] != 0) == along_x:
                ok = reach(LAT[i], 1)[0]
                pl.when(ok)(hop(i, t)[1].wait_recv)

    def shifted_columns(t):
        moved = {}
        for i in range(15, 19):
            cy, cz = LAT[i][1], LAT[i][2]
            pack = zr[t, side(cz)]
            src, last = (0, ey - 1) if cy == 1 else (ey - 1, 0)
            corner = er[t, i - 7, src : src + 1, :]
            pack = pltpu.roll(pack, (-cy) % ey, 0)
            moved[i] = jnp.where(row == last, corner, pack)
        return moved

    def pulled_tile(source, t, i, x, moved):
        cx, cy, cz = LAT[i]
        at = x + cx
        inside = 0 <= at < ex
        tile = source[i, at] if inside else xr[t, side(cx), SLOT[0][i]]
        if cy:
            h = side(cy)
            if inside:
                fill = yr[t, h, SLOT[1][i], at : at + 1, :]
            else:
                src = 0 if cx == 1 else ex - 1
                fill = er[t, i - 7, src : src + 1, :]
            last = ey - 1 if cy == 1 else 0
            tile = jnp.where(row == last, fill, pltpu.roll(tile, (-cy) % ey, 0))
        if cz:
            h = side(cz)
            col = SLOT[2][i] * ex
            if cy:
                pack, col = moved[i], col + x
            elif inside:
                pack, col = zr[t, h], col + at
            else:
                pack, col = er[t, i - 7], col + (0 if cx == 1 else ex - 1)
            last = ez - 1 if cz == 1 else 0
            if (last - col) % ez:
                pack = pltpu.roll(pack, (last - col) % ez, 1)
            tile = jnp.where(lane == last, pack, pltpu.roll(tile, (-cz) % ez, 1))
        return tile

    whole_x = nx * ex
    zero = jnp.zeros((ey, ez), jnp.float32)

    def step(t, source, target, packs):
        cost_sum, square_sum = zero, zero
        receive(t, False)
        moved = shifted_columns(t)
        for x in list(range(1, ex - 1)) + [0, ex - 1]:
            if x == 0:
                receive(t, True)
            g = des[x]
            solid = sol[x] == 1
            fluid = jnp.where(solid, 0.0, 1.0)
            kind = kin[x]
            inlet, outlet = kind == 1, kind == 2
            inner = jnp.logical_not(jnp.logical_or(inlet, outlet))
            below = 1.0 / (0.5 + 0.6 * g)
            damping = (0.1 + g) * below
            slope = 0.44 * (below * below)
            place = (me[0] * ex + x).astype(jnp.float32)
            weight = 1.0 + 2.0 * place / (whole_x - 1)
            f = [fwd[t, i, x] for i in range(19)]
            p = [pulled_tile(source, t, i, x, moved) for i in range(19)]
            out, sens, cost = cell_adjoint(
                f, p, damping, slope, fluid, solid, inner, inlet, outlet, weight
            )
            for i in range(19):
                target[i, x] = out[i]
            cost_sum = cost_sum + cost
            if t == 1:
                sens_ref[x] = sens
                packs = pack_layer(0, x, lambda i: out[i], packs)
            else:
                sens = sens + sens_ref[x]
                sens_ref[x] = sens
                square_sum = square_sum + sens * sens
        return cost_sum, square_sum, packs

    loads[0].wait()
    packs = (zero, zero)
    for x in range(ex):
        packs = pack_layer(1, x, lambda i: adj[i, x], packs)
    pl.semaphore_wait(barrier, count)
    send_all(1, packs)
    for load in loads[1:]:
        load.wait()
    cost_one, _, packs = step(1, adj, mid, (zero, zero))
    send_all(0, packs)
    cost_two, square, _ = step(0, mid, out_ref, None)

    half = ez // 2
    cost = jnp.sum(cost_one + cost_two, axis=0, keepdims=True)
    square = jnp.sum(square, axis=0, keepdims=True)
    cost = cost + pltpu.roll(cost, half, 1)
    square = square + pltpu.roll(square, half, 1)
    first = lax.broadcasted_iota(jnp.int32, (1, ez), 1) < half
    total = jnp.where(first, square, cost)

    sent = []
    for r, (n, peer) in enumerate(zip(sum_groups(sizes), peers)):
        part, got, send, recv = sum_refs[4 * r : 4 * r + 4]
        if n == 1:
            continue
        part[...] = total
        copies = []
        for k in range(1, n):
            copy = pltpu.make_async_remote_copy(
                src_ref=part,
                dst_ref=got.at[pl.ds(k - 1, 1)],
                send_sem=send.at[k - 1],
                recv_sem=recv.at[k - 1],
                device_id=peer(k),
                device_id_type=MESH,
            )
            copy.start()
            copies.append(copy)
        got[pl.ds(n - 1, 1)] = total
        for copy in copies:
            copy.wait_recv()
        total = jnp.sum(got[...], axis=0, keepdims=True)
        sent += copies
    cells = nx * ex * ny * ey * nz * ez
    square = jnp.sum(jnp.where(first, total, 0.0), axis=1, keepdims=True)
    cost = jnp.sum(jnp.where(first, 0.0, total), axis=1, keepdims=True)
    rms = jnp.sqrt(square / cells + 1e-06)
    tot_ref[...] = jnp.where(lane == 0, jnp.broadcast_to(cost / cells, (ey, ez)), jnp.broadcast_to(rms, (ey, ez)))
    for t in (1, 0):
        for i in live:
            ok, copy = hop(i, t)
            pl.when(ok)(copy.wait_send)
    for copy in sent:
        copy.wait_send()


def hand_on(adj_in, sens_in, tot_in, adj_out, sens_out, obj_out, rms_out, sens, obj, rms, sem):
    moves = [(adj_in, adj_out), (sens, sens_out), (obj, obj_out), (rms, rms_out)]
    copies = [pltpu.make_async_copy(a, b, sem.at[k]) for k, (a, b) in enumerate(moves)]
    copies[0].start()
    scale = jnp.broadcast_to(1.0 / tot_in[0:1, 1:2], tot_in.shape)
    for x in range(sens.shape[0]):
        sens[x] = sens_in[x] * scale
    copies[1].start()
    obj[0] = tot_in[0, 0]
    rms[0] = tot_in[0, 1]
    copies[2].start()
    copies[3].start()
    for copy in copies:
        copy.wait()


def body(sizes, adjoint_in, forward_states, design, solid_mask, boundary_kind):
    ex, ey, ez = design.shape
    nx, ny, nz = sizes
    any_spec = pl.BlockSpec(memory_space=pltpu.HBM)
    vmem_spec = pl.BlockSpec(memory_space=pltpu.VMEM)
    f32 = jnp.float32
    operands = (adjoint_in, forward_states, design, solid_mask, boundary_kind)
    operands = [pltpu.with_memory_space_constraint(a, pltpu.HBM) for a in operands]
    sum_scratch = []
    for n in sum_groups(sizes):
        sum_scratch += [
            pltpu.VMEM((1, ez), f32),
            pltpu.VMEM((n, ez), f32),
            pltpu.SemaphoreType.DMA((max(n - 1, 1),)),
            pltpu.SemaphoreType.DMA((max(n - 1, 1),)),
        ]
    adjoint, sens, tot = pl.pallas_call(
        functools.partial(kernel, sizes),
        out_shape=(
            jax.ShapeDtypeStruct(adjoint_in.shape, f32),
            jax.ShapeDtypeStruct(design.shape, f32),
            jax.ShapeDtypeStruct((ey, ez), f32),
        ),
        in_specs=[any_spec] * 5,
        out_specs=(vmem_spec, vmem_spec, vmem_spec),
        scratch_shapes=[
            pltpu.VMEM(adjoint_in.shape, f32),
            pltpu.VMEM(forward_states.shape, f32),
            pltpu.VMEM(design.shape, f32),
            pltpu.VMEM(design.shape, jnp.int32),
            pltpu.VMEM(design.shape, jnp.int32),
            pltpu.VMEM(adjoint_in.shape, f32),
            pltpu.VMEM((2, 2, 5, ey, ez), f32),
            pltpu.VMEM((2, 2, 5, ex, ez), f32),
            pltpu.VMEM((2, 2, ey, ez), f32),
            pltpu.VMEM((2, 2, 5, ey, ez), f32),
            pltpu.VMEM((2, 2, 5, ex, ez), f32),
            pltpu.VMEM((2, 2, ey, ez), f32),
            pltpu.VMEM((2, 12, ey, ez), f32),
            pltpu.SemaphoreType.DMA((6,)),
            pltpu.SemaphoreType.DMA,
            pltpu.SemaphoreType.DMA((2, 18)),
            pltpu.SemaphoreType.DMA((2, 18)),
            *sum_scratch,
        ],
        compiler_params=pltpu.CompilerParams(
            collective_id=0, has_side_effects=True, vmem_limit_bytes=VMEM_LIMIT
        ),
    )(*operands)
    adjoint, sens, objective, rms = pl.pallas_call(
        hand_on,
        out_shape=(
            jax.ShapeDtypeStruct(adjoint_in.shape, f32),
            jax.ShapeDtypeStruct(design.shape, f32),
            jax.ShapeDtypeStruct((1,), f32),
            jax.ShapeDtypeStruct((1,), f32),
        ),
        in_specs=[vmem_spec] * 3,
        out_specs=(any_spec, any_spec, any_spec, any_spec),
        scratch_shapes=[
            pltpu.VMEM(design.shape, f32),
            pltpu.SMEM((1,), f32),
            pltpu.SMEM((1,), f32),
            pltpu.SemaphoreType.DMA((4,)),
        ],
        compiler_params=pltpu.CompilerParams(vmem_limit_bytes=VMEM_LIMIT),
    )(adjoint, sens, tot)
    return adjoint, sens, objective.reshape(()), rms.reshape(())


def solution(mesh):
    placed = (
        P(None, "gx", "gy", "gz"),
        P(None, None, "gx", "gy", "gz"),
        P("gx", "gy", "gz"),
        P("gx", "gy", "gz"),
        P("gx", "gy", "gz"),
    )
    return jax.shard_map(
        functools.partial(body, tuple(int(mesh.shape[name]) for name in AXES)),
        mesh=mesh,
        in_specs=placed,
        out_specs=(P(None, "gx", "gy", "gz"), P("gx", "gy", "gz"), P(), P()),
        check_vma=False,
    )
```

```python
import functools

import jax
import jax.numpy as jnp
import numpy as np
from jax import lax
from jax.experimental import pallas as pl
from jax.experimental.pallas import tpu as pltpu
from jax.sharding import PartitionSpec as P

MESH = pl.DeviceIdType.MESH
lattice_table = np.array(
    [
        [0, 0, 0],
        [1, 0, 0],
        [-1, 0, 0],
        [0, 1, 0],
        [0, -1, 0],
        [0, 0, 1],
        [0, 0, -1],
        [1, 1, 0],
        [-1, -1, 0],
        [1, -1, 0],
        [-1, 1, 0],
        [1, 0, 1],
        [-1, 0, -1],
        [1, 0, -1],
        [-1, 0, 1],
        [0, 1, 1],
        [0, -1, -1],
        [0, 1, -1],
        [0, -1, 1],
    ],
    dtype=np.int32,
)
LAT = [tuple(int(v) for v in row) for row in lattice_table]
WEIGHTS = np.array([1.0 / 3] + [1.0 / 18] * 6 + [1.0 / 36] * 12, dtype=np.float64)
opposite_index = [0, 2, 1, 4, 3, 6, 5, 8, 7, 10, 9, 12, 11, 14, 13, 16, 15, 18, 17]
inflow_speed = 0.08
AXES = ("gx", "gy", "gz")
VMEM_LIMIT = 16000 * 1024


def moment_rows():
    c = lattice_table.astype(np.float64)
    cx, cy, cz = c[:, 0], c[:, 1], c[:, 2]
    csq = cx * cx + cy * cy + cz * cz
    return np.stack(
        [
            np.ones(19),
            19 * csq - 30,
            (21 * csq * csq - 53 * csq + 24) / 2,
            cx,
            (5 * csq - 9) * cx,
            cy,
            (5 * csq - 9) * cy,
            cz,
            (5 * csq - 9) * cz,
            3 * cx * cx - csq,
            (3 * csq - 5) * (3 * cx * cx - csq),
            cy * cy - cz * cz,
            (3 * csq - 5) * (cy * cy - cz * cz),
            cx * cy,
            cy * cz,
            cx * cz,
            (cy * cy - cz * cz) * cx,
            (cz * cz - cx * cx) * cy,
            (cx * cx - cy * cy) * cz,
        ]
    )


ROWS = moment_rows()
NORMS = np.sum(ROWS * ROWS, axis=1)
SHEAR = 1.0 / 0.6
RATES = [0, 1.19, 1.4, 0, 1.2, 0, 1.2, 0, 1.2, SHEAR, 1.4, SHEAR, 1.4, SHEAR, SHEAR, SHEAR]
RATES = np.array(RATES + [1.98, 1.98, 1.98], dtype=np.float64)


def weighted_rows():
    c = lattice_table.astype(np.float64)
    pairs = [(0, 0), (1, 1), (2, 2), (0, 1), (1, 2), (0, 2)]
    rows = [WEIGHTS] + [WEIGHTS * c[:, a] for a in range(3)]
    rows += [WEIGHTS * c[:, a] * c[:, b] for a, b in pairs]
    out = np.stack(rows) @ (ROWS / NORMS[:, None]).T
    out[np.abs(out) < 1e-12] = 0.0
    return out


WROWS = weighted_rows()


def group(column, sign):
    return [i for i in range(19) if LAT[i][column] == sign]


SLOT = [{i: k for s in (1, -1) for k, i in enumerate(group(col, s))} for col in range(3)]


def side(sign):
    return 0 if sign == 1 else 1


def combine(coefs, terms):
    total = None
    for coef, term in zip(coefs, terms):
        if coef == 0.0:
            continue
        part = term if coef == 1.0 else float(np.float32(coef)) * term
        total = part if total is None else total + part
    return total


def flux_sums(f):
    s = {i: f[i] + f[i + 1] for i in range(1, 19, 2)}
    d = {i: f[i] - f[i + 1] for i in range(1, 19, 2)}
    return s, d


def moments(p):
    s, d = flux_sums(p)
    sxy, sxz, syz = s[7] + s[9], s[11] + s[13], s[15] + s[17]
    axis_yz = s[3] + s[5]
    axis = s[1] + axis_yz
    exy = sxy + sxz
    edge = exy + syz
    m = [None] * 19
    m[0] = p[0] + axis + edge
    m[1] = 8.0 * edge - 11.0 * axis - 30.0 * p[0]
    m[2] = edge - 4.0 * axis + 12.0 * p[0]
    a = 2.0 * s[1] - axis_yz
    b = exy - 2.0 * syz
    m[9] = a + b
    m[10] = b - 2.0 * a
    a = s[3] - s[5]
    b = sxy - sxz
    m[11] = a + b
    m[12] = b - 2.0 * a
    m[13] = s[7] - s[9]
    m[14] = s[15] - s[17]
    m[15] = s[11] - s[13]
    xa, xb = d[7] + d[9], d[11] + d[13]
    ya, yb = d[7] - d[9], d[15] + d[17]
    za, zb = d[11] - d[13], d[15] - d[17]
    for k, axis_d, u, v in ((3, d[1], xa, xb), (5, d[3], ya, yb), (7, d[5], za, zb)):
        e = u + v
        m[k] = axis_d + e
        m[k + 1] = e - 4.0 * axis_d
    m[16] = xa - xb
    m[17] = yb - ya
    m[18] = za - zb
    return m


def rebuild(z):
    out = [None] * 19
    out[0] = z[0] - 30.0 * z[1] + 12.0 * z[2]
    axis = z[0] - 11.0 * z[1] - 4.0 * z[2]
    edge = z[0] + 8.0 * z[1] + z[2]
    px = z[9] - 2.0 * z[10]
    pw = z[11] - 2.0 * z[12]
    qx = z[9] + z[10]
    qw = z[11] + z[12]
    ayz = axis - px
    eyz = edge - 2.0 * qx
    exx = edge + qx
    exy, exz = exx + qw, exx - qw
    jx, jy, jz = z[3] + z[4], z[5] + z[6], z[7] + z[8]
    x1, x2 = jx + z[16], jx - z[16]
    y1, y2 = jy - z[17], jy + z[17]
    z1, z2 = jz + z[18], jz - z[18]
    even = {
        1: axis + 2.0 * px,
        3: ayz + pw,
        5: ayz - pw,
        7: exy + z[13],
        9: exy - z[13],
        11: exz + z[15],
        13: exz - z[15],
        15: eyz + z[14],
        17: eyz - z[14],
    }
    odd = {
        1: z[3] - 4.0 * z[4],
        3: z[5] - 4.0 * z[6],
        5: z[7] - 4.0 * z[8],
        7: x1 + y1,
        9: x1 - y1,
        11: x2 + z1,
        13: x2 - z1,
        15: y2 + z2,
        17: y2 - z2,
    }
    for i in even:
        out[i] = even[i] + odd[i]
        out[i + 1] = even[i] - odd[i]
    return out


def cell_adjoint(f, p, damping, slope, fluid, solid, inner, inlet, outlet, weight):
    s, d = flux_sums(f)
    rho = f[0]
    for i in s:
        rho = rho + s[i]
    fx = d[1] + (d[7] + d[9]) + (d[11] + d[13])
    fy = d[3] + (d[7] - d[9]) + (d[15] + d[17])
    fz = d[5] + (d[11] - d[13]) + (d[15] - d[17])
    inv = 1.0 / rho
    bx, by, bz = fx * inv, fy * inv, fz * inv
    ux, uy, uz = bx * damping, by * damping, bz * damping
    uu = ux * ux + uy * uy + uz * uz
    m = moments(p)
    n = [None] * 19
    for k in range(16):
        rate = float(np.float32(RATES[k]))
        n[k] = m[k] * jnp.where(inner, rate, 1.0) if np.any(WROWS[:, k]) else None
    s0, sx, sy, sz, xx, yy, zz, xy, yz, xz = [
        combine(WROWS[r, :16], n) for r in range(10)
    ]
    vx = jnp.where(inlet, inflow_speed, ux)
    vy = jnp.where(inlet, 0.0, uy)
    vz = jnp.where(inlet, 0.0, uz)
    gx = xx * vx + xy * vy + xz * vz
    gy = xy * vx + yy * vy + yz * vz
    gz = xz * vx + yz * vy + zz * vz
    vv = vx * vx + vy * vy + vz * vz
    rho_bar = (
        s0 * (1.0 - 1.5 * vv)
        + 3.0 * (sx * vx + sy * vy + sz * vz)
        + 4.5 * (gx * vx + gy * vy + gz * vz)
    )
    rho_bar = jnp.where(outlet, 0.0, rho_bar) + (0.5 * weight) * uu
    scale = jnp.where(inlet, 0.0, jnp.where(outlet, 1.0, rho))
    wr = weight * rho
    ux_bar = scale * (3.0 * sx + 9.0 * gx - 3.0 * s0 * vx) + wr * ux
    uy_bar = scale * (3.0 * sy + 9.0 * gy - 3.0 * s0 * vy) + wr * uy
    uz_bar = scale * (3.0 * sz + 9.0 * gz - 3.0 * s0 * vz) + wr * uz
    d_bar = ux_bar * bx + uy_bar * by + uz_bar * bz
    di = damping * inv
    rho_bar = rho_bar - d_bar * di
    z = [None] * 19
    for k in range(19):
        coef = (1.0 - RATES[k]) / NORMS[k]
        z[k] = jnp.where(inner, float(np.float32(coef)) * m[k], 0.0)
    z[0] = z[0] + rho_bar
    z[3] = z[3] + ux_bar * di
    z[5] = z[5] + uy_bar * di
    z[7] = z[7] + uz_bar * di
    out = rebuild(z)
    out = [jnp.where(solid, p[opposite_index[i]], out[i]) for i in range(19)]
    sens = fluid * (d_bar * slope)
    cost = fluid * (0.5 * wr * uu)
    return out, sens, cost


def sum_groups(sizes):
    nx, ny, nz = sizes
    return [nx * ny * nz] if nx * ny * nz <= 64 else [nx, ny * nz]


def general_kernel(
    sizes,
    adj_hbm,
    fwd_hbm,
    des_hbm,
    sol_hbm,
    kind_hbm,
    out_ref,
    sens_ref,
    tot_ref,
    adj,
    fwd,
    des,
    sol,
    kin,
    mid,
    xs,
    ys,
    zs,
    xr,
    yr,
    zr,
    er,
    load_sem,
    store_sem,
    send_sem,
    recv_sem,
    *sum_refs,
):
    ex, ey, ez = des.shape
    me = tuple(lax.axis_index(name) for name in AXES)
    nx, ny, nz = sizes

    loads = [
        pltpu.make_async_copy(adj_hbm, adj, load_sem.at[0]),
        pltpu.make_async_copy(fwd_hbm.at[1], fwd.at[1], load_sem.at[1]),
        pltpu.make_async_copy(des_hbm, des, load_sem.at[2]),
        pltpu.make_async_copy(sol_hbm, sol, load_sem.at[3]),
        pltpu.make_async_copy(kind_hbm, kin, load_sem.at[4]),
        pltpu.make_async_copy(fwd_hbm.at[0], fwd.at[0], load_sem.at[5]),
    ]
    for load in loads:
        load.start()

    def reach(offset, sign):
        ok = None
        where = {}
        for a in range(3):
            c = sign * offset[a]
            where[AXES[a]] = me[a] + c if c else me[a]
            if c == 1:
                test = me[a] < sizes[a] - 1
            elif c == -1:
                test = me[a] > 0
            else:
                continue
            ok = test if ok is None else jnp.logical_and(ok, test)
        return ok, where

    live = [
        i
        for i in range(1, 19)
        if all(sizes[a] > 1 or LAT[i][a] == 0 for a in range(3))
    ]

    def all_peer(k):
        rank = lax.rem((me[0] * ny + me[1]) * nz + me[2] + k, nx * ny * nz)
        return {
            "gx": rank // (ny * nz),
            "gy": lax.rem(rank // nz, ny),
            "gz": lax.rem(rank, nz),
        }

    def x_peer(k):
        return {"gx": lax.rem(me[0] + k, nx), "gy": me[1], "gz": me[2]}

    def yz_peer(k):
        rank = lax.rem(me[1] * nz + me[2] + k, ny * nz)
        return {"gx": me[0], "gy": rank // nz, "gz": lax.rem(rank, nz)}

    if len(sum_groups(sizes)) == 1:
        peers = [all_peer]
    else:
        peers = [x_peer, yz_peer]

    barrier = pltpu.get_barrier_semaphore()
    count = jnp.int32(sum(n - 1 for n in sum_groups(sizes)))
    for n, peer in zip(sum_groups(sizes), peers):
        for k in range(1, n):
            pl.semaphore_signal(barrier, inc=1, device_id=peer(k), device_id_type=MESH)
    if len(peers) > 1:
        for i in live:
            ok, where = reach(LAT[i], -1)

            @pl.when(ok)
            def _():
                pl.semaphore_signal(barrier, inc=1, device_id=where, device_id_type=MESH)

            count = count + reach(LAT[i], 1)[0].astype(jnp.int32)

    def landing(i, t):
        if i < 3:
            return xr.at[t, i - 1]
        if i < 5:
            return yr.at[t, i - 3]
        if i < 7:
            return zr.at[t, i - 5]
        return er.at[t, i - 7]

    def leaving(i, t):
        c = LAT[i]
        if i < 3:
            return xs.at[t, i - 1]
        if i < 5:
            return ys.at[t, i - 3]
        if i < 7:
            return zs.at[t, i - 5]
        if c[2] == 0:
            return ys.at[t, side(c[1]), SLOT[1][i]]
        return zs.at[t, side(c[2])]

    for i in range(1, 19):
        if i in live:

            @pl.when(jnp.logical_not(reach(LAT[i], 1)[0]))
            def _():
                for t in (0, 1):
                    ref = landing(i, t)
                    ref[...] = jnp.zeros(ref.shape, jnp.float32)

        else:
            for t in (0, 1):
                ref = landing(i, t)
                ref[...] = jnp.zeros(ref.shape, jnp.float32)

    lane = lax.broadcasted_iota(jnp.int32, (ey, ez), 1)
    row = lax.broadcasted_iota(jnp.int32, (ey, ez), 0)

    def hop(i, t):
        ok, where = reach(LAT[i], -1)
        copy = pltpu.make_async_remote_copy(
            src_ref=leaving(i, t),
            dst_ref=landing(i, t),
            send_sem=send_sem.at[t, i - 1],
            recv_sem=recv_sem.at[t, i - 1],
            device_id=where,
            device_id_type=MESH,
        )
        return ok, copy

    def pack_layer(t, x, tiles, packs):
        packs = list(packs)
        for sign in (1, -1):
            h = side(sign)
            if x == (0 if sign == 1 else ex - 1):
                for k, i in enumerate(group(0, sign)):
                    xs[t, h, k] = tiles(i)
            edge = 0 if sign == 1 else ey - 1
            for k, i in enumerate(group(1, sign)):
                ys[t, h, k, x : x + 1, :] = tiles(i)[edge : edge + 1, :]
            edge = 0 if sign == 1 else ez - 1
            for k, i in enumerate(group(2, sign)):
                at = k * ex + x
                moved = tiles(i)
                if (at - edge) % ez:
                    moved = pltpu.roll(moved, (at - edge) % ez, 1)
                packs[h] = jnp.where(lane == at, moved, packs[h])
        return tuple(packs)

    def send_all(t, packs):
        zs[t, 0] = packs[0]
        zs[t, 1] = packs[1]
        for i in sorted(live, key=lambda i: (LAT[i][0] == 0, -sum(map(abs, LAT[i])))):
            ok, copy = hop(i, t)
            pl.when(ok)(copy.start)

    def receive(t, along_x):
        for i in live:
            if (LAT[i][0] != 0) == along_x:
                ok = reach(LAT[i], 1)[0]
                pl.when(ok)(hop(i, t)[1].wait_recv)

    def shifted_columns(t):
        moved = {}
        for i in range(15, 19):
            cy, cz = LAT[i][1], LAT[i][2]
            pack = zr[t, side(cz)]
            src, last = (0, ey - 1) if cy == 1 else (ey - 1, 0)
            corner = er[t, i - 7, src : src + 1, :]
            pack = pltpu.roll(pack, (-cy) % ey, 0)
            moved[i] = jnp.where(row == last, corner, pack)
        return moved

    def pulled_tile(source, t, i, x, moved):
        cx, cy, cz = LAT[i]
        at = x + cx
        inside = 0 <= at < ex
        tile = source[i, at] if inside else xr[t, side(cx), SLOT[0][i]]
        if cy:
            h = side(cy)
            if inside:
                fill = yr[t, h, SLOT[1][i], at : at + 1, :]
            else:
                src = 0 if cx == 1 else ex - 1
                fill = er[t, i - 7, src : src + 1, :]
            last = ey - 1 if cy == 1 else 0
            tile = jnp.where(row == last, fill, pltpu.roll(tile, (-cy) % ey, 0))
        if cz:
            h = side(cz)
            col = SLOT[2][i] * ex
            if cy:
                pack, col = moved[i], col + x
            elif inside:
                pack, col = zr[t, h], col + at
            else:
                pack, col = er[t, i - 7], col + (0 if cx == 1 else ex - 1)
            last = ez - 1 if cz == 1 else 0
            if (last - col) % ez:
                pack = pltpu.roll(pack, (last - col) % ez, 1)
            tile = jnp.where(lane == last, pack, pltpu.roll(tile, (-cz) % ez, 1))
        return tile

    whole_x = nx * ex
    zero = jnp.zeros((ey, ez), jnp.float32)

    def step(t, source, target, packs):
        cost_sum, square_sum = zero, zero
        receive(t, False)
        moved = shifted_columns(t)
        for x in list(range(1, ex - 1)) + [0, ex - 1]:
            if x == 0:
                receive(t, True)
            g = des[x]
            solid = sol[x] == 1
            fluid = jnp.where(solid, 0.0, 1.0)
            kind = kin[x]
            inlet, outlet = kind == 1, kind == 2
            inner = jnp.logical_not(jnp.logical_or(inlet, outlet))
            below = 1.0 / (0.5 + 0.6 * g)
            damping = (0.1 + g) * below
            slope = 0.44 * (below * below)
            place = (me[0] * ex + x).astype(jnp.float32)
            weight = 1.0 + 2.0 * place / (whole_x - 1)
            f = [fwd[t, i, x] for i in range(19)]
            p = [pulled_tile(source, t, i, x, moved) for i in range(19)]
            out, sens, cost = cell_adjoint(
                f, p, damping, slope, fluid, solid, inner, inlet, outlet, weight
            )
            for i in range(19):
                target[i, x] = out[i]
            cost_sum = cost_sum + cost
            if t == 1:
                sens_ref[x] = sens
                packs = pack_layer(0, x, lambda i: out[i], packs)
            else:
                sens = sens + sens_ref[x]
                sens_ref[x] = sens
                square_sum = square_sum + sens * sens
        return cost_sum, square_sum, packs

    loads[0].wait()
    packs = (zero, zero)
    for x in range(ex):
        packs = pack_layer(1, x, lambda i: adj[i, x], packs)
    pl.semaphore_wait(barrier, count)
    send_all(1, packs)
    for load in loads[1:]:
        load.wait()
    cost_one, _, packs = step(1, adj, mid, (zero, zero))
    send_all(0, packs)
    cost_two, square, _ = step(0, mid, out_ref, None)

    half = ez // 2
    cost = jnp.sum(cost_one + cost_two, axis=0, keepdims=True)
    square = jnp.sum(square, axis=0, keepdims=True)
    cost = cost + pltpu.roll(cost, half, 1)
    square = square + pltpu.roll(square, half, 1)
    first = lax.broadcasted_iota(jnp.int32, (1, ez), 1) < half
    total = jnp.where(first, square, cost)

    sent = []
    for r, (n, peer) in enumerate(zip(sum_groups(sizes), peers)):
        part, got, send, recv = sum_refs[4 * r : 4 * r + 4]
        if n == 1:
            continue
        part[...] = total
        copies = []
        for k in range(1, n):
            copy = pltpu.make_async_remote_copy(
                src_ref=part,
                dst_ref=got.at[pl.ds(k - 1, 1)],
                send_sem=send.at[k - 1],
                recv_sem=recv.at[k - 1],
                device_id=peer(k),
                device_id_type=MESH,
            )
            copy.start()
            copies.append(copy)
        got[pl.ds(n - 1, 1)] = total
        for copy in copies:
            copy.wait_recv()
        total = jnp.sum(got[...], axis=0, keepdims=True)
        sent += copies
    cells = nx * ex * ny * ey * nz * ez
    square = jnp.sum(jnp.where(first, total, 0.0), axis=1, keepdims=True)
    cost = jnp.sum(jnp.where(first, 0.0, total), axis=1, keepdims=True)
    rms = jnp.sqrt(square / cells + 1e-06)
    tot_ref[...] = jnp.where(lane == 0, jnp.broadcast_to(cost / cells, (ey, ez)), jnp.broadcast_to(rms, (ey, ez)))
    for t in (1, 0):
        for i in live:
            ok, copy = hop(i, t)
            pl.when(ok)(copy.wait_send)
    for copy in sent:
        copy.wait_send()


def near(sizes, cells):
    nx, ny, nz = sizes
    return ny == 2 and nz == 2 and nx * ny * nz <= 64 and cells[0] == cells[1]


def rounds(nx):
    return max((nx - 1) // 2, 0)


def fast_kernel(
    sizes,
    adj_hbm,
    fwd_hbm,
    des_hbm,
    sol_hbm,
    kind_hbm,
    out_ref,
    sens_ref,
    tot_ref,
    adj,
    fwd,
    des,
    marks,
    mid,
    xs,
    ys,
    zs,
    xr,
    yr,
    zr,
    er,
    part,
    got,
    load_sem,
    send_sem,
    side_sem,
    face_sem,
    sum_sem,
    round_sem,
):
    ex, ey, ez = des.shape
    nx, ny, nz = sizes
    mx, my, mz = (lax.axis_index(name) for name in AXES)
    oy, oz = 1 - my, 1 - mz
    has = {1: mx < nx - 1, -1: mx > 0}
    far = {2: mx < nx - 2, -2: mx > 1}

    loads = [
        pltpu.make_async_copy(adj_hbm, adj, load_sem.at[0]),
        pltpu.make_async_copy(fwd_hbm, fwd, load_sem.at[1]),
        pltpu.make_async_copy(des_hbm, des, load_sem.at[2]),
        pltpu.make_async_copy(sol_hbm, marks.at[0], load_sem.at[3]),
        pltpu.make_async_copy(kind_hbm, marks.at[1], load_sem.at[3]),
    ]
    loads[0].start()

    barrier = pltpu.get_barrier_semaphore()

    def greet(x, y, z):
        pl.semaphore_signal(
            barrier, inc=1, device_id={"gx": x, "gy": y, "gz": z}, device_id_type=MESH
        )

    for s in (1, -1):

        @pl.when(has[s])
        def _():
            for y, z in ((my, oz), (oy, oz), (oy, mz), (my, mz)):
                greet(mx + s, y, z)

    for y, z in ((my, oz), (oy, oz), (oy, mz)):
        greet(mx, y, z)
    for s in (2, -2):

        @pl.when(far[s])
        def _():
            greet(mx + s, my, mz)

    far_count = far[2].astype(jnp.int32) + far[-2].astype(jnp.int32)
    count = 3 + 4 * (has[1].astype(jnp.int32) + has[-1].astype(jnp.int32)) + far_count
    for load in loads[1:]:
        load.start()

    def tell(j):
        for s in (2, -2):

            @pl.when(far[s])
            def _():
                pl.semaphore_signal(
                    round_sem.at[j],
                    inc=1,
                    device_id={"gx": mx + s, "gy": my, "gz": mz},
                    device_id_type=MESH,
                )

    def hear(j):
        pl.semaphore_wait(round_sem.at[j], far_count)

    def relay(j):
        if j < rounds(nx):
            if j > 0:
                hear(j - 1)
            tell(j)

    def clear(ref):
        ref[...] = jnp.zeros(ref.shape, jnp.float32)

    for t in (0, 1):
        clear(yr.at[t, oy])
        clear(zr.at[t, oz])
        clear(er.at[t, oy, mz])
        clear(er.at[t, my, oz])
        clear(er.at[t, oy, oz])
    for s in (1, -1):

        @pl.when(jnp.logical_not(has[s]))
        def _():
            clear(xr.at[side(s)])

    lane = lax.broadcasted_iota(jnp.int32, (ey, ez), 1)
    row = lax.broadcasted_iota(jnp.int32, (ey, ez), 0)
    low_z = jnp.broadcast_to(mz == 1, (ey, ez))
    slot_lane = jnp.where(low_z, lane, jnp.where(lane == ez - 1, 0, lane + 1))
    match_y = [jnp.broadcast_to(my == h, (1, ez)) for h in (0, 1)]
    match_z = [jnp.broadcast_to(mz == h, (ey, ez)) for h in (0, 1)]

    def push(src, dst, sent, came, x, y, z):
        return pltpu.make_async_remote_copy(
            src_ref=src,
            dst_ref=dst,
            send_sem=sent,
            recv_sem=came,
            device_id={"gx": x, "gy": y, "gz": z},
            device_id_type=MESH,
        )

    def x_sends(t, s):
        h = side(s)
        sent, came = send_sem.at[h], face_sem.at[h, t]
        slot = 1 + oy if s == 1 else 2 - oy
        return [
            push(zs.at[t], xr.at[h, t, 6], sent, came, mx - s, my, oz),
            push(xs.at[t, h], xr.at[h, t, pl.ds(0, 5)], sent, came, mx - s, my, mz),
            push(ys.at[t, oy, slot], xr.at[h, t, 5], sent, came, mx - s, oy, mz),
        ]

    def side_sends(t):
        sent = send_sem.at[2]
        return [
            push(zs.at[t], er.at[t, oy, oz], sent, side_sem.at[2, t], mx, oy, oz),
            push(zs.at[t], zr.at[t, oz], sent, side_sem.at[1, t], mx, my, oz),
            push(ys.at[t, oy], yr.at[t, oy], sent, side_sem.at[0, t], mx, oy, mz),
        ]

    def pack_layer(t, x, tiles, pack):
        for sign in (1, -1):
            h = side(sign)
            if x == (0 if sign == 1 else ex - 1):
                for k, i in enumerate(group(0, sign)):
                    xs[t, h, k] = tiles(i)
            edge = 0 if sign == 1 else ey - 1
            for k, i in enumerate(group(1, sign)):
                ys[t, h, k, x : x + 1, :] = tiles(i)[edge : edge + 1, :]
        for k, (i, j) in enumerate(zip(group(2, 1), group(2, -1))):
            at = k * ex + x
            moved = jnp.where(low_z, tiles(i), tiles(j))
            if at % ez:
                moved = pltpu.roll(moved, at % ez, 1)
            pack = jnp.where(slot_lane == at, moved, pack)
        return pack

    def send_all(t, pack):
        zs[t] = pack
        for s in (1, -1):

            @pl.when(has[-s])
            def _():
                for copy in x_sends(t, s):
                    copy.start()

        for copy in side_sends(t):
            copy.start()

    def receive_sides(t):
        for copy in side_sends(t)[::-1]:
            copy.wait_recv()

    def receive_face(t, s):
        h = side(s)
        ref = xr.at[h, t]
        copy = push(ref, ref, send_sem.at[h], face_sem.at[h, t], mx, my, mz)
        pl.when(has[s])(copy.wait_recv)

    def shifted_columns(t):
        moved = {}
        for i in range(15, 19):
            cy, cz = LAT[i][1], LAT[i][2]
            pack = zr[t, side(cz)]
            src, last = (0, ey - 1) if cy == 1 else (ey - 1, 0)
            corner = er[t, side(cy), side(cz), src : src + 1, :]
            pack = pltpu.roll(pack, (-cy) % ey, 0)
            moved[i] = jnp.where(row == last, corner, pack)
        return moved

    def pulled_tile(source, t, i, x, moved):
        cx, cy, cz = LAT[i]
        at = x + cx
        inside = 0 <= at < ex
        tile = source[i, at] if inside else xr[side(cx), t, SLOT[0][i]]
        src = 0 if cx == 1 else ex - 1
        if cy:
            h = side(cy)
            if inside:
                fill = yr[t, h, SLOT[1][i], at : at + 1, :]
            else:
                fill = jnp.where(match_y[h], xr[side(cx), t, 5, src : src + 1, :], 0.0)
            last = ey - 1 if cy == 1 else 0
            tile = jnp.where(row == last, fill, pltpu.roll(tile, (-cy) % ey, 0))
        if cz:
            h = side(cz)
            col = SLOT[2][i] * ex - h
            if cy:
                pack, col = moved[i], col + x
            elif inside:
                pack, col = zr[t, h], col + at
            else:
                pack = jnp.where(match_z[h], xr[side(cx), t, 6], 0.0)
                col = col + src
            last = ez - 1 if cz == 1 else 0
            if (last - col) % ez:
                pack = pltpu.roll(pack, (last - col) % ez, 1)
            tile = jnp.where(lane == last, pack, pltpu.roll(tile, (-cz) % ez, 1))
        return tile

    whole_x = nx * ex
    zero = jnp.zeros((ey, ez), jnp.float32)

    def step(t, source, target, pack):
        cost_sum, square_sum = zero, zero
        with jax.named_scope(f"sides {t}"):
            receive_sides(t)
        if t == 1:
            relay(1)
        moved = shifted_columns(t)
        for x in sorted(range(ex), key=lambda x: x in (0, ex - 1)):
            with jax.named_scope(f"faces {t}"):
                if x == 0:
                    receive_face(t, -1)
                if x == ex - 1:
                    receive_face(t, 1)
            g = des[x]
            solid = marks[0, x] == 1
            fluid = jnp.where(solid, 0.0, 1.0)
            kind = marks[1, x]
            inlet, outlet = kind == 1, kind == 2
            inner = jnp.logical_not(jnp.logical_or(inlet, outlet))
            below = 1.0 / (0.5 + 0.6 * g)
            damping = (0.1 + g) * below
            slope = 0.44 * (below * below)
            place = (mx * ex + x).astype(jnp.float32)
            weight = 1.0 + 2.0 * place / (whole_x - 1)
            f = [fwd[t, i, x] for i in range(19)]
            p = [pulled_tile(source, t, i, x, moved) for i in range(19)]
            out, sens, cost = cell_adjoint(
                f, p, damping, slope, fluid, solid, inner, inlet, outlet, weight
            )
            for i in range(19):
                target[i, x] = out[i]
            cost_sum = cost_sum + cost
            if t == 1:
                sens_ref[x] = sens
                pack = pack_layer(0, x, lambda i: out[i], pack)
            else:
                sens = sens + sens_ref[x]
                sens_ref[x] = sens
                square_sum = square_sum + sens * sens
        return cost_sum, square_sum, pack

    with jax.named_scope("load"):
        loads[0].wait()
    pack = zero
    for x in range(ex):
        pack = pack_layer(1, x, lambda i: adj[i, x], pack)
    with jax.named_scope("greeted"):
        pl.semaphore_wait(barrier, count)
    with jax.named_scope("send 1"):
        send_all(1, pack)
        relay(0)
    for load in loads[1:3]:
        load.wait()
    pltpu.make_async_copy(marks, marks, load_sem.at[3]).wait()
    cost_one, _, pack = step(1, adj, mid, zero)
    with jax.named_scope("send 0"):
        send_all(0, pack)
    for j in range(2, rounds(nx)):
        relay(j)
    cost_two, square, _ = step(0, mid, out_ref, None)
    part[0:1, :] = jnp.sum(square, axis=0, keepdims=True)
    part[1:2, :] = jnp.sum(cost_one + cost_two, axis=0, keepdims=True)

    with jax.named_scope("heard"):
        if rounds(nx):
            hear(rounds(nx) - 1)
    n = nx * ny * nz
    with jax.named_scope("send sums"):
        for dx in sorted(range(nx), key=lambda d: (d == 0, min(d, nx - d))):
            px = jnp.where(mx + dx >= nx, mx + dx - nx, mx + dx)
            for dy, dz in ((1, 1), (0, 1), (1, 0), (0, 0)):
                k = (dx * ny + dy) * nz + dz
                if k == 0:
                    continue
                y, z = (oy if dy else my), (oz if dz else mz)
                push(part, got.at[k - 1], sum_sem.at[0], sum_sem.at[1], px, y, z).start()
    got[n - 1] = part[...]
    every = got.at[pl.ds(0, n - 1)]
    sums = push(every, every, sum_sem.at[0], sum_sem.at[1], mx, my, mz)
    with jax.named_scope("sums"):
        sums.wait_recv()
    total = jnp.sum(jnp.sum(got[...], axis=0), axis=1, keepdims=True)
    cells = nx * ex * ny * ey * nz * ez
    rms = jnp.broadcast_to(jnp.sqrt(total[0:1] / cells + 1e-06), (ey, ez))
    cost = jnp.broadcast_to(total[1:2] / cells, (ey, ez))
    tot_ref[...] = jnp.where(lane == 0, cost, rms)
    with jax.named_scope("drain"):
        for s in (1, -1):
            h = side(s)
            copy = push(xr.at[h], xr.at[h], send_sem.at[h], sum_sem.at[1], mx, my, mz)
            pl.when(has[-s])(copy.wait_send)
        push(xr.at[0], xr.at[0], send_sem.at[2], sum_sem.at[1], mx, my, mz).wait_send()
        sums.wait_send()


def hand_on(adj_in, sens_in, tot_in, adj_out, sens_out, obj_out, rms_out, sens, obj, rms, sem):
    moves = [(adj_in, adj_out), (sens, sens_out), (obj, obj_out), (rms, rms_out)]
    copies = [pltpu.make_async_copy(a, b, sem.at[k]) for k, (a, b) in enumerate(moves)]
    copies[0].start()
    scale = jnp.broadcast_to(1.0 / tot_in[0:1, 1:2], tot_in.shape)
    for x in range(sens.shape[0]):
        sens[x] = sens_in[x] * scale
    copies[1].start()
    obj[0] = tot_in[0, 0]
    rms[0] = tot_in[0, 1]
    copies[2].start()
    copies[3].start()
    for copy in copies:
        copy.wait()


def body(sizes, adjoint_in, forward_states, design, solid_mask, boundary_kind):
    ex, ey, ez = design.shape
    nx, ny, nz = sizes
    any_spec = pl.BlockSpec(memory_space=pltpu.HBM)
    vmem_spec = pl.BlockSpec(memory_space=pltpu.VMEM)
    f32 = jnp.float32
    operands = (adjoint_in, forward_states, design, solid_mask, boundary_kind)
    operands = [pltpu.with_memory_space_constraint(a, pltpu.HBM) for a in operands]
    if near(sizes, design.shape):
        n = nx * ny * nz
        run = fast_kernel
        scratch = [
            pltpu.VMEM(adjoint_in.shape, f32),
            pltpu.VMEM(forward_states.shape, f32),
            pltpu.VMEM(design.shape, f32),
            pltpu.VMEM((2, *design.shape), jnp.int32),
            pltpu.VMEM(adjoint_in.shape, f32),
            pltpu.VMEM((2, 2, 5, ey, ez), f32),
            pltpu.VMEM((2, 2, 5, ex, ez), f32),
            pltpu.VMEM((2, ey, ez), f32),
            pltpu.VMEM((2, 2, 7, ey, ez), f32),
            pltpu.VMEM((2, 2, 5, ex, ez), f32),
            pltpu.VMEM((2, 2, ey, ez), f32),
            pltpu.VMEM((2, 2, 2, ey, ez), f32),
            pltpu.VMEM((2, ez), f32),
            pltpu.VMEM((n, 2, ez), f32),
            pltpu.SemaphoreType.DMA((4,)),
            pltpu.SemaphoreType.DMA((3,)),
            pltpu.SemaphoreType.DMA((3, 2)),
            pltpu.SemaphoreType.DMA((2, 2)),
            pltpu.SemaphoreType.DMA((2,)),
            pltpu.SemaphoreType.REGULAR((max(rounds(nx), 1),)),
        ]
    else:
        run = general_kernel
        sum_scratch = []
        for n in sum_groups(sizes):
            sum_scratch += [
                pltpu.VMEM((1, ez), f32),
                pltpu.VMEM((n, ez), f32),
                pltpu.SemaphoreType.DMA((max(n - 1, 1),)),
                pltpu.SemaphoreType.DMA((max(n - 1, 1),)),
            ]
        scratch = [
            pltpu.VMEM(adjoint_in.shape, f32),
            pltpu.VMEM(forward_states.shape, f32),
            pltpu.VMEM(design.shape, f32),
            pltpu.VMEM(design.shape, jnp.int32),
            pltpu.VMEM(design.shape, jnp.int32),
            pltpu.VMEM(adjoint_in.shape, f32),
            pltpu.VMEM((2, 2, 5, ey, ez), f32),
            pltpu.VMEM((2, 2, 5, ex, ez), f32),
            pltpu.VMEM((2, 2, ey, ez), f32),
            pltpu.VMEM((2, 2, 5, ey, ez), f32),
            pltpu.VMEM((2, 2, 5, ex, ez), f32),
            pltpu.VMEM((2, 2, ey, ez), f32),
            pltpu.VMEM((2, 12, ey, ez), f32),
            pltpu.SemaphoreType.DMA((6,)),
            pltpu.SemaphoreType.DMA,
            pltpu.SemaphoreType.DMA((2, 18)),
            pltpu.SemaphoreType.DMA((2, 18)),
            *sum_scratch,
        ]
    adjoint, sens, tot = pl.pallas_call(
        functools.partial(run, sizes),
        out_shape=(
            jax.ShapeDtypeStruct(adjoint_in.shape, f32),
            jax.ShapeDtypeStruct(design.shape, f32),
            jax.ShapeDtypeStruct((ey, ez), f32),
        ),
        in_specs=[any_spec] * 5,
        out_specs=(vmem_spec, vmem_spec, vmem_spec),
        scratch_shapes=scratch,
        compiler_params=pltpu.CompilerParams(
            collective_id=0, has_side_effects=True, vmem_limit_bytes=VMEM_LIMIT
        ),
    )(*operands)
    adjoint, sens, objective, rms = pl.pallas_call(
        hand_on,
        out_shape=(
            jax.ShapeDtypeStruct(adjoint_in.shape, f32),
            jax.ShapeDtypeStruct(design.shape, f32),
            jax.ShapeDtypeStruct((1,), f32),
            jax.ShapeDtypeStruct((1,), f32),
        ),
        in_specs=[vmem_spec] * 3,
        out_specs=(any_spec, any_spec, any_spec, any_spec),
        scratch_shapes=[
            pltpu.VMEM(design.shape, f32),
            pltpu.SMEM((1,), f32),
            pltpu.SMEM((1,), f32),
            pltpu.SemaphoreType.DMA((4,)),
        ],
        compiler_params=pltpu.CompilerParams(vmem_limit_bytes=VMEM_LIMIT),
    )(adjoint, sens, tot)
    return adjoint, sens, objective.reshape(()), rms.reshape(())


def solution(mesh):
    placed = (
        P(None, "gx", "gy", "gz"),
        P(None, None, "gx", "gy", "gz"),
        P("gx", "gy", "gz"),
        P("gx", "gy", "gz"),
        P("gx", "gy", "gz"),
    )
    return jax.shard_map(
        functools.partial(body, tuple(int(mesh.shape[name]) for name in AXES)),
        mesh=mesh,
        in_specs=placed,
        out_specs=(P(None, "gx", "gy", "gz"), P("gx", "gy", "gz"), P(), P()),
        check_vma=False,
    )
```

```python
import functools

import jax
import jax.numpy as jnp
import numpy as np
from jax import lax
from jax.experimental import pallas as pl
from jax.experimental.pallas import tpu as pltpu
from jax.sharding import PartitionSpec as P

MESH = pl.DeviceIdType.MESH
lattice_table = np.array(
    [
        [0, 0, 0],
        [1, 0, 0],
        [-1, 0, 0],
        [0, 1, 0],
        [0, -1, 0],
        [0, 0, 1],
        [0, 0, -1],
        [1, 1, 0],
        [-1, -1, 0],
        [1, -1, 0],
        [-1, 1, 0],
        [1, 0, 1],
        [-1, 0, -1],
        [1, 0, -1],
        [-1, 0, 1],
        [0, 1, 1],
        [0, -1, -1],
        [0, 1, -1],
        [0, -1, 1],
    ],
    dtype=np.int32,
)
LAT = [tuple(int(v) for v in row) for row in lattice_table]
WEIGHTS = np.array([1.0 / 3] + [1.0 / 18] * 6 + [1.0 / 36] * 12, dtype=np.float64)
opposite_index = [0, 2, 1, 4, 3, 6, 5, 8, 7, 10, 9, 12, 11, 14, 13, 16, 15, 18, 17]
inflow_speed = 0.08
AXES = ("gx", "gy", "gz")
VMEM_LIMIT = 16000 * 1024


def moment_rows():
    c = lattice_table.astype(np.float64)
    cx, cy, cz = c[:, 0], c[:, 1], c[:, 2]
    csq = cx * cx + cy * cy + cz * cz
    return np.stack(
        [
            np.ones(19),
            19 * csq - 30,
            (21 * csq * csq - 53 * csq + 24) / 2,
            cx,
            (5 * csq - 9) * cx,
            cy,
            (5 * csq - 9) * cy,
            cz,
            (5 * csq - 9) * cz,
            3 * cx * cx - csq,
            (3 * csq - 5) * (3 * cx * cx - csq),
            cy * cy - cz * cz,
            (3 * csq - 5) * (cy * cy - cz * cz),
            cx * cy,
            cy * cz,
            cx * cz,
            (cy * cy - cz * cz) * cx,
            (cz * cz - cx * cx) * cy,
            (cx * cx - cy * cy) * cz,
        ]
    )


ROWS = moment_rows()
NORMS = np.sum(ROWS * ROWS, axis=1)
SHEAR = 1.0 / 0.6
RATES = [0, 1.19, 1.4, 0, 1.2, 0, 1.2, 0, 1.2, SHEAR, 1.4, SHEAR, 1.4, SHEAR, SHEAR, SHEAR]
RATES = np.array(RATES + [1.98, 1.98, 1.98], dtype=np.float64)


def weighted_rows():
    c = lattice_table.astype(np.float64)
    pairs = [(0, 0), (1, 1), (2, 2), (0, 1), (1, 2), (0, 2)]
    rows = [WEIGHTS] + [WEIGHTS * c[:, a] for a in range(3)]
    rows += [WEIGHTS * c[:, a] * c[:, b] for a, b in pairs]
    out = np.stack(rows) @ (ROWS / NORMS[:, None]).T
    out[np.abs(out) < 1e-12] = 0.0
    return out


WROWS = weighted_rows()


def group(column, sign):
    return [i for i in range(19) if LAT[i][column] == sign]


SLOT = [{i: k for s in (1, -1) for k, i in enumerate(group(col, s))} for col in range(3)]


def side(sign):
    return 0 if sign == 1 else 1


def combine(coefs, terms):
    total = None
    for coef, term in zip(coefs, terms):
        if coef == 0.0:
            continue
        part = term if coef == 1.0 else float(np.float32(coef)) * term
        total = part if total is None else total + part
    return total


def flux_sums(f):
    s = {i: f[i] + f[i + 1] for i in range(1, 19, 2)}
    d = {i: f[i] - f[i + 1] for i in range(1, 19, 2)}
    return s, d


def moments(p):
    s, d = flux_sums(p)
    sxy, sxz, syz = s[7] + s[9], s[11] + s[13], s[15] + s[17]
    axis_yz = s[3] + s[5]
    axis = s[1] + axis_yz
    exy = sxy + sxz
    edge = exy + syz
    m = [None] * 19
    m[0] = p[0] + axis + edge
    m[1] = 8.0 * edge - 11.0 * axis - 30.0 * p[0]
    m[2] = edge - 4.0 * axis + 12.0 * p[0]
    a = 2.0 * s[1] - axis_yz
    b = exy - 2.0 * syz
    m[9] = a + b
    m[10] = b - 2.0 * a
    a = s[3] - s[5]
    b = sxy - sxz
    m[11] = a + b
    m[12] = b - 2.0 * a
    m[13] = s[7] - s[9]
    m[14] = s[15] - s[17]
    m[15] = s[11] - s[13]
    xa, xb = d[7] + d[9], d[11] + d[13]
    ya, yb = d[7] - d[9], d[15] + d[17]
    za, zb = d[11] - d[13], d[15] - d[17]
    for k, axis_d, u, v in ((3, d[1], xa, xb), (5, d[3], ya, yb), (7, d[5], za, zb)):
        e = u + v
        m[k] = axis_d + e
        m[k + 1] = e - 4.0 * axis_d
    m[16] = xa - xb
    m[17] = yb - ya
    m[18] = za - zb
    return m


def rebuild(z):
    out = [None] * 19
    out[0] = z[0] - 30.0 * z[1] + 12.0 * z[2]
    axis = z[0] - 11.0 * z[1] - 4.0 * z[2]
    edge = z[0] + 8.0 * z[1] + z[2]
    px = z[9] - 2.0 * z[10]
    pw = z[11] - 2.0 * z[12]
    qx = z[9] + z[10]
    qw = z[11] + z[12]
    ayz = axis - px
    eyz = edge - 2.0 * qx
    exx = edge + qx
    exy, exz = exx + qw, exx - qw
    jx, jy, jz = z[3] + z[4], z[5] + z[6], z[7] + z[8]
    x1, x2 = jx + z[16], jx - z[16]
    y1, y2 = jy - z[17], jy + z[17]
    z1, z2 = jz + z[18], jz - z[18]
    even = {
        1: axis + 2.0 * px,
        3: ayz + pw,
        5: ayz - pw,
        7: exy + z[13],
        9: exy - z[13],
        11: exz + z[15],
        13: exz - z[15],
        15: eyz + z[14],
        17: eyz - z[14],
    }
    odd = {
        1: z[3] - 4.0 * z[4],
        3: z[5] - 4.0 * z[6],
        5: z[7] - 4.0 * z[8],
        7: x1 + y1,
        9: x1 - y1,
        11: x2 + z1,
        13: x2 - z1,
        15: y2 + z2,
        17: y2 - z2,
    }
    for i in even:
        out[i] = even[i] + odd[i]
        out[i + 1] = even[i] - odd[i]
    return out


def cell_adjoint(f, p, damping, slope, fluid, solid, inner, inlet, outlet, weight):
    s, d = flux_sums(f)
    rho = f[0]
    for i in s:
        rho = rho + s[i]
    fx = d[1] + (d[7] + d[9]) + (d[11] + d[13])
    fy = d[3] + (d[7] - d[9]) + (d[15] + d[17])
    fz = d[5] + (d[11] - d[13]) + (d[15] - d[17])
    inv = 1.0 / rho
    bx, by, bz = fx * inv, fy * inv, fz * inv
    ux, uy, uz = bx * damping, by * damping, bz * damping
    uu = ux * ux + uy * uy + uz * uz
    m = moments(p)
    n = [None] * 19
    for k in range(16):
        rate = float(np.float32(RATES[k]))
        n[k] = m[k] * jnp.where(inner, rate, 1.0) if np.any(WROWS[:, k]) else None
    s0, sx, sy, sz, xx, yy, zz, xy, yz, xz = [
        combine(WROWS[r, :16], n) for r in range(10)
    ]
    vx = jnp.where(inlet, inflow_speed, ux)
    vy = jnp.where(inlet, 0.0, uy)
    vz = jnp.where(inlet, 0.0, uz)
    gx = xx * vx + xy * vy + xz * vz
    gy = xy * vx + yy * vy + yz * vz
    gz = xz * vx + yz * vy + zz * vz
    vv = vx * vx + vy * vy + vz * vz
    rho_bar = (
        s0 * (1.0 - 1.5 * vv)
        + 3.0 * (sx * vx + sy * vy + sz * vz)
        + 4.5 * (gx * vx + gy * vy + gz * vz)
    )
    rho_bar = jnp.where(outlet, 0.0, rho_bar) + (0.5 * weight) * uu
    scale = jnp.where(inlet, 0.0, jnp.where(outlet, 1.0, rho))
    wr = weight * rho
    ux_bar = scale * (3.0 * sx + 9.0 * gx - 3.0 * s0 * vx) + wr * ux
    uy_bar = scale * (3.0 * sy + 9.0 * gy - 3.0 * s0 * vy) + wr * uy
    uz_bar = scale * (3.0 * sz + 9.0 * gz - 3.0 * s0 * vz) + wr * uz
    d_bar = ux_bar * bx + uy_bar * by + uz_bar * bz
    di = damping * inv
    rho_bar = rho_bar - d_bar * di
    z = [None] * 19
    for k in range(19):
        coef = (1.0 - RATES[k]) / NORMS[k]
        z[k] = jnp.where(inner, float(np.float32(coef)) * m[k], 0.0)
    z[0] = z[0] + rho_bar
    z[3] = z[3] + ux_bar * di
    z[5] = z[5] + uy_bar * di
    z[7] = z[7] + uz_bar * di
    out = rebuild(z)
    out = [jnp.where(solid, p[opposite_index[i]], out[i]) for i in range(19)]
    sens = fluid * (d_bar * slope)
    cost = fluid * (0.5 * wr * uu)
    return out, sens, cost


def sum_groups(sizes):
    nx, ny, nz = sizes
    return [nx * ny * nz] if nx * ny * nz <= 64 else [nx, ny * nz]


def general_kernel(
    sizes,
    adj_hbm,
    fwd_hbm,
    des_hbm,
    sol_hbm,
    kind_hbm,
    out_ref,
    sens_ref,
    tot_ref,
    adj,
    fwd,
    des,
    sol,
    kin,
    mid,
    xs,
    ys,
    zs,
    xr,
    yr,
    zr,
    er,
    load_sem,
    store_sem,
    send_sem,
    recv_sem,
    *sum_refs,
):
    ex, ey, ez = des.shape
    me = tuple(lax.axis_index(name) for name in AXES)
    nx, ny, nz = sizes

    loads = [
        pltpu.make_async_copy(adj_hbm, adj, load_sem.at[0]),
        pltpu.make_async_copy(fwd_hbm.at[1], fwd.at[1], load_sem.at[1]),
        pltpu.make_async_copy(des_hbm, des, load_sem.at[2]),
        pltpu.make_async_copy(sol_hbm, sol, load_sem.at[3]),
        pltpu.make_async_copy(kind_hbm, kin, load_sem.at[4]),
        pltpu.make_async_copy(fwd_hbm.at[0], fwd.at[0], load_sem.at[5]),
    ]
    for load in loads:
        load.start()

    def reach(offset, sign):
        ok = None
        where = {}
        for a in range(3):
            c = sign * offset[a]
            where[AXES[a]] = me[a] + c if c else me[a]
            if c == 1:
                test = me[a] < sizes[a] - 1
            elif c == -1:
                test = me[a] > 0
            else:
                continue
            ok = test if ok is None else jnp.logical_and(ok, test)
        return ok, where

    live = [
        i
        for i in range(1, 19)
        if all(sizes[a] > 1 or LAT[i][a] == 0 for a in range(3))
    ]

    def all_peer(k):
        rank = lax.rem((me[0] * ny + me[1]) * nz + me[2] + k, nx * ny * nz)
        return {
            "gx": rank // (ny * nz),
            "gy": lax.rem(rank // nz, ny),
            "gz": lax.rem(rank, nz),
        }

    def x_peer(k):
        return {"gx": lax.rem(me[0] + k, nx), "gy": me[1], "gz": me[2]}

    def yz_peer(k):
        rank = lax.rem(me[1] * nz + me[2] + k, ny * nz)
        return {"gx": me[0], "gy": rank // nz, "gz": lax.rem(rank, nz)}

    if len(sum_groups(sizes)) == 1:
        peers = [all_peer]
    else:
        peers = [x_peer, yz_peer]

    barrier = pltpu.get_barrier_semaphore()
    count = jnp.int32(sum(n - 1 for n in sum_groups(sizes)))
    for n, peer in zip(sum_groups(sizes), peers):
        for k in range(1, n):
            pl.semaphore_signal(barrier, inc=1, device_id=peer(k), device_id_type=MESH)
    if len(peers) > 1:
        for i in live:
            ok, where = reach(LAT[i], -1)

            @pl.when(ok)
            def _():
                pl.semaphore_signal(barrier, inc=1, device_id=where, device_id_type=MESH)

            count = count + reach(LAT[i], 1)[0].astype(jnp.int32)

    def landing(i, t):
        if i < 3:
            return xr.at[t, i - 1]
        if i < 5:
            return yr.at[t, i - 3]
        if i < 7:
            return zr.at[t, i - 5]
        return er.at[t, i - 7]

    def leaving(i, t):
        c = LAT[i]
        if i < 3:
            return xs.at[t, i - 1]
        if i < 5:
            return ys.at[t, i - 3]
        if i < 7:
            return zs.at[t, i - 5]
        if c[2] == 0:
            return ys.at[t, side(c[1]), SLOT[1][i]]
        return zs.at[t, side(c[2])]

    for i in range(1, 19):
        if i in live:

            @pl.when(jnp.logical_not(reach(LAT[i], 1)[0]))
            def _():
                for t in (0, 1):
                    ref = landing(i, t)
                    ref[...] = jnp.zeros(ref.shape, jnp.float32)

        else:
            for t in (0, 1):
                ref = landing(i, t)
                ref[...] = jnp.zeros(ref.shape, jnp.float32)

    lane = lax.broadcasted_iota(jnp.int32, (ey, ez), 1)
    row = lax.broadcasted_iota(jnp.int32, (ey, ez), 0)

    def hop(i, t):
        ok, where = reach(LAT[i], -1)
        copy = pltpu.make_async_remote_copy(
            src_ref=leaving(i, t),
            dst_ref=landing(i, t),
            send_sem=send_sem.at[t, i - 1],
            recv_sem=recv_sem.at[t, i - 1],
            device_id=where,
            device_id_type=MESH,
        )
        return ok, copy

    def pack_layer(t, x, tiles, packs):
        packs = list(packs)
        for sign in (1, -1):
            h = side(sign)
            if x == (0 if sign == 1 else ex - 1):
                for k, i in enumerate(group(0, sign)):
                    xs[t, h, k] = tiles(i)
            edge = 0 if sign == 1 else ey - 1
            for k, i in enumerate(group(1, sign)):
                ys[t, h, k, x : x + 1, :] = tiles(i)[edge : edge + 1, :]
            edge = 0 if sign == 1 else ez - 1
            for k, i in enumerate(group(2, sign)):
                at = k * ex + x
                moved = tiles(i)
                if (at - edge) % ez:
                    moved = pltpu.roll(moved, (at - edge) % ez, 1)
                packs[h] = jnp.where(lane == at, moved, packs[h])
        return tuple(packs)

    def send_all(t, packs):
        zs[t, 0] = packs[0]
        zs[t, 1] = packs[1]
        for i in sorted(live, key=lambda i: (LAT[i][0] == 0, -sum(map(abs, LAT[i])))):
            ok, copy = hop(i, t)
            pl.when(ok)(copy.start)

    def receive(t, along_x):
        for i in live:
            if (LAT[i][0] != 0) == along_x:
                ok = reach(LAT[i], 1)[0]
                pl.when(ok)(hop(i, t)[1].wait_recv)

    def shifted_columns(t):
        moved = {}
        for i in range(15, 19):
            cy, cz = LAT[i][1], LAT[i][2]
            pack = zr[t, side(cz)]
            src, last = (0, ey - 1) if cy == 1 else (ey - 1, 0)
            corner = er[t, i - 7, src : src + 1, :]
            pack = pltpu.roll(pack, (-cy) % ey, 0)
            moved[i] = jnp.where(row == last, corner, pack)
        return moved

    def pulled_tile(source, t, i, x, moved):
        cx, cy, cz = LAT[i]
        at = x + cx
        inside = 0 <= at < ex
        tile = source[i, at] if inside else xr[t, side(cx), SLOT[0][i]]
        if cy:
            h = side(cy)
            if inside:
                fill = yr[t, h, SLOT[1][i], at : at + 1, :]
            else:
                src = 0 if cx == 1 else ex - 1
                fill = er[t, i - 7, src : src + 1, :]
            last = ey - 1 if cy == 1 else 0
            tile = jnp.where(row == last, fill, pltpu.roll(tile, (-cy) % ey, 0))
        if cz:
            h = side(cz)
            col = SLOT[2][i] * ex
            if cy:
                pack, col = moved[i], col + x
            elif inside:
                pack, col = zr[t, h], col + at
            else:
                pack, col = er[t, i - 7], col + (0 if cx == 1 else ex - 1)
            last = ez - 1 if cz == 1 else 0
            if (last - col) % ez:
                pack = pltpu.roll(pack, (last - col) % ez, 1)
            tile = jnp.where(lane == last, pack, pltpu.roll(tile, (-cz) % ez, 1))
        return tile

    whole_x = nx * ex
    zero = jnp.zeros((ey, ez), jnp.float32)

    def step(t, source, target, packs):
        cost_sum, square_sum = zero, zero
        receive(t, False)
        moved = shifted_columns(t)
        for x in list(range(1, ex - 1)) + [0, ex - 1]:
            if x == 0:
                receive(t, True)
            g = des[x]
            solid = sol[x] == 1
            fluid = jnp.where(solid, 0.0, 1.0)
            kind = kin[x]
            inlet, outlet = kind == 1, kind == 2
            inner = jnp.logical_not(jnp.logical_or(inlet, outlet))
            below = 1.0 / (0.5 + 0.6 * g)
            damping = (0.1 + g) * below
            slope = 0.44 * (below * below)
            place = (me[0] * ex + x).astype(jnp.float32)
            weight = 1.0 + 2.0 * place / (whole_x - 1)
            f = [fwd[t, i, x] for i in range(19)]
            p = [pulled_tile(source, t, i, x, moved) for i in range(19)]
            out, sens, cost = cell_adjoint(
                f, p, damping, slope, fluid, solid, inner, inlet, outlet, weight
            )
            for i in range(19):
                target[i, x] = out[i]
            cost_sum = cost_sum + cost
            if t == 1:
                sens_ref[x] = sens
                packs = pack_layer(0, x, lambda i: out[i], packs)
            else:
                sens = sens + sens_ref[x]
                sens_ref[x] = sens
                square_sum = square_sum + sens * sens
        return cost_sum, square_sum, packs

    loads[0].wait()
    packs = (zero, zero)
    for x in range(ex):
        packs = pack_layer(1, x, lambda i: adj[i, x], packs)
    pl.semaphore_wait(barrier, count)
    send_all(1, packs)
    for load in loads[1:]:
        load.wait()
    cost_one, _, packs = step(1, adj, mid, (zero, zero))
    send_all(0, packs)
    cost_two, square, _ = step(0, mid, out_ref, None)

    half = ez // 2
    cost = jnp.sum(cost_one + cost_two, axis=0, keepdims=True)
    square = jnp.sum(square, axis=0, keepdims=True)
    cost = cost + pltpu.roll(cost, half, 1)
    square = square + pltpu.roll(square, half, 1)
    first = lax.broadcasted_iota(jnp.int32, (1, ez), 1) < half
    total = jnp.where(first, square, cost)

    sent = []
    for r, (n, peer) in enumerate(zip(sum_groups(sizes), peers)):
        part, got, send, recv = sum_refs[4 * r : 4 * r + 4]
        if n == 1:
            continue
        part[...] = total
        copies = []
        for k in range(1, n):
            copy = pltpu.make_async_remote_copy(
                src_ref=part,
                dst_ref=got.at[pl.ds(k - 1, 1)],
                send_sem=send.at[k - 1],
                recv_sem=recv.at[k - 1],
                device_id=peer(k),
                device_id_type=MESH,
            )
            copy.start()
            copies.append(copy)
        got[pl.ds(n - 1, 1)] = total
        for copy in copies:
            copy.wait_recv()
        total = jnp.sum(got[...], axis=0, keepdims=True)
        sent += copies
    tot_ref[0, 0:1, :] = jnp.where(first, total, 0.0)
    tot_ref[0, 1:2, :] = jnp.where(first, 0.0, total)
    for t in (1, 0):
        for i in live:
            ok, copy = hop(i, t)
            pl.when(ok)(copy.wait_send)
    for copy in sent:
        copy.wait_send()


def sum_rows():
    trace = (WROWS[4] + WROWS[5] + WROWS[6]) / 3
    along = WROWS[4] - trace
    across = (WROWS[5] - WROWS[6]) / 2
    assert np.allclose(WROWS[5], trace - along / 2 + across)
    rows = [WROWS[0], WROWS[1], WROWS[2], WROWS[3]]
    rows += [3 * trace, 3 * along, 3 * across, 3 * WROWS[7], 3 * WROWS[8], 3 * WROWS[9]]
    out = np.stack(rows)[:, :16]
    out[np.abs(out) < 1e-12] = 0.0
    return out


SUM_ROWS = sum_rows()


def plus(a, b):
    if a is None or b is None:
        return b if a is None else a
    return a + b


def minus(a, b):
    if b is None:
        return a
    return -b if a is None else a - b


def times(c, a):
    return None if a is None else c * a


def some_moments(p):
    s = {i: plus(p[i], p[i + 1]) for i in range(1, 19, 2)}
    d = {i: minus(p[i], p[i + 1]) for i in range(1, 19, 2)}
    sxy, sxz, syz = plus(s[7], s[9]), plus(s[11], s[13]), plus(s[15], s[17])
    axis_yz = plus(s[3], s[5])
    axis = plus(s[1], axis_yz)
    exy = plus(sxy, sxz)
    edge = plus(exy, syz)
    m = [None] * 19
    m[0] = plus(plus(p[0], axis), edge)
    m[1] = minus(minus(times(8.0, edge), times(11.0, axis)), times(30.0, p[0]))
    m[2] = plus(minus(edge, times(4.0, axis)), times(12.0, p[0]))
    a = minus(times(2.0, s[1]), axis_yz)
    b = minus(exy, times(2.0, syz))
    m[9] = plus(a, b)
    m[10] = minus(b, times(2.0, a))
    a = minus(s[3], s[5])
    b = minus(sxy, sxz)
    m[11] = plus(a, b)
    m[12] = minus(b, times(2.0, a))
    m[13] = minus(s[7], s[9])
    m[14] = minus(s[15], s[17])
    m[15] = minus(s[11], s[13])
    xa, xb = plus(d[7], d[9]), plus(d[11], d[13])
    ya, yb = minus(d[7], d[9]), plus(d[15], d[17])
    za, zb = minus(d[11], d[13]), minus(d[15], d[17])
    for k, axis_d, u, v in ((3, d[1], xa, xb), (5, d[3], ya, yb), (7, d[5], za, zb)):
        e = plus(u, v)
        m[k] = plus(axis_d, e)
        m[k + 1] = minus(e, times(4.0, axis_d))
    m[16] = minus(xa, xb)
    m[17] = minus(yb, ya)
    m[18] = minus(za, zb)
    return m


def cell_state(f, g, fluid, inlet, outlet, weight):
    s, d = flux_sums(f)
    rho = f[0]
    for i in s:
        rho = rho + s[i]
    fx = d[1] + (d[7] + d[9]) + (d[11] + d[13])
    fy = d[3] + (d[7] - d[9]) + (d[15] + d[17])
    fz = d[5] + (d[11] - d[13]) + (d[15] - d[17])
    below = 1.0 / (0.5 + 0.6 * g)
    damping = (0.1 + g) * below
    slope = 0.44 * (below * below)
    inv = 1.0 / rho
    b = [fx * inv, fy * inv, fz * inv]
    u = [c * damping for c in b]
    uu = u[0] * u[0] + u[1] * u[1] + u[2] * u[2]
    wr = weight * rho
    v = [jnp.where(inlet, c, a) for a, c in zip(u, (inflow_speed, 0.0, 0.0))]
    scale = jnp.where(inlet, 0.0, jnp.where(outlet, 3.0, 3.0 * rho))
    half = (0.5 * weight) * uu
    state = v + [wr * c for c in u] + b + [scale, damping * inv, half, fluid * slope]
    return state, fluid * (rho * half)


def cell_sums(m, state, inner, outlet):
    vx, vy, vz, wx, wy, wz, bx, by, bz, scale, di, half, slope = state
    n = [None] * 19
    for k in range(16):
        rate = float(np.float32(RATES[k]))
        n[k] = m[k] * jnp.where(inner, rate, 1.0) if np.any(SUM_ROWS[:, k]) else None
    s0, sx, sy, sz, trace, along, across, xy, yz, xz = [combine(r, n) for r in SUM_ROWS]
    xx = trace + along
    side_on = trace - 0.5 * along
    yy, zz = side_on + across, side_on - across
    ax = sx + (xx * vx + xy * vy + xz * vz) - s0 * vx
    ay = sy + (xy * vx + yy * vy + yz * vz) - s0 * vy
    az = sz + (xz * vx + yz * vy + zz * vz) - s0 * vz
    along_v = (ax + sx) * vx + (ay + sy) * vy + (az + sz) * vz
    rho_bar = jnp.where(outlet, 0.0, s0 + 1.5 * along_v) + half
    ux_bar, uy_bar, uz_bar = scale * ax + wx, scale * ay + wy, scale * az + wz
    d_bar = ux_bar * bx + uy_bar * by + uz_bar * bz
    extra = [rho_bar - d_bar * di, ux_bar * di, uy_bar * di, uz_bar * di]
    return extra, d_bar * slope


def cell_out(p, m, extra, inner, solid):
    z = [None] * 19
    for k in range(19):
        coef = float(np.float32((1.0 - RATES[k]) / NORMS[k]))
        z[k] = jnp.where(inner, coef * m[k], 0.0)
    for k, e in zip((0, 3, 5, 7), extra):
        z[k] = z[k] + e
    out = rebuild(z)
    return [jnp.where(solid, p[opposite_index[i]], out[i]) for i in range(19)]


def near(sizes, cells):
    nx, ny, nz = sizes
    ex, ey, _ = cells
    return ny == 2 and nz == 2 and nx * ny * nz <= 64 and ex == ey and ey % 8 == 0


def rounds(nx):
    return max((nx - 1) // 2, 0)


def fast_kernel(
    sizes,
    adj_hbm,
    fwd_hbm,
    des_hbm,
    sol_hbm,
    kind_hbm,
    out_ref,
    sens_ref,
    tot_ref,
    adj,
    fwd,
    des,
    marks,
    mid,
    pre,
    mom,
    xs,
    xe,
    ys,
    zs,
    xr,
    yr,
    zr,
    er,
    part,
    got,
    load_sem,
    send_sem,
    side_sem,
    face_sem,
    sum_sem,
    round_sem,
):
    ex, ey, ez = des.shape
    nx, ny, nz = sizes
    mx, my, mz = (lax.axis_index(name) for name in AXES)
    oy, oz = 1 - my, 1 - mz
    has = {1: mx < nx - 1, -1: mx > 0}
    far = {2: mx < nx - 2, -2: mx > 1}

    loads = [
        pltpu.make_async_copy(adj_hbm, adj, load_sem.at[0]),
        pltpu.make_async_copy(fwd_hbm, fwd, load_sem.at[1]),
        pltpu.make_async_copy(des_hbm, des, load_sem.at[2]),
        pltpu.make_async_copy(sol_hbm, marks.at[0], load_sem.at[2]),
        pltpu.make_async_copy(kind_hbm, marks.at[1], load_sem.at[2]),
    ]
    loads[0].start()

    barrier = pltpu.get_barrier_semaphore()

    def greet(x, y, z):
        pl.semaphore_signal(
            barrier, inc=1, device_id={"gx": x, "gy": y, "gz": z}, device_id_type=MESH
        )

    for s in (1, -1):

        @pl.when(has[s])
        def _():
            for y, z in ((my, oz), (oy, oz), (oy, mz), (my, mz)):
                greet(mx + s, y, z)

    for y, z in ((my, oz), (oy, oz), (oy, mz)):
        greet(mx, y, z)
    for s in (2, -2):

        @pl.when(far[s])
        def _():
            greet(mx + s, my, mz)

    far_count = far[2].astype(jnp.int32) + far[-2].astype(jnp.int32)
    count = 3 + 4 * (has[1].astype(jnp.int32) + has[-1].astype(jnp.int32)) + far_count
    for load in loads[1:]:
        load.start()

    def tell(j):
        for s in (2, -2):

            @pl.when(far[s])
            def _():
                pl.semaphore_signal(
                    round_sem.at[j],
                    inc=1,
                    device_id={"gx": mx + s, "gy": my, "gz": mz},
                    device_id_type=MESH,
                )

    def hear(j):
        pl.semaphore_wait(round_sem.at[j], far_count)

    def relay(j):
        if j < rounds(nx):
            if j > 0:
                hear(j - 1)
            tell(j)

    def clear(ref):
        ref[...] = jnp.zeros(ref.shape, jnp.float32)

    for t in (0, 1):
        clear(yr.at[t, oy])
        clear(zr.at[t, oz])
        clear(er.at[t, oy, mz])
        clear(er.at[t, my, oz])
        clear(er.at[t, oy, oz])
    for s in (1, -1):

        @pl.when(jnp.logical_not(has[s]))
        def _():
            clear(xr.at[side(s)])

    lane = lax.broadcasted_iota(jnp.int32, (ey, ez), 1)
    row = lax.broadcasted_iota(jnp.int32, (ey, ez), 0)
    low_z = jnp.broadcast_to(mz == 1, (ey, ez))
    slot_lane = jnp.where(low_z, lane, jnp.where(lane == ez - 1, 0, lane + 1))
    match_y = [jnp.broadcast_to(my == h, (1, ez)) for h in (0, 1)]
    match_z = [jnp.broadcast_to(mz == h, (ey, ez)) for h in (0, 1)]

    def push(src, dst, sent, came, x, y, z):
        return pltpu.make_async_remote_copy(
            src_ref=src,
            dst_ref=dst,
            send_sem=sent,
            recv_sem=came,
            device_id={"gx": x, "gy": y, "gz": z},
            device_id_type=MESH,
        )

    def x_sends(t, turn):
        h = lax.rem(mx + turn, 2)
        sent, came, at = send_sem.at[h], face_sem.at[h, t], mx - 1 + 2 * h
        face, last = 5 * ey, 6 * ey
        copies = [
            push(zs.at[t], xr.at[h, t, pl.ds(face, ey)], sent, came, at, my, oz),
            push(xs.at[t, h], xr.at[h, t, pl.ds(0, face)], sent, came, at, my, mz),
            push(xe.at[t, h, oy], xr.at[h, t, pl.ds(last, 1)], sent, came, at, oy, mz),
        ]
        return jnp.where(h == 0, mx > 0, mx < nx - 1), copies

    def side_sends(t):
        sent, came = send_sem.at[2], side_sem.at[t]
        return [
            push(zs.at[t], zr.at[t, oz], sent, came, mx, my, oz),
            push(zs.at[t], er.at[t, oy, oz], sent, came, mx, oy, oz),
            push(ys.at[t, oy], yr.at[t, oy], sent, came, mx, oy, mz),
        ]

    def pack_layer(t, x, tiles, pack):
        for sign in (1, -1):
            h = side(sign)
            edge = 0 if sign == 1 else ey - 1
            if x == (0 if sign == 1 else ex - 1):
                for k, i in enumerate(group(0, sign)):
                    xs[t, h, k * ey : (k + 1) * ey, :] = tiles(i)
                    cy = LAT[i][1]
                    if cy:
                        cut = 0 if cy == 1 else ey - 1
                        xe[t, h, side(cy)] = tiles(i)[cut : cut + 1, :]
            for k, i in enumerate(group(1, sign)):
                ys[t, h, k, x : x + 1, :] = tiles(i)[edge : edge + 1, :]
        for k, (i, j) in enumerate(zip(group(2, 1), group(2, -1))):
            at = k * ex + x
            moved = jnp.where(low_z, tiles(i), tiles(j))
            if at % ez:
                moved = pltpu.roll(moved, at % ez, 1)
            pack = jnp.where(slot_lane == at, moved, pack)
        return pack

    def send_all(t, pack):
        zs[t] = pack
        for turn in (0, 1):
            ok, copies = x_sends(t, turn)

            @pl.when(ok)
            def _():
                for copy in copies:
                    copy.start()

        for copy in side_sends(t):
            copy.start()

    def await_bytes(ref, sem):
        pltpu.make_async_copy(ref, ref, sem).wait()

    def receive_sides(t):
        await_bytes(xr.at[0, t], side_sem.at[t])

    def receive_faces(t):
        for s in (-1, 1):
            h = side(s)
            ref = xr.at[h, t, pl.ds(0, 6 * ey + 1)]
            pl.when(has[s])(functools.partial(await_bytes, ref, face_sem.at[h, t]))

    def shifted_columns(t):
        moved = {}
        for i in range(15, 19):
            cy, cz = LAT[i][1], LAT[i][2]
            pack = zr[t, side(cz)]
            src, last = (0, ey - 1) if cy == 1 else (ey - 1, 0)
            corner = er[t, side(cy), side(cz), src : src + 1, :]
            pack = pltpu.roll(pack, (-cy) % ey, 0)
            moved[i] = jnp.where(row == last, corner, pack)
        return moved

    def pulled_tile(source, t, i, x, moved):
        cx, cy, cz = LAT[i]
        at = x + cx
        inside = 0 <= at < ex
        if inside:
            tile = source[i, at]
        else:
            k = SLOT[0][i] * ey
            tile = xr[side(cx), t, k : k + ey, :]
        src = 0 if cx == 1 else ex - 1
        if cy:
            h = side(cy)
            if inside:
                fill = yr[t, h, SLOT[1][i], at : at + 1, :]
            else:
                fill = xr[side(cx), t, 6 * ey : 6 * ey + 1, :]
                fill = jnp.where(match_y[h], fill, 0.0)
            last = ey - 1 if cy == 1 else 0
            tile = jnp.where(row == last, fill, pltpu.roll(tile, (-cy) % ey, 0))
        if cz:
            h = side(cz)
            col = SLOT[2][i] * ex - h
            if cy:
                pack, col = moved[i], col + x
            elif inside:
                pack, col = zr[t, h], col + at
            else:
                pack = xr[side(cx), t, 5 * ey : 6 * ey, :]
                pack = jnp.where(match_z[h], pack, 0.0)
                col = col + src
            last = ez - 1 if cz == 1 else 0
            if (last - col) % ez:
                pack = pltpu.roll(pack, (last - col) % ez, 1)
            tile = jnp.where(lane == last, pack, pltpu.roll(tile, (-cz) % ez, 1))
        return tile

    whole_x = nx * ex
    zero = jnp.zeros((ey, ez), jnp.float32)

    def marked(x):
        kind = marks[1, x]
        return kind == 0, kind == 1, kind == 2, marks[0, x] == 1

    def prepare(t):
        total = zero
        for x in range(ex):
            _, inlet, outlet, solid = marked(x)
            fluid = jnp.where(solid, 0.0, 1.0)
            place = (mx * ex + x).astype(jnp.float32)
            weight = 1.0 + 2.0 * place / (whole_x - 1)
            f = [fwd[t, i, x] for i in range(19)]
            state, cost = cell_state(f, des[x], fluid, inlet, outlet, weight)
            for q, value in enumerate(state):
                pre[q, x] = value
            total = total + cost
        return total

    def is_late(i, x):
        return not 0 <= x + LAT[i][0] < ex

    def sums_of(m, x):
        inner, _, outlet, _ = marked(x)
        return cell_sums(m, [pre[q, x] for q in range(13)], inner, outlet)

    edges = sorted({0, ex - 1})
    inner_planes = range(1, ex - 1)

    def pull(t, source, done):
        receive_sides(t)
        if t == 1:
            relay(1)
        moved = shifted_columns(t)
        for x in inner_planes:
            p = [pulled_tile(source, t, i, x, moved) for i in range(19)]
            done(x, p, some_moments(p))
        early = {}
        for x in edges:
            p = [
                None if is_late(i, x) else pulled_tile(source, t, i, x, moved)
                for i in range(19)
            ]
            early[x] = p, some_moments(p)
        with jax.named_scope(f"faces {t}"):
            receive_faces(t)
        for x in edges:
            p, m = early[x]
            late = [
                pulled_tile(source, t, i, x, moved) if is_late(i, x) else None
                for i in range(19)
            ]
            p = [b if a is None else a for a, b in zip(p, late)]
            done(x, p, [plus(a, b) for a, b in zip(m, some_moments(late))])

    with jax.named_scope("load"):
        loads[0].wait()
    pack = zero
    for x in range(ex):
        pack = pack_layer(1, x, lambda i: adj[i, x], pack)
    with jax.named_scope("greeted"):
        pl.semaphore_wait(barrier, count)
    with jax.named_scope("send 1"):
        send_all(1, pack)
        relay(0)
    loads[1].wait()
    await_bytes(fwd.at[0, pl.ds(0, 3)], load_sem.at[2])
    cost = prepare(1)
    packs = [zero]

    def first_done(x, p, m):
        inner, _, _, solid = marked(x)
        extra, sens = sums_of(m, x)
        out = cell_out(p, m, extra, inner, solid)
        for i in range(19):
            mid[i, x] = out[i]
        sens_ref[x] = sens
        packs[0] = pack_layer(0, x, lambda i: out[i], packs[0])

    with jax.named_scope("step 1"):
        pull(1, adj, first_done)
    with jax.named_scope("send 0"):
        send_all(0, packs[0])
    for j in range(2, rounds(nx)):
        relay(j)
    cost = cost + prepare(0)
    squares = [zero]

    def second_done(x, p, m):
        extra, sens = sums_of(m, x)
        sens = sens + sens_ref[x]
        sens_ref[x] = sens
        squares[0] = squares[0] + sens * sens
        for i in range(19):
            adj[i, x] = p[i]
        for k, value in enumerate(m + extra):
            mom[k, x] = value

    with jax.named_scope("step 0"):
        pull(0, mid, second_done)
    part[0:1, :] = jnp.sum(squares[0], axis=0, keepdims=True)
    part[1:2, :] = jnp.sum(cost, axis=0, keepdims=True)

    with jax.named_scope("heard"):
        if rounds(nx):
            hear(rounds(nx) - 1)
    n = nx * ny * nz
    with jax.named_scope("send sums"):
        for dx in sorted(range(nx), key=lambda d: (d == 0, min(d, nx - d))):
            px = jnp.where(mx + dx >= nx, mx + dx - nx, mx + dx)
            for dy, dz in ((1, 1), (0, 1), (1, 0), (0, 0)):
                k = (dx * ny + dy) * nz + dz
                if k == 0:
                    continue
                y, z = (oy if dy else my), (oz if dz else mz)
                push(part, got.at[k - 1], sum_sem.at[0], sum_sem.at[1], px, y, z).start()
    got[n - 1] = part[...]
    with jax.named_scope("out"):
        for x in range(ex):
            inner, _, _, solid = marked(x)
            m = [mom[k, x] for k in range(23)]
            out = cell_out([adj[i, x] for i in range(19)], m[:19], m[19:], inner, solid)
            for i in range(19):
                out_ref[i, x] = out[i]
    every = got.at[pl.ds(0, n - 1)]
    sums = push(every, every, sum_sem.at[0], sum_sem.at[1], mx, my, mz)
    with jax.named_scope("sums"):
        sums.wait_recv()
    tot_ref[...] = got[...]
    with jax.named_scope("drain"):
        for s in (1, -1):
            h = side(s)
            ref = xr.at[h, :, pl.ds(0, 6 * ey + 1)]
            pl.when(has[-s])(functools.partial(await_bytes, ref, send_sem.at[h]))
        await_bytes(xr.at[0], send_sem.at[2])
        sums.wait_send()


def hand_on(
    cells,
    adj_in,
    sens_in,
    sums_in,
    adj_out,
    sens_out,
    obj_out,
    rms_out,
    sens,
    obj,
    rms,
    sem,
):
    moves = [(adj_in, adj_out), (sens, sens_out), (obj, obj_out), (rms, rms_out)]
    copies = [pltpu.make_async_copy(a, b, sem.at[k]) for k, (a, b) in enumerate(moves)]
    copies[0].start()
    total = jnp.sum(jnp.sum(sums_in[...], axis=0), axis=1, keepdims=True) / cells
    root = jnp.sqrt(total[0:1] + 1e-06)
    scale = jnp.broadcast_to(1.0 / root, sens.shape[1:])
    for x in range(sens.shape[0]):
        sens[x] = sens_in[x] * scale
    copies[1].start()
    obj[0] = total[1, 0]
    rms[0] = root[0, 0]
    copies[2].start()
    copies[3].start()
    for copy in copies:
        copy.wait()


def body(sizes, adjoint_in, forward_states, design, solid_mask, boundary_kind):
    ex, ey, ez = design.shape
    nx, ny, nz = sizes
    any_spec = pl.BlockSpec(memory_space=pltpu.HBM)
    vmem_spec = pl.BlockSpec(memory_space=pltpu.VMEM)
    f32 = jnp.float32
    operands = (adjoint_in, forward_states, design, solid_mask, boundary_kind)
    operands = [pltpu.with_memory_space_constraint(a, pltpu.HBM) for a in operands]
    if near(sizes, design.shape):
        n = nx * ny * nz
        run = fast_kernel
        scratch = [
            pltpu.VMEM(adjoint_in.shape, f32),
            pltpu.VMEM(forward_states.shape, f32),
            pltpu.VMEM(design.shape, f32),
            pltpu.VMEM((2, *design.shape), jnp.int32),
            pltpu.VMEM(adjoint_in.shape, f32),
            pltpu.VMEM((13, *design.shape), f32),
            pltpu.VMEM((23, *design.shape), f32),
            pltpu.VMEM((2, 2, 5 * ey, ez), f32),
            pltpu.VMEM((2, 2, 2, 1, ez), f32),
            pltpu.VMEM((2, 2, 5, ex, ez), f32),
            pltpu.VMEM((2, ey, ez), f32),
            pltpu.VMEM((2, 2, 7 * ey, ez), f32),
            pltpu.VMEM((2, 2, 5, ex, ez), f32),
            pltpu.VMEM((2, 2, ey, ez), f32),
            pltpu.VMEM((2, 2, 2, ey, ez), f32),
            pltpu.VMEM((2, ez), f32),
            pltpu.VMEM((n, 2, ez), f32),
            pltpu.SemaphoreType.DMA((3,)),
            pltpu.SemaphoreType.DMA((3,)),
            pltpu.SemaphoreType.DMA((2,)),
            pltpu.SemaphoreType.DMA((2, 2)),
            pltpu.SemaphoreType.DMA((2,)),
            pltpu.SemaphoreType.REGULAR((max(rounds(nx), 1),)),
        ]
    else:
        n = 1
        run = general_kernel
        sum_scratch = []
        for n in sum_groups(sizes):
            sum_scratch += [
                pltpu.VMEM((1, ez), f32),
                pltpu.VMEM((n, ez), f32),
                pltpu.SemaphoreType.DMA((max(n - 1, 1),)),
                pltpu.SemaphoreType.DMA((max(n - 1, 1),)),
            ]
        scratch = [
            pltpu.VMEM(adjoint_in.shape, f32),
            pltpu.VMEM(forward_states.shape, f32),
            pltpu.VMEM(design.shape, f32),
            pltpu.VMEM(design.shape, jnp.int32),
            pltpu.VMEM(design.shape, jnp.int32),
            pltpu.VMEM(adjoint_in.shape, f32),
            pltpu.VMEM((2, 2, 5, ey, ez), f32),
            pltpu.VMEM((2, 2, 5, ex, ez), f32),
            pltpu.VMEM((2, 2, ey, ez), f32),
            pltpu.VMEM((2, 2, 5, ey, ez), f32),
            pltpu.VMEM((2, 2, 5, ex, ez), f32),
            pltpu.VMEM((2, 2, ey, ez), f32),
            pltpu.VMEM((2, 12, ey, ez), f32),
            pltpu.SemaphoreType.DMA((6,)),
            pltpu.SemaphoreType.DMA,
            pltpu.SemaphoreType.DMA((2, 18)),
            pltpu.SemaphoreType.DMA((2, 18)),
            *sum_scratch,
        ]
    adjoint, sens, tot = pl.pallas_call(
        functools.partial(run, sizes),
        out_shape=(
            jax.ShapeDtypeStruct(adjoint_in.shape, f32),
            jax.ShapeDtypeStruct(design.shape, f32),
            jax.ShapeDtypeStruct((n, 2, ez), f32),
        ),
        in_specs=[any_spec] * 5,
        out_specs=(vmem_spec, vmem_spec, vmem_spec),
        scratch_shapes=scratch,
        compiler_params=pltpu.CompilerParams(
            collective_id=0, has_side_effects=True, vmem_limit_bytes=VMEM_LIMIT
        ),
    )(*operands)
    adjoint, sens, objective, rms = pl.pallas_call(
        functools.partial(hand_on, nx * ex * ny * ey * nz * ez),
        out_shape=(
            jax.ShapeDtypeStruct(adjoint_in.shape, f32),
            jax.ShapeDtypeStruct(design.shape, f32),
            jax.ShapeDtypeStruct((1,), f32),
            jax.ShapeDtypeStruct((1,), f32),
        ),
        in_specs=[vmem_spec] * 3,
        out_specs=(any_spec, any_spec, any_spec, any_spec),
        scratch_shapes=[
            pltpu.VMEM(design.shape, f32),
            pltpu.SMEM((1,), f32),
            pltpu.SMEM((1,), f32),
            pltpu.SemaphoreType.DMA((4,)),
        ],
        compiler_params=pltpu.CompilerParams(vmem_limit_bytes=VMEM_LIMIT),
    )(adjoint, sens, tot)
    return adjoint, sens, objective.reshape(()), rms.reshape(())


def solution(mesh):
    placed = (
        P(None, "gx", "gy", "gz"),
        P(None, None, "gx", "gy", "gz"),
        P("gx", "gy", "gz"),
        P("gx", "gy", "gz"),
        P("gx", "gy", "gz"),
    )
    return jax.shard_map(
        functools.partial(body, tuple(int(mesh.shape[name]) for name in AXES)),
        mesh=mesh,
        in_specs=placed,
        out_specs=(P(None, "gx", "gy", "gz"), P("gx", "gy", "gz"), P(), P()),
        check_vma=False,
    )
```

```python
import functools

import jax
import jax.numpy as jnp
import numpy as np
from jax import lax
from jax.experimental import pallas as pl
from jax.experimental.pallas import tpu as pltpu
from jax.sharding import PartitionSpec as P

MESH = pl.DeviceIdType.MESH
lattice_table = np.array(
    [
        [0, 0, 0],
        [1, 0, 0],
        [-1, 0, 0],
        [0, 1, 0],
        [0, -1, 0],
        [0, 0, 1],
        [0, 0, -1],
        [1, 1, 0],
        [-1, -1, 0],
        [1, -1, 0],
        [-1, 1, 0],
        [1, 0, 1],
        [-1, 0, -1],
        [1, 0, -1],
        [-1, 0, 1],
        [0, 1, 1],
        [0, -1, -1],
        [0, 1, -1],
        [0, -1, 1],
    ],
    dtype=np.int32,
)
LAT = [tuple(int(v) for v in row) for row in lattice_table]
WEIGHTS = np.array([1.0 / 3] + [1.0 / 18] * 6 + [1.0 / 36] * 12, dtype=np.float64)
opposite_index = [0, 2, 1, 4, 3, 6, 5, 8, 7, 10, 9, 12, 11, 14, 13, 16, 15, 18, 17]
inflow_speed = 0.08
AXES = ("gx", "gy", "gz")
VMEM_LIMIT = 16000 * 1024


def moment_rows():
    c = lattice_table.astype(np.float64)
    cx, cy, cz = c[:, 0], c[:, 1], c[:, 2]
    csq = cx * cx + cy * cy + cz * cz
    return np.stack(
        [
            np.ones(19),
            19 * csq - 30,
            (21 * csq * csq - 53 * csq + 24) / 2,
            cx,
            (5 * csq - 9) * cx,
            cy,
            (5 * csq - 9) * cy,
            cz,
            (5 * csq - 9) * cz,
            3 * cx * cx - csq,
            (3 * csq - 5) * (3 * cx * cx - csq),
            cy * cy - cz * cz,
            (3 * csq - 5) * (cy * cy - cz * cz),
            cx * cy,
            cy * cz,
            cx * cz,
            (cy * cy - cz * cz) * cx,
            (cz * cz - cx * cx) * cy,
            (cx * cx - cy * cy) * cz,
        ]
    )


ROWS = moment_rows()
NORMS = np.sum(ROWS * ROWS, axis=1)
SHEAR = 1.0 / 0.6
RATES = [0, 1.19, 1.4, 0, 1.2, 0, 1.2, 0, 1.2, SHEAR, 1.4, SHEAR, 1.4, SHEAR, SHEAR, SHEAR]
RATES = np.array(RATES + [1.98, 1.98, 1.98], dtype=np.float64)


def weighted_rows():
    c = lattice_table.astype(np.float64)
    pairs = [(0, 0), (1, 1), (2, 2), (0, 1), (1, 2), (0, 2)]
    rows = [WEIGHTS] + [WEIGHTS * c[:, a] for a in range(3)]
    rows += [WEIGHTS * c[:, a] * c[:, b] for a, b in pairs]
    out = np.stack(rows) @ (ROWS / NORMS[:, None]).T
    out[np.abs(out) < 1e-12] = 0.0
    return out


WROWS = weighted_rows()


def group(column, sign):
    return [i for i in range(19) if LAT[i][column] == sign]


SLOT = [{i: k for s in (1, -1) for k, i in enumerate(group(col, s))} for col in range(3)]


def side(sign):
    return 0 if sign == 1 else 1


def combine(coefs, terms):
    total = None
    for coef, term in zip(coefs, terms):
        if coef == 0.0:
            continue
        part = term if coef == 1.0 else float(np.float32(coef)) * term
        total = part if total is None else total + part
    return total


def flux_sums(f):
    s = {i: f[i] + f[i + 1] for i in range(1, 19, 2)}
    d = {i: f[i] - f[i + 1] for i in range(1, 19, 2)}
    return s, d


def moments(p):
    s, d = flux_sums(p)
    sxy, sxz, syz = s[7] + s[9], s[11] + s[13], s[15] + s[17]
    axis_yz = s[3] + s[5]
    axis = s[1] + axis_yz
    exy = sxy + sxz
    edge = exy + syz
    m = [None] * 19
    m[0] = p[0] + axis + edge
    m[1] = 8.0 * edge - 11.0 * axis - 30.0 * p[0]
    m[2] = edge - 4.0 * axis + 12.0 * p[0]
    a = 2.0 * s[1] - axis_yz
    b = exy - 2.0 * syz
    m[9] = a + b
    m[10] = b - 2.0 * a
    a = s[3] - s[5]
    b = sxy - sxz
    m[11] = a + b
    m[12] = b - 2.0 * a
    m[13] = s[7] - s[9]
    m[14] = s[15] - s[17]
    m[15] = s[11] - s[13]
    xa, xb = d[7] + d[9], d[11] + d[13]
    ya, yb = d[7] - d[9], d[15] + d[17]
    za, zb = d[11] - d[13], d[15] - d[17]
    for k, axis_d, u, v in ((3, d[1], xa, xb), (5, d[3], ya, yb), (7, d[5], za, zb)):
        e = u + v
        m[k] = axis_d + e
        m[k + 1] = e - 4.0 * axis_d
    m[16] = xa - xb
    m[17] = yb - ya
    m[18] = za - zb
    return m


def rebuild(z):
    out = [None] * 19
    out[0] = z[0] - 30.0 * z[1] + 12.0 * z[2]
    axis = z[0] - 11.0 * z[1] - 4.0 * z[2]
    edge = z[0] + 8.0 * z[1] + z[2]
    px = z[9] - 2.0 * z[10]
    pw = z[11] - 2.0 * z[12]
    qx = z[9] + z[10]
    qw = z[11] + z[12]
    ayz = axis - px
    eyz = edge - 2.0 * qx
    exx = edge + qx
    exy, exz = exx + qw, exx - qw
    jx, jy, jz = z[3] + z[4], z[5] + z[6], z[7] + z[8]
    x1, x2 = jx + z[16], jx - z[16]
    y1, y2 = jy - z[17], jy + z[17]
    z1, z2 = jz + z[18], jz - z[18]
    even = {
        1: axis + 2.0 * px,
        3: ayz + pw,
        5: ayz - pw,
        7: exy + z[13],
        9: exy - z[13],
        11: exz + z[15],
        13: exz - z[15],
        15: eyz + z[14],
        17: eyz - z[14],
    }
    odd = {
        1: z[3] - 4.0 * z[4],
        3: z[5] - 4.0 * z[6],
        5: z[7] - 4.0 * z[8],
        7: x1 + y1,
        9: x1 - y1,
        11: x2 + z1,
        13: x2 - z1,
        15: y2 + z2,
        17: y2 - z2,
    }
    for i in even:
        out[i] = even[i] + odd[i]
        out[i + 1] = even[i] - odd[i]
    return out


def cell_adjoint(f, p, damping, slope, fluid, solid, inner, inlet, outlet, weight):
    s, d = flux_sums(f)
    rho = f[0]
    for i in s:
        rho = rho + s[i]
    fx = d[1] + (d[7] + d[9]) + (d[11] + d[13])
    fy = d[3] + (d[7] - d[9]) + (d[15] + d[17])
    fz = d[5] + (d[11] - d[13]) + (d[15] - d[17])
    inv = 1.0 / rho
    bx, by, bz = fx * inv, fy * inv, fz * inv
    ux, uy, uz = bx * damping, by * damping, bz * damping
    uu = ux * ux + uy * uy + uz * uz
    m = moments(p)
    n = [None] * 19
    for k in range(16):
        rate = float(np.float32(RATES[k]))
        n[k] = m[k] * jnp.where(inner, rate, 1.0) if np.any(WROWS[:, k]) else None
    s0, sx, sy, sz, xx, yy, zz, xy, yz, xz = [
        combine(WROWS[r, :16], n) for r in range(10)
    ]
    vx = jnp.where(inlet, inflow_speed, ux)
    vy = jnp.where(inlet, 0.0, uy)
    vz = jnp.where(inlet, 0.0, uz)
    gx = xx * vx + xy * vy + xz * vz
    gy = xy * vx + yy * vy + yz * vz
    gz = xz * vx + yz * vy + zz * vz
    vv = vx * vx + vy * vy + vz * vz
    rho_bar = (
        s0 * (1.0 - 1.5 * vv)
        + 3.0 * (sx * vx + sy * vy + sz * vz)
        + 4.5 * (gx * vx + gy * vy + gz * vz)
    )
    rho_bar = jnp.where(outlet, 0.0, rho_bar) + (0.5 * weight) * uu
    scale = jnp.where(inlet, 0.0, jnp.where(outlet, 1.0, rho))
    wr = weight * rho
    ux_bar = scale * (3.0 * sx + 9.0 * gx - 3.0 * s0 * vx) + wr * ux
    uy_bar = scale * (3.0 * sy + 9.0 * gy - 3.0 * s0 * vy) + wr * uy
    uz_bar = scale * (3.0 * sz + 9.0 * gz - 3.0 * s0 * vz) + wr * uz
    d_bar = ux_bar * bx + uy_bar * by + uz_bar * bz
    di = damping * inv
    rho_bar = rho_bar - d_bar * di
    z = [None] * 19
    for k in range(19):
        coef = (1.0 - RATES[k]) / NORMS[k]
        z[k] = jnp.where(inner, float(np.float32(coef)) * m[k], 0.0)
    z[0] = z[0] + rho_bar
    z[3] = z[3] + ux_bar * di
    z[5] = z[5] + uy_bar * di
    z[7] = z[7] + uz_bar * di
    out = rebuild(z)
    out = [jnp.where(solid, p[opposite_index[i]], out[i]) for i in range(19)]
    sens = fluid * (d_bar * slope)
    cost = fluid * (0.5 * wr * uu)
    return out, sens, cost


def sum_groups(sizes):
    nx, ny, nz = sizes
    return [nx * ny * nz] if nx * ny * nz <= 64 else [nx, ny * nz]


def general_kernel(
    sizes,
    adj_hbm,
    fwd_hbm,
    des_hbm,
    sol_hbm,
    kind_hbm,
    out_ref,
    sens_ref,
    tot_ref,
    adj,
    fwd,
    des,
    sol,
    kin,
    mid,
    xs,
    ys,
    zs,
    xr,
    yr,
    zr,
    er,
    load_sem,
    store_sem,
    send_sem,
    recv_sem,
    *sum_refs,
):
    ex, ey, ez = des.shape
    me = tuple(lax.axis_index(name) for name in AXES)
    nx, ny, nz = sizes

    loads = [
        pltpu.make_async_copy(adj_hbm, adj, load_sem.at[0]),
        pltpu.make_async_copy(fwd_hbm.at[1], fwd.at[1], load_sem.at[1]),
        pltpu.make_async_copy(des_hbm, des, load_sem.at[2]),
        pltpu.make_async_copy(sol_hbm, sol, load_sem.at[3]),
        pltpu.make_async_copy(kind_hbm, kin, load_sem.at[4]),
        pltpu.make_async_copy(fwd_hbm.at[0], fwd.at[0], load_sem.at[5]),
    ]
    for load in loads:
        load.start()

    def reach(offset, sign):
        ok = None
        where = {}
        for a in range(3):
            c = sign * offset[a]
            where[AXES[a]] = me[a] + c if c else me[a]
            if c == 1:
                test = me[a] < sizes[a] - 1
            elif c == -1:
                test = me[a] > 0
            else:
                continue
            ok = test if ok is None else jnp.logical_and(ok, test)
        return ok, where

    live = [
        i
        for i in range(1, 19)
        if all(sizes[a] > 1 or LAT[i][a] == 0 for a in range(3))
    ]

    def all_peer(k):
        rank = lax.rem((me[0] * ny + me[1]) * nz + me[2] + k, nx * ny * nz)
        return {
            "gx": rank // (ny * nz),
            "gy": lax.rem(rank // nz, ny),
            "gz": lax.rem(rank, nz),
        }

    def x_peer(k):
        return {"gx": lax.rem(me[0] + k, nx), "gy": me[1], "gz": me[2]}

    def yz_peer(k):
        rank = lax.rem(me[1] * nz + me[2] + k, ny * nz)
        return {"gx": me[0], "gy": rank // nz, "gz": lax.rem(rank, nz)}

    if len(sum_groups(sizes)) == 1:
        peers = [all_peer]
    else:
        peers = [x_peer, yz_peer]

    barrier = pltpu.get_barrier_semaphore()
    count = jnp.int32(sum(n - 1 for n in sum_groups(sizes)))
    for n, peer in zip(sum_groups(sizes), peers):
        for k in range(1, n):
            pl.semaphore_signal(barrier, inc=1, device_id=peer(k), device_id_type=MESH)
    if len(peers) > 1:
        for i in live:
            ok, where = reach(LAT[i], -1)

            @pl.when(ok)
            def _():
                pl.semaphore_signal(barrier, inc=1, device_id=where, device_id_type=MESH)

            count = count + reach(LAT[i], 1)[0].astype(jnp.int32)

    def landing(i, t):
        if i < 3:
            return xr.at[t, i - 1]
        if i < 5:
            return yr.at[t, i - 3]
        if i < 7:
            return zr.at[t, i - 5]
        return er.at[t, i - 7]

    def leaving(i, t):
        c = LAT[i]
        if i < 3:
            return xs.at[t, i - 1]
        if i < 5:
            return ys.at[t, i - 3]
        if i < 7:
            return zs.at[t, i - 5]
        if c[2] == 0:
            return ys.at[t, side(c[1]), SLOT[1][i]]
        return zs.at[t, side(c[2])]

    for i in range(1, 19):
        if i in live:

            @pl.when(jnp.logical_not(reach(LAT[i], 1)[0]))
            def _():
                for t in (0, 1):
                    ref = landing(i, t)
                    ref[...] = jnp.zeros(ref.shape, jnp.float32)

        else:
            for t in (0, 1):
                ref = landing(i, t)
                ref[...] = jnp.zeros(ref.shape, jnp.float32)

    lane = lax.broadcasted_iota(jnp.int32, (ey, ez), 1)
    row = lax.broadcasted_iota(jnp.int32, (ey, ez), 0)

    def hop(i, t):
        ok, where = reach(LAT[i], -1)
        copy = pltpu.make_async_remote_copy(
            src_ref=leaving(i, t),
            dst_ref=landing(i, t),
            send_sem=send_sem.at[t, i - 1],
            recv_sem=recv_sem.at[t, i - 1],
            device_id=where,
            device_id_type=MESH,
        )
        return ok, copy

    def pack_layer(t, x, tiles, packs):
        packs = list(packs)
        for sign in (1, -1):
            h = side(sign)
            if x == (0 if sign == 1 else ex - 1):
                for k, i in enumerate(group(0, sign)):
                    xs[t, h, k] = tiles(i)
            edge = 0 if sign == 1 else ey - 1
            for k, i in enumerate(group(1, sign)):
                ys[t, h, k, x : x + 1, :] = tiles(i)[edge : edge + 1, :]
            edge = 0 if sign == 1 else ez - 1
            for k, i in enumerate(group(2, sign)):
                at = k * ex + x
                moved = tiles(i)
                if (at - edge) % ez:
                    moved = pltpu.roll(moved, (at - edge) % ez, 1)
                packs[h] = jnp.where(lane == at, moved, packs[h])
        return tuple(packs)

    def send_all(t, packs):
        zs[t, 0] = packs[0]
        zs[t, 1] = packs[1]
        for i in sorted(live, key=lambda i: (LAT[i][0] == 0, -sum(map(abs, LAT[i])))):
            ok, copy = hop(i, t)
            pl.when(ok)(copy.start)

    def receive(t, along_x):
        for i in live:
            if (LAT[i][0] != 0) == along_x:
                ok = reach(LAT[i], 1)[0]
                pl.when(ok)(hop(i, t)[1].wait_recv)

    def shifted_columns(t):
        moved = {}
        for i in range(15, 19):
            cy, cz = LAT[i][1], LAT[i][2]
            pack = zr[t, side(cz)]
            src, last = (0, ey - 1) if cy == 1 else (ey - 1, 0)
            corner = er[t, i - 7, src : src + 1, :]
            pack = pltpu.roll(pack, (-cy) % ey, 0)
            moved[i] = jnp.where(row == last, corner, pack)
        return moved

    def pulled_tile(source, t, i, x, moved):
        cx, cy, cz = LAT[i]
        at = x + cx
        inside = 0 <= at < ex
        tile = source[i, at] if inside else xr[t, side(cx), SLOT[0][i]]
        if cy:
            h = side(cy)
            if inside:
                fill = yr[t, h, SLOT[1][i], at : at + 1, :]
            else:
                src = 0 if cx == 1 else ex - 1
                fill = er[t, i - 7, src : src + 1, :]
            last = ey - 1 if cy == 1 else 0
            tile = jnp.where(row == last, fill, pltpu.roll(tile, (-cy) % ey, 0))
        if cz:
            h = side(cz)
            col = SLOT[2][i] * ex
            if cy:
                pack, col = moved[i], col + x
            elif inside:
                pack, col = zr[t, h], col + at
            else:
                pack, col = er[t, i - 7], col + (0 if cx == 1 else ex - 1)
            last = ez - 1 if cz == 1 else 0
            if (last - col) % ez:
                pack = pltpu.roll(pack, (last - col) % ez, 1)
            tile = jnp.where(lane == last, pack, pltpu.roll(tile, (-cz) % ez, 1))
        return tile

    whole_x = nx * ex
    zero = jnp.zeros((ey, ez), jnp.float32)

    def step(t, source, target, packs):
        cost_sum, square_sum = zero, zero
        receive(t, False)
        moved = shifted_columns(t)
        for x in list(range(1, ex - 1)) + [0, ex - 1]:
            if x == 0:
                receive(t, True)
            g = des[x]
            solid = sol[x] == 1
            fluid = jnp.where(solid, 0.0, 1.0)
            kind = kin[x]
            inlet, outlet = kind == 1, kind == 2
            inner = jnp.logical_not(jnp.logical_or(inlet, outlet))
            below = 1.0 / (0.5 + 0.6 * g)
            damping = (0.1 + g) * below
            slope = 0.44 * (below * below)
            place = (me[0] * ex + x).astype(jnp.float32)
            weight = 1.0 + 2.0 * place / (whole_x - 1)
            f = [fwd[t, i, x] for i in range(19)]
            p = [pulled_tile(source, t, i, x, moved) for i in range(19)]
            out, sens, cost = cell_adjoint(
                f, p, damping, slope, fluid, solid, inner, inlet, outlet, weight
            )
            for i in range(19):
                target[i, x] = out[i]
            cost_sum = cost_sum + cost
            if t == 1:
                sens_ref[x] = sens
                packs = pack_layer(0, x, lambda i: out[i], packs)
            else:
                sens = sens + sens_ref[x]
                sens_ref[x] = sens
                square_sum = square_sum + sens * sens
        return cost_sum, square_sum, packs

    loads[0].wait()
    packs = (zero, zero)
    for x in range(ex):
        packs = pack_layer(1, x, lambda i: adj[i, x], packs)
    pl.semaphore_wait(barrier, count)
    send_all(1, packs)
    for load in loads[1:]:
        load.wait()
    cost_one, _, packs = step(1, adj, mid, (zero, zero))
    send_all(0, packs)
    cost_two, square, _ = step(0, mid, out_ref, None)

    half = ez // 2
    cost = jnp.sum(cost_one + cost_two, axis=0, keepdims=True)
    square = jnp.sum(square, axis=0, keepdims=True)
    cost = cost + pltpu.roll(cost, half, 1)
    square = square + pltpu.roll(square, half, 1)
    first = lax.broadcasted_iota(jnp.int32, (1, ez), 1) < half
    total = jnp.where(first, square, cost)

    sent = []
    for r, (n, peer) in enumerate(zip(sum_groups(sizes), peers)):
        part, got, send, recv = sum_refs[4 * r : 4 * r + 4]
        if n == 1:
            continue
        part[...] = total
        copies = []
        for k in range(1, n):
            copy = pltpu.make_async_remote_copy(
                src_ref=part,
                dst_ref=got.at[pl.ds(k - 1, 1)],
                send_sem=send.at[k - 1],
                recv_sem=recv.at[k - 1],
                device_id=peer(k),
                device_id_type=MESH,
            )
            copy.start()
            copies.append(copy)
        got[pl.ds(n - 1, 1)] = total
        for copy in copies:
            copy.wait_recv()
        total = jnp.sum(got[...], axis=0, keepdims=True)
        sent += copies
    tot_ref[0, 0:1, :] = jnp.where(first, total, 0.0)
    tot_ref[0, 1:2, :] = jnp.where(first, 0.0, total)
    for t in (1, 0):
        for i in live:
            ok, copy = hop(i, t)
            pl.when(ok)(copy.wait_send)
    for copy in sent:
        copy.wait_send()


def sum_rows():
    trace = (WROWS[4] + WROWS[5] + WROWS[6]) / 3
    along = WROWS[4] - trace
    across = (WROWS[5] - WROWS[6]) / 2
    assert np.allclose(WROWS[5], trace - along / 2 + across)
    rows = [WROWS[0], WROWS[1], WROWS[2], WROWS[3]]
    rows += [3 * trace, 3 * along, 3 * across, 3 * WROWS[7], 3 * WROWS[8], 3 * WROWS[9]]
    out = np.stack(rows)[:, :16]
    out[np.abs(out) < 1e-12] = 0.0
    return out


SUM_ROWS = sum_rows()


def plus(a, b):
    if a is None or b is None:
        return b if a is None else a
    return a + b


def minus(a, b):
    if b is None:
        return a
    return -b if a is None else a - b


def times(c, a):
    return None if a is None else c * a


def some_moments(p):
    s = {i: plus(p[i], p[i + 1]) for i in range(1, 19, 2)}
    d = {i: minus(p[i], p[i + 1]) for i in range(1, 19, 2)}
    sxy, sxz, syz = plus(s[7], s[9]), plus(s[11], s[13]), plus(s[15], s[17])
    axis_yz = plus(s[3], s[5])
    axis = plus(s[1], axis_yz)
    exy = plus(sxy, sxz)
    edge = plus(exy, syz)
    m = [None] * 19
    m[0] = plus(plus(p[0], axis), edge)
    m[1] = minus(minus(times(8.0, edge), times(11.0, axis)), times(30.0, p[0]))
    m[2] = plus(minus(edge, times(4.0, axis)), times(12.0, p[0]))
    a = minus(times(2.0, s[1]), axis_yz)
    b = minus(exy, times(2.0, syz))
    m[9] = plus(a, b)
    m[10] = minus(b, times(2.0, a))
    a = minus(s[3], s[5])
    b = minus(sxy, sxz)
    m[11] = plus(a, b)
    m[12] = minus(b, times(2.0, a))
    m[13] = minus(s[7], s[9])
    m[14] = minus(s[15], s[17])
    m[15] = minus(s[11], s[13])
    xa, xb = plus(d[7], d[9]), plus(d[11], d[13])
    ya, yb = minus(d[7], d[9]), plus(d[15], d[17])
    za, zb = minus(d[11], d[13]), minus(d[15], d[17])
    for k, axis_d, u, v in ((3, d[1], xa, xb), (5, d[3], ya, yb), (7, d[5], za, zb)):
        e = plus(u, v)
        m[k] = plus(axis_d, e)
        m[k + 1] = minus(e, times(4.0, axis_d))
    m[16] = minus(xa, xb)
    m[17] = minus(yb, ya)
    m[18] = minus(za, zb)
    return m


def cell_state(f, g, fluid, inlet, outlet, weight):
    s, d = flux_sums(f)
    rho = f[0]
    for i in s:
        rho = rho + s[i]
    fx = d[1] + (d[7] + d[9]) + (d[11] + d[13])
    fy = d[3] + (d[7] - d[9]) + (d[15] + d[17])
    fz = d[5] + (d[11] - d[13]) + (d[15] - d[17])
    below = 1.0 / (0.5 + 0.6 * g)
    damping = (0.1 + g) * below
    slope = 0.44 * (below * below)
    inv = 1.0 / rho
    b = [fx * inv, fy * inv, fz * inv]
    u = [c * damping for c in b]
    uu = u[0] * u[0] + u[1] * u[1] + u[2] * u[2]
    wr = weight * rho
    v = [jnp.where(inlet, c, a) for a, c in zip(u, (inflow_speed, 0.0, 0.0))]
    scale = jnp.where(inlet, 0.0, jnp.where(outlet, 3.0, 3.0 * rho))
    half = (0.5 * weight) * uu
    state = v + [wr * c for c in u] + b + [scale, damping * inv, half, fluid * slope]
    return state, fluid * (rho * half)


def cell_sums(m, state, inner, outlet):
    vx, vy, vz, wx, wy, wz, bx, by, bz, scale, di, half, slope = state
    n = [None] * 19
    for k in range(16):
        rate = float(np.float32(RATES[k]))
        n[k] = m[k] * jnp.where(inner, rate, 1.0) if np.any(SUM_ROWS[:, k]) else None
    s0, sx, sy, sz, trace, along, across, xy, yz, xz = [combine(r, n) for r in SUM_ROWS]
    xx = trace + along
    side_on = trace - 0.5 * along
    yy, zz = side_on + across, side_on - across
    ax = sx + (xx * vx + xy * vy + xz * vz) - s0 * vx
    ay = sy + (xy * vx + yy * vy + yz * vz) - s0 * vy
    az = sz + (xz * vx + yz * vy + zz * vz) - s0 * vz
    along_v = (ax + sx) * vx + (ay + sy) * vy + (az + sz) * vz
    rho_bar = jnp.where(outlet, 0.0, s0 + 1.5 * along_v) + half
    ux_bar, uy_bar, uz_bar = scale * ax + wx, scale * ay + wy, scale * az + wz
    d_bar = ux_bar * bx + uy_bar * by + uz_bar * bz
    extra = [rho_bar - d_bar * di, ux_bar * di, uy_bar * di, uz_bar * di]
    return extra, d_bar * slope


def cell_out(p, m, extra, inner, solid):
    z = [None] * 19
    for k in range(19):
        coef = float(np.float32((1.0 - RATES[k]) / NORMS[k]))
        z[k] = jnp.where(inner, coef * m[k], 0.0)
    for k, e in zip((0, 3, 5, 7), extra):
        z[k] = z[k] + e
    out = rebuild(z)
    return [jnp.where(solid, p[opposite_index[i]], out[i]) for i in range(19)]


def near(sizes, cells):
    nx, ny, nz = sizes
    ex, ey, _ = cells
    return ny == 2 and nz == 2 and nx * ny * nz <= 64 and ex == ey and ey % 8 == 0


def rounds(nx):
    return max((nx - 1) // 2, 0)


def end_rows(n, ey, faces):
    return 2 * (7 * ey + faces * (6 * ey + 1)) + 2 * (n - 1)


def fast_kernel(
    sizes,
    adj_hbm,
    fwd_hbm,
    des_hbm,
    sol_hbm,
    kind_hbm,
    out_ref,
    sens_ref,
    tot_ref,
    adj,
    fwd,
    des,
    marks,
    mid,
    pre,
    mom,
    xs,
    xe,
    ys,
    zs,
    xr,
    yr,
    zr,
    er,
    part,
    size_loads,
    size_sends,
    load_sem,
    send_sem,
    side_sem,
    face_sem,
    sum_sem,
    round_sem,
):
    ex, ey, ez = des.shape
    nx, ny, nz = sizes
    mx, my, mz = (lax.axis_index(name) for name in AXES)
    oy, oz = 1 - my, 1 - mz
    has = {1: mx < nx - 1, -1: mx > 0}
    far = {2: mx < nx - 2, -2: mx > 1}

    loads = [
        pltpu.make_async_copy(adj_hbm, adj, load_sem.at[0]),
        pltpu.make_async_copy(fwd_hbm, fwd, load_sem.at[1]),
        pltpu.make_async_copy(des_hbm, des, load_sem.at[1]),
        pltpu.make_async_copy(sol_hbm, marks.at[0], load_sem.at[1]),
        pltpu.make_async_copy(kind_hbm, marks.at[1], load_sem.at[1]),
    ]
    loads[0].start()

    barrier = pltpu.get_barrier_semaphore()

    def greet(x, y, z):
        pl.semaphore_signal(
            barrier, inc=1, device_id={"gx": x, "gy": y, "gz": z}, device_id_type=MESH
        )

    for y, z in ((my, oz), (oy, oz), (my, mz), (oy, mz)):
        for s in (1, -1):
            pl.when(has[s])(functools.partial(greet, mx + s, y, z))
    for y, z in ((my, oz), (oy, oz), (oy, mz)):
        greet(mx, y, z)
    for s in (2, -2):

        @pl.when(far[s])
        def _():
            greet(mx + s, my, mz)

    far_count = far[2].astype(jnp.int32) + far[-2].astype(jnp.int32)
    count = 3 + 4 * (has[1].astype(jnp.int32) + has[-1].astype(jnp.int32)) + far_count
    for load in loads[1:]:
        load.start()

    def tell(j):
        for s in (2, -2):

            @pl.when(far[s])
            def _():
                pl.semaphore_signal(
                    round_sem.at[j],
                    inc=1,
                    device_id={"gx": mx + s, "gy": my, "gz": mz},
                    device_id_type=MESH,
                )

    def hear(j):
        pl.semaphore_wait(round_sem.at[j], far_count)

    def relay(j):
        if j < rounds(nx):
            if j > 0:
                hear(j - 1)
            tell(j)

    def clear(ref):
        ref[...] = jnp.zeros(ref.shape, jnp.float32)

    for t in (0, 1):
        clear(yr.at[t, oy])
        clear(zr.at[t, oz])
        clear(er.at[t, oy, mz])
        clear(er.at[t, my, oz])
        clear(er.at[t, oy, oz])
    for s in (1, -1):

        @pl.when(jnp.logical_not(has[s]))
        def _():
            clear(xr.at[side(s)])

    lane = lax.broadcasted_iota(jnp.int32, (ey, ez), 1)
    row = lax.broadcasted_iota(jnp.int32, (ey, ez), 0)
    low_z = jnp.broadcast_to(mz == 1, (ey, ez))
    slot_lane = jnp.where(low_z, lane, jnp.where(lane == ez - 1, 0, lane + 1))
    match_y = [jnp.broadcast_to(my == h, (1, ez)) for h in (0, 1)]
    match_z = [jnp.broadcast_to(mz == h, (ey, ez)) for h in (0, 1)]

    def push(src, dst, sent, came, x, y, z):
        return pltpu.make_async_remote_copy(
            src_ref=src,
            dst_ref=dst,
            send_sem=sent,
            recv_sem=came,
            device_id={"gx": x, "gy": y, "gz": z},
            device_id_type=MESH,
        )

    def x_sends(t, turn):
        h = lax.rem(mx + turn, 2)
        sent, came, at = send_sem, face_sem.at[t], mx - 1 + 2 * h
        face, last = 5 * ey, 6 * ey
        tilted = pl.multiple_of((3 + jnp.where(h == 0, oz, mz)) * ey, 8)
        edge = xs.at[t, h, pl.ds(tilted, ey)]
        copies = [
            push(edge, xr.at[h, t, pl.ds(face, ey)], sent, came, at, my, oz),
            push(xs.at[t, h], xr.at[h, t, pl.ds(0, face)], sent, came, at, my, mz),
            push(xe.at[t, h, oy], xr.at[h, t, pl.ds(last, 1)], sent, came, at, oy, mz),
        ]
        return jnp.where(h == 0, mx > 0, mx < nx - 1), copies

    def side_sends(t):
        sent, came = send_sem, side_sem.at[t]
        return [
            push(zs.at[t], zr.at[t, oz], sent, came, mx, my, oz),
            push(zs.at[t], er.at[t, oy, oz], sent, came, mx, oy, oz),
            push(ys.at[t, oy], yr.at[t, oy], sent, came, mx, oy, mz),
        ]

    shifted = (1,)

    def store_face(t, x, tiles):
        for sign in (1, -1):
            h = side(sign)
            if x != (0 if sign == 1 else ex - 1):
                continue
            for k, i in enumerate(group(0, sign)):
                cy, cz = LAT[i][1:]
                sent = pltpu.roll(tiles(i), (-cz) % ez, 1) if cz and t in shifted else tiles(i)
                xs[t, h, k * ey : (k + 1) * ey, :] = sent
                if cy:
                    cut = 0 if cy == 1 else ey - 1
                    xe[t, h, side(cy)] = tiles(i)[cut : cut + 1, :]

    def pack_sides(t, x, tiles, pack):
        for sign in (1, -1):
            h = side(sign)
            edge = 0 if sign == 1 else ey - 1
            for k, i in enumerate(group(1, sign)):
                ys[t, h, k, x : x + 1, :] = tiles(i)[edge : edge + 1, :]
        for k, (i, j) in enumerate(zip(group(2, 1), group(2, -1))):
            at = k * ex + x
            moved = jnp.where(low_z, tiles(i), tiles(j))
            if at % ez:
                moved = pltpu.roll(moved, at % ez, 1)
            pack = jnp.where(slot_lane == at, moved, pack)
        return pack

    def send_faces(t):
        for turn in (0, 1):
            ok, copies = x_sends(t, turn)

            @pl.when(ok)
            def _():
                for copy in copies:
                    copy.start()

    def send_sides(t, pack):
        zs[t] = pack
        for copy in side_sends(t):
            copy.start()

    def await_bytes(ref, sem):
        pltpu.make_async_copy(ref, ref, sem).wait()

    def receive_sides(t):
        await_bytes(xr.at[0, t], side_sem.at[t])

    both = jnp.logical_and(has[1], has[-1])

    def receive_faces(t):
        rows = pl.ds(0, 6 * ey + 1)

        @pl.when(both)
        def _():
            await_bytes(xr.at[:, t, rows], face_sem.at[t])

        if nx > 1:

            @pl.when(jnp.logical_not(both))
            def _():
                await_bytes(xr.at[0, t, rows], face_sem.at[t])

    def shifted_columns(t):
        moved = {}
        for i in range(15, 19):
            cy, cz = LAT[i][1], LAT[i][2]
            pack = zr[t, side(cz)]
            src, last = (0, ey - 1) if cy == 1 else (ey - 1, 0)
            corner = er[t, side(cy), side(cz), src : src + 1, :]
            pack = pltpu.roll(pack, (-cy) % ey, 0)
            moved[i] = jnp.where(row == last, corner, pack)
        return moved

    def pulled_tile(source, t, i, x, moved):
        cx, cy, cz = LAT[i]
        at = x + cx
        inside = 0 <= at < ex
        if inside:
            tile = source[i, at]
        else:
            k = SLOT[0][i] * ey
            tile = xr[side(cx), t, k : k + ey, :]
        src = 0 if cx == 1 else ex - 1
        if cy:
            h = side(cy)
            if inside:
                fill = yr[t, h, SLOT[1][i], at : at + 1, :]
            else:
                fill = xr[side(cx), t, 6 * ey : 6 * ey + 1, :]
                fill = jnp.where(match_y[h], fill, 0.0)
            last = ey - 1 if cy == 1 else 0
            tile = jnp.where(row == last, fill, pltpu.roll(tile, (-cy) % ey, 0))
        if cz:
            h = side(cz)
            last = ez - 1 if cz == 1 else 0
            if not inside:
                pack = xr[side(cx), t, 5 * ey : 6 * ey, :]
                pack = jnp.where(match_z[h], pack, 0.0)
                if t in shifted:
                    return jnp.where(lane == last, pack, tile)
                tile = jnp.where(lane == ez - 1 - last, pack, tile)
                return pltpu.roll(tile, (-cz) % ez, 1)
            col = SLOT[2][i] * ex - h
            if cy:
                pack, col = moved[i], col + x
            else:
                pack, col = zr[t, h], col + at
            if (last - col) % ez:
                pack = pltpu.roll(pack, (last - col) % ez, 1)
            tile = jnp.where(lane == last, pack, pltpu.roll(tile, (-cz) % ez, 1))
        return tile

    whole_x = nx * ex
    zero = jnp.zeros((ey, ez), jnp.float32)

    def marked(x):
        kind = marks[1, x]
        return kind == 0, kind == 1, kind == 2, marks[0, x] == 1

    def prepare(t):
        total = zero
        for x in range(ex):
            _, inlet, outlet, solid = marked(x)
            fluid = jnp.where(solid, 0.0, 1.0)
            place = (mx * ex + x).astype(jnp.float32)
            weight = 1.0 + 2.0 * place / (whole_x - 1)
            f = [fwd[t, i, x] for i in range(19)]
            state, cost = cell_state(f, des[x], fluid, inlet, outlet, weight)
            for q, value in enumerate(state):
                pre[q, x] = value
            total = total + cost
        return total

    def is_late(i, x):
        return not 0 <= x + LAT[i][0] < ex

    def sums_of(m, x):
        inner, _, outlet, _ = marked(x)
        return cell_sums(m, [pre[q, x] for q in range(13)], inner, outlet)

    edges = sorted({0, ex - 1})
    inner_planes = range(1, ex - 1)

    def pull(t, source, done):
        receive_sides(t)
        if t == 1:
            relay(1)
        moved = shifted_columns(t)
        for x in inner_planes:
            p = [pulled_tile(source, t, i, x, moved) for i in range(19)]
            done(x, p, some_moments(p))
        early = {}
        for x in edges:
            p = [
                None if is_late(i, x) else pulled_tile(source, t, i, x, moved)
                for i in range(19)
            ]
            early[x] = p, some_moments(p)
        with jax.named_scope(f"faces {t}"):
            receive_faces(t)
        for x in edges:
            p, m = early[x]
            late = [
                pulled_tile(source, t, i, x, moved) if is_late(i, x) else None
                for i in range(19)
            ]
            p = [b if a is None else a for a, b in zip(p, late)]
            done(x, p, [plus(a, b) for a, b in zip(m, some_moments(late))])

    with jax.named_scope("load"):
        loads[0].wait()
    for x in edges:
        store_face(1, x, lambda i: adj[i, x])
    with jax.named_scope("greeted"):
        pl.semaphore_wait(barrier, count)
    with jax.named_scope("send 1"):
        send_faces(1)
    pack = zero
    for x in range(ex):
        pack = pack_sides(1, x, lambda i: adj[i, x], pack)
    with jax.named_scope("sides 1"):
        send_sides(1, pack)
        relay(0)
    await_bytes(size_loads, load_sem.at[1])
    cost = prepare(1)
    packs = [zero]
    kept = {}

    def keep(x, out, sens):
        for i in range(19):
            mid[i, x] = out[i]
        sens_ref[x] = sens
        packs[0] = pack_sides(0, x, lambda i: out[i], packs[0])

    def first_done(x, p, m):
        inner, _, _, solid = marked(x)
        extra, sens = sums_of(m, x)
        out = cell_out(p, m, extra, inner, solid)
        if x in edges:
            store_face(0, x, lambda i: out[i])
            kept[x] = out, sens
        else:
            keep(x, out, sens)

    with jax.named_scope("step 1"):
        pull(1, adj, first_done)
    with jax.named_scope("send 0"):
        send_faces(0)
    for x, (out, sens) in kept.items():
        keep(x, out, sens)
    with jax.named_scope("sides 0"):
        send_sides(0, packs[0])
    for j in range(2, rounds(nx)):
        relay(j)
    cost = cost + prepare(0)
    squares = [zero]

    def second_done(x, p, m):
        extra, sens = sums_of(m, x)
        sens = sens + sens_ref[x]
        sens_ref[x] = sens
        squares[0] = squares[0] + sens * sens
        for i in range(19):
            adj[i, x] = p[i]
        for k, value in enumerate(m + extra):
            mom[k, x] = value

    with jax.named_scope("step 0"):
        pull(0, mid, second_done)
    part[0:1, :] = jnp.sum(squares[0], axis=0, keepdims=True)
    part[1:2, :] = jnp.sum(cost, axis=0, keepdims=True)

    with jax.named_scope("heard"):
        if rounds(nx):
            hear(rounds(nx) - 1)
    n = nx * ny * nz

    def sum_send(k, x, y, z):
        return push(part, tot_ref.at[k - 1], send_sem, sum_sem, x, y, z)

    with jax.named_scope("send sums"):
        for px in range(nx):
            dx = jnp.where(px < mx, px - mx + nx, px - mx)
            for dy, dz in ((0, 1), (1, 1), (0, 0), (1, 0)):
                k = (dx * ny + dy) * nz + dz
                y, z = (oy if dy else my), (oz if dz else mz)
                if dy or dz:
                    sum_send(k, px, y, z).start()
                else:
                    pl.when(px != mx)(sum_send(k, px, y, z).start)
    tot_ref[n - 1] = part[...]
    with jax.named_scope("out"):
        for x in range(ex):
            inner, _, _, solid = marked(x)
            m = [mom[k, x] for k in range(23)]
            out = cell_out([adj[i, x] for i in range(19)], m[:19], m[19:], inner, solid)
            for i in range(19):
                out_ref[i, x] = out[i]
    with jax.named_scope("sums"):
        await_bytes(tot_ref.at[pl.ds(0, n - 1)], sum_sem)
    with jax.named_scope("drain"):

        @pl.when(both)
        def _():
            await_bytes(size_sends, send_sem)

        @pl.when(jnp.logical_not(both))
        def _():
            await_bytes(size_sends.at[pl.ds(0, end_rows(n, ey, nx > 1))], send_sem)


def hand_on(
    cells,
    adj_in,
    sens_in,
    sums_in,
    adj_out,
    sens_out,
    obj_out,
    rms_out,
    sens,
    obj,
    rms,
    sem,
):
    moves = [(adj_in, adj_out), (sens, sens_out), (obj, obj_out), (rms, rms_out)]
    copies = [pltpu.make_async_copy(a, b, sem.at[k]) for k, (a, b) in enumerate(moves)]
    copies[0].start()
    total = jnp.sum(jnp.sum(sums_in[...], axis=0), axis=1, keepdims=True) / cells
    root = jnp.sqrt(total[0:1] + 1e-06)
    scale = jnp.broadcast_to(1.0 / root, sens.shape[1:])
    for x in range(sens.shape[0]):
        sens[x] = sens_in[x] * scale
    copies[1].start()
    obj[0] = total[1, 0]
    rms[0] = root[0, 0]
    copies[2].start()
    copies[3].start()
    for copy in copies:
        copy.wait()


def body(sizes, adjoint_in, forward_states, design, solid_mask, boundary_kind):
    ex, ey, ez = design.shape
    nx, ny, nz = sizes
    any_spec = pl.BlockSpec(memory_space=pltpu.HBM)
    vmem_spec = pl.BlockSpec(memory_space=pltpu.VMEM)
    f32 = jnp.float32
    operands = (adjoint_in, forward_states, design, solid_mask, boundary_kind)
    operands = [pltpu.with_memory_space_constraint(a, pltpu.HBM) for a in operands]
    if near(sizes, design.shape):
        n = nx * ny * nz
        count = adjoint_in.shape[0]
        run = fast_kernel
        scratch = [
            pltpu.VMEM(adjoint_in.shape, f32),
            pltpu.VMEM(forward_states.shape, f32),
            pltpu.VMEM(design.shape, f32),
            pltpu.VMEM((2, *design.shape), jnp.int32),
            pltpu.VMEM(adjoint_in.shape, f32),
            pltpu.VMEM((13, *design.shape), f32),
            pltpu.VMEM((23, *design.shape), f32),
            pltpu.VMEM((2, 2, 5 * ey, ez), f32),
            pltpu.VMEM((2, 2, 2, 1, ez), f32),
            pltpu.VMEM((2, 2, 5, ex, ez), f32),
            pltpu.VMEM((2, ey, ez), f32),
            pltpu.VMEM((2, 2, 7 * ey, ez), f32),
            pltpu.VMEM((2, 2, 5, ex, ez), f32),
            pltpu.VMEM((2, 2, ey, ez), f32),
            pltpu.VMEM((2, 2, 2, ey, ez), f32),
            pltpu.VMEM((2, ez), f32),
            pltpu.VMEM((2 * count + 3, *design.shape), f32),
            pltpu.VMEM((end_rows(n, ey, 2), ez), f32),
            pltpu.SemaphoreType.DMA((2,)),
            pltpu.SemaphoreType.DMA,
            pltpu.SemaphoreType.DMA((2,)),
            pltpu.SemaphoreType.DMA((2,)),
            pltpu.SemaphoreType.DMA,
            pltpu.SemaphoreType.REGULAR((max(rounds(nx), 1),)),
        ]
    else:
        n = 1
        run = general_kernel
        sum_scratch = []
        for n in sum_groups(sizes):
            sum_scratch += [
                pltpu.VMEM((1, ez), f32),
                pltpu.VMEM((n, ez), f32),
                pltpu.SemaphoreType.DMA((max(n - 1, 1),)),
                pltpu.SemaphoreType.DMA((max(n - 1, 1),)),
            ]
        scratch = [
            pltpu.VMEM(adjoint_in.shape, f32),
            pltpu.VMEM(forward_states.shape, f32),
            pltpu.VMEM(design.shape, f32),
            pltpu.VMEM(design.shape, jnp.int32),
            pltpu.VMEM(design.shape, jnp.int32),
            pltpu.VMEM(adjoint_in.shape, f32),
            pltpu.VMEM((2, 2, 5, ey, ez), f32),
            pltpu.VMEM((2, 2, 5, ex, ez), f32),
            pltpu.VMEM((2, 2, ey, ez), f32),
            pltpu.VMEM((2, 2, 5, ey, ez), f32),
            pltpu.VMEM((2, 2, 5, ex, ez), f32),
            pltpu.VMEM((2, 2, ey, ez), f32),
            pltpu.VMEM((2, 12, ey, ez), f32),
            pltpu.SemaphoreType.DMA((6,)),
            pltpu.SemaphoreType.DMA,
            pltpu.SemaphoreType.DMA((2, 18)),
            pltpu.SemaphoreType.DMA((2, 18)),
            *sum_scratch,
        ]
    adjoint, sens, tot = pl.pallas_call(
        functools.partial(run, sizes),
        out_shape=(
            jax.ShapeDtypeStruct(adjoint_in.shape, f32),
            jax.ShapeDtypeStruct(design.shape, f32),
            jax.ShapeDtypeStruct((n, 2, ez), f32),
        ),
        in_specs=[any_spec] * 5,
        out_specs=(vmem_spec, vmem_spec, vmem_spec),
        scratch_shapes=scratch,
        compiler_params=pltpu.CompilerParams(
            collective_id=0, has_side_effects=True, vmem_limit_bytes=VMEM_LIMIT
        ),
    )(*operands)
    adjoint, sens, objective, rms = pl.pallas_call(
        functools.partial(hand_on, nx * ex * ny * ey * nz * ez),
        out_shape=(
            jax.ShapeDtypeStruct(adjoint_in.shape, f32),
            jax.ShapeDtypeStruct(design.shape, f32),
            jax.ShapeDtypeStruct((1,), f32),
            jax.ShapeDtypeStruct((1,), f32),
        ),
        in_specs=[vmem_spec] * 3,
        out_specs=(any_spec, any_spec, any_spec, any_spec),
        scratch_shapes=[
            pltpu.VMEM(design.shape, f32),
            pltpu.SMEM((1,), f32),
            pltpu.SMEM((1,), f32),
            pltpu.SemaphoreType.DMA((4,)),
        ],
        compiler_params=pltpu.CompilerParams(vmem_limit_bytes=VMEM_LIMIT),
    )(adjoint, sens, tot)
    return adjoint, sens, objective.reshape(()), rms.reshape(())


def solution(mesh):
    placed = (
        P(None, "gx", "gy", "gz"),
        P(None, None, "gx", "gy", "gz"),
        P("gx", "gy", "gz"),
        P("gx", "gy", "gz"),
        P("gx", "gy", "gz"),
    )
    return jax.shard_map(
        functools.partial(body, tuple(int(mesh.shape[name]) for name in AXES)),
        mesh=mesh,
        in_specs=placed,
        out_specs=(P(None, "gx", "gy", "gz"), P("gx", "gy", "gz"), P(), P()),
        check_vma=False,
    )
```

```python
import functools

import jax
import jax.numpy as jnp
import numpy as np
from jax import lax
from jax.experimental import pallas as pl
from jax.experimental.pallas import tpu as pltpu
from jax.sharding import PartitionSpec as P

MESH = pl.DeviceIdType.MESH
lattice_table = np.array(
    [
        [0, 0, 0],
        [1, 0, 0],
        [-1, 0, 0],
        [0, 1, 0],
        [0, -1, 0],
        [0, 0, 1],
        [0, 0, -1],
        [1, 1, 0],
        [-1, -1, 0],
        [1, -1, 0],
        [-1, 1, 0],
        [1, 0, 1],
        [-1, 0, -1],
        [1, 0, -1],
        [-1, 0, 1],
        [0, 1, 1],
        [0, -1, -1],
        [0, 1, -1],
        [0, -1, 1],
    ],
    dtype=np.int32,
)
LAT = [tuple(int(v) for v in row) for row in lattice_table]
WEIGHTS = np.array([1.0 / 3] + [1.0 / 18] * 6 + [1.0 / 36] * 12, dtype=np.float64)
opposite_index = [0, 2, 1, 4, 3, 6, 5, 8, 7, 10, 9, 12, 11, 14, 13, 16, 15, 18, 17]
inflow_speed = 0.08
AXES = ("gx", "gy", "gz")
VMEM_LIMIT = 16000 * 1024


def moment_rows():
    c = lattice_table.astype(np.float64)
    cx, cy, cz = c[:, 0], c[:, 1], c[:, 2]
    csq = cx * cx + cy * cy + cz * cz
    return np.stack(
        [
            np.ones(19),
            19 * csq - 30,
            (21 * csq * csq - 53 * csq + 24) / 2,
            cx,
            (5 * csq - 9) * cx,
            cy,
            (5 * csq - 9) * cy,
            cz,
            (5 * csq - 9) * cz,
            3 * cx * cx - csq,
            (3 * csq - 5) * (3 * cx * cx - csq),
            cy * cy - cz * cz,
            (3 * csq - 5) * (cy * cy - cz * cz),
            cx * cy,
            cy * cz,
            cx * cz,
            (cy * cy - cz * cz) * cx,
            (cz * cz - cx * cx) * cy,
            (cx * cx - cy * cy) * cz,
        ]
    )


ROWS = moment_rows()
NORMS = np.sum(ROWS * ROWS, axis=1)
SHEAR = 1.0 / 0.6
RATES = [0, 1.19, 1.4, 0, 1.2, 0, 1.2, 0, 1.2, SHEAR, 1.4, SHEAR, 1.4, SHEAR, SHEAR, SHEAR]
RATES = np.array(RATES + [1.98, 1.98, 1.98], dtype=np.float64)


def weighted_rows():
    c = lattice_table.astype(np.float64)
    pairs = [(0, 0), (1, 1), (2, 2), (0, 1), (1, 2), (0, 2)]
    rows = [WEIGHTS] + [WEIGHTS * c[:, a] for a in range(3)]
    rows += [WEIGHTS * c[:, a] * c[:, b] for a, b in pairs]
    out = np.stack(rows) @ (ROWS / NORMS[:, None]).T
    out[np.abs(out) < 1e-12] = 0.0
    return out


WROWS = weighted_rows()


def group(column, sign):
    return [i for i in range(19) if LAT[i][column] == sign]


SLOT = [{i: k for s in (1, -1) for k, i in enumerate(group(col, s))} for col in range(3)]


def side(sign):
    return 0 if sign == 1 else 1


def combine(coefs, terms):
    total = None
    for coef, term in zip(coefs, terms):
        if coef == 0.0:
            continue
        part = term if coef == 1.0 else float(np.float32(coef)) * term
        total = part if total is None else total + part
    return total


def flux_sums(f):
    s = {i: f[i] + f[i + 1] for i in range(1, 19, 2)}
    d = {i: f[i] - f[i + 1] for i in range(1, 19, 2)}
    return s, d


def moments(p):
    s, d = flux_sums(p)
    sxy, sxz, syz = s[7] + s[9], s[11] + s[13], s[15] + s[17]
    axis_yz = s[3] + s[5]
    axis = s[1] + axis_yz
    exy = sxy + sxz
    edge = exy + syz
    m = [None] * 19
    m[0] = p[0] + axis + edge
    m[1] = 8.0 * edge - 11.0 * axis - 30.0 * p[0]
    m[2] = edge - 4.0 * axis + 12.0 * p[0]
    a = 2.0 * s[1] - axis_yz
    b = exy - 2.0 * syz
    m[9] = a + b
    m[10] = b - 2.0 * a
    a = s[3] - s[5]
    b = sxy - sxz
    m[11] = a + b
    m[12] = b - 2.0 * a
    m[13] = s[7] - s[9]
    m[14] = s[15] - s[17]
    m[15] = s[11] - s[13]
    xa, xb = d[7] + d[9], d[11] + d[13]
    ya, yb = d[7] - d[9], d[15] + d[17]
    za, zb = d[11] - d[13], d[15] - d[17]
    for k, axis_d, u, v in ((3, d[1], xa, xb), (5, d[3], ya, yb), (7, d[5], za, zb)):
        e = u + v
        m[k] = axis_d + e
        m[k + 1] = e - 4.0 * axis_d
    m[16] = xa - xb
    m[17] = yb - ya
    m[18] = za - zb
    return m


def rebuild(z):
    out = [None] * 19
    out[0] = z[0] - 30.0 * z[1] + 12.0 * z[2]
    axis = z[0] - 11.0 * z[1] - 4.0 * z[2]
    edge = z[0] + 8.0 * z[1] + z[2]
    px = z[9] - 2.0 * z[10]
    pw = z[11] - 2.0 * z[12]
    qx = z[9] + z[10]
    qw = z[11] + z[12]
    ayz = axis - px
    eyz = edge - 2.0 * qx
    exx = edge + qx
    exy, exz = exx + qw, exx - qw
    jx, jy, jz = z[3] + z[4], z[5] + z[6], z[7] + z[8]
    x1, x2 = jx + z[16], jx - z[16]
    y1, y2 = jy - z[17], jy + z[17]
    z1, z2 = jz + z[18], jz - z[18]
    even = {
        1: axis + 2.0 * px,
        3: ayz + pw,
        5: ayz - pw,
        7: exy + z[13],
        9: exy - z[13],
        11: exz + z[15],
        13: exz - z[15],
        15: eyz + z[14],
        17: eyz - z[14],
    }
    odd = {
        1: z[3] - 4.0 * z[4],
        3: z[5] - 4.0 * z[6],
        5: z[7] - 4.0 * z[8],
        7: x1 + y1,
        9: x1 - y1,
        11: x2 + z1,
        13: x2 - z1,
        15: y2 + z2,
        17: y2 - z2,
    }
    for i in even:
        out[i] = even[i] + odd[i]
        out[i + 1] = even[i] - odd[i]
    return out


def cell_adjoint(f, p, damping, slope, fluid, solid, inner, inlet, outlet, weight):
    s, d = flux_sums(f)
    rho = f[0]
    for i in s:
        rho = rho + s[i]
    fx = d[1] + (d[7] + d[9]) + (d[11] + d[13])
    fy = d[3] + (d[7] - d[9]) + (d[15] + d[17])
    fz = d[5] + (d[11] - d[13]) + (d[15] - d[17])
    inv = 1.0 / rho
    bx, by, bz = fx * inv, fy * inv, fz * inv
    ux, uy, uz = bx * damping, by * damping, bz * damping
    uu = ux * ux + uy * uy + uz * uz
    m = moments(p)
    n = [None] * 19
    for k in range(16):
        rate = float(np.float32(RATES[k]))
        n[k] = m[k] * jnp.where(inner, rate, 1.0) if np.any(WROWS[:, k]) else None
    s0, sx, sy, sz, xx, yy, zz, xy, yz, xz = [
        combine(WROWS[r, :16], n) for r in range(10)
    ]
    vx = jnp.where(inlet, inflow_speed, ux)
    vy = jnp.where(inlet, 0.0, uy)
    vz = jnp.where(inlet, 0.0, uz)
    gx = xx * vx + xy * vy + xz * vz
    gy = xy * vx + yy * vy + yz * vz
    gz = xz * vx + yz * vy + zz * vz
    vv = vx * vx + vy * vy + vz * vz
    rho_bar = (
        s0 * (1.0 - 1.5 * vv)
        + 3.0 * (sx * vx + sy * vy + sz * vz)
        + 4.5 * (gx * vx + gy * vy + gz * vz)
    )
    rho_bar = jnp.where(outlet, 0.0, rho_bar) + (0.5 * weight) * uu
    scale = jnp.where(inlet, 0.0, jnp.where(outlet, 1.0, rho))
    wr = weight * rho
    ux_bar = scale * (3.0 * sx + 9.0 * gx - 3.0 * s0 * vx) + wr * ux
    uy_bar = scale * (3.0 * sy + 9.0 * gy - 3.0 * s0 * vy) + wr * uy
    uz_bar = scale * (3.0 * sz + 9.0 * gz - 3.0 * s0 * vz) + wr * uz
    d_bar = ux_bar * bx + uy_bar * by + uz_bar * bz
    di = damping * inv
    rho_bar = rho_bar - d_bar * di
    z = [None] * 19
    for k in range(19):
        coef = (1.0 - RATES[k]) / NORMS[k]
        z[k] = jnp.where(inner, float(np.float32(coef)) * m[k], 0.0)
    z[0] = z[0] + rho_bar
    z[3] = z[3] + ux_bar * di
    z[5] = z[5] + uy_bar * di
    z[7] = z[7] + uz_bar * di
    out = rebuild(z)
    out = [jnp.where(solid, p[opposite_index[i]], out[i]) for i in range(19)]
    sens = fluid * (d_bar * slope)
    cost = fluid * (0.5 * wr * uu)
    return out, sens, cost


def sum_groups(sizes):
    nx, ny, nz = sizes
    return [nx * ny * nz] if nx * ny * nz <= 64 else [nx, ny * nz]


def general_kernel(
    sizes,
    adj_hbm,
    fwd_hbm,
    des_hbm,
    sol_hbm,
    kind_hbm,
    out_ref,
    sens_ref,
    tot_ref,
    adj,
    fwd,
    des,
    sol,
    kin,
    mid,
    xs,
    ys,
    zs,
    xr,
    yr,
    zr,
    er,
    load_sem,
    store_sem,
    send_sem,
    recv_sem,
    *sum_refs,
):
    ex, ey, ez = des.shape
    me = tuple(lax.axis_index(name) for name in AXES)
    nx, ny, nz = sizes

    loads = [
        pltpu.make_async_copy(adj_hbm, adj, load_sem.at[0]),
        pltpu.make_async_copy(fwd_hbm.at[1], fwd.at[1], load_sem.at[1]),
        pltpu.make_async_copy(des_hbm, des, load_sem.at[2]),
        pltpu.make_async_copy(sol_hbm, sol, load_sem.at[3]),
        pltpu.make_async_copy(kind_hbm, kin, load_sem.at[4]),
        pltpu.make_async_copy(fwd_hbm.at[0], fwd.at[0], load_sem.at[5]),
    ]
    for load in loads:
        load.start()

    def reach(offset, sign):
        ok = None
        where = {}
        for a in range(3):
            c = sign * offset[a]
            where[AXES[a]] = me[a] + c if c else me[a]
            if c == 1:
                test = me[a] < sizes[a] - 1
            elif c == -1:
                test = me[a] > 0
            else:
                continue
            ok = test if ok is None else jnp.logical_and(ok, test)
        return ok, where

    live = [
        i
        for i in range(1, 19)
        if all(sizes[a] > 1 or LAT[i][a] == 0 for a in range(3))
    ]

    def all_peer(k):
        rank = lax.rem((me[0] * ny + me[1]) * nz + me[2] + k, nx * ny * nz)
        return {
            "gx": rank // (ny * nz),
            "gy": lax.rem(rank // nz, ny),
            "gz": lax.rem(rank, nz),
        }

    def x_peer(k):
        return {"gx": lax.rem(me[0] + k, nx), "gy": me[1], "gz": me[2]}

    def yz_peer(k):
        rank = lax.rem(me[1] * nz + me[2] + k, ny * nz)
        return {"gx": me[0], "gy": rank // nz, "gz": lax.rem(rank, nz)}

    if len(sum_groups(sizes)) == 1:
        peers = [all_peer]
    else:
        peers = [x_peer, yz_peer]

    barrier = pltpu.get_barrier_semaphore()
    count = jnp.int32(sum(n - 1 for n in sum_groups(sizes)))
    for n, peer in zip(sum_groups(sizes), peers):
        for k in range(1, n):
            pl.semaphore_signal(barrier, inc=1, device_id=peer(k), device_id_type=MESH)
    if len(peers) > 1:
        for i in live:
            ok, where = reach(LAT[i], -1)

            @pl.when(ok)
            def _():
                pl.semaphore_signal(barrier, inc=1, device_id=where, device_id_type=MESH)

            count = count + reach(LAT[i], 1)[0].astype(jnp.int32)

    def landing(i, t):
        if i < 3:
            return xr.at[t, i - 1]
        if i < 5:
            return yr.at[t, i - 3]
        if i < 7:
            return zr.at[t, i - 5]
        return er.at[t, i - 7]

    def leaving(i, t):
        c = LAT[i]
        if i < 3:
            return xs.at[t, i - 1]
        if i < 5:
            return ys.at[t, i - 3]
        if i < 7:
            return zs.at[t, i - 5]
        if c[2] == 0:
            return ys.at[t, side(c[1]), SLOT[1][i]]
        return zs.at[t, side(c[2])]

    for i in range(1, 19):
        if i in live:

            @pl.when(jnp.logical_not(reach(LAT[i], 1)[0]))
            def _():
                for t in (0, 1):
                    ref = landing(i, t)
                    ref[...] = jnp.zeros(ref.shape, jnp.float32)

        else:
            for t in (0, 1):
                ref = landing(i, t)
                ref[...] = jnp.zeros(ref.shape, jnp.float32)

    lane = lax.broadcasted_iota(jnp.int32, (ey, ez), 1)
    row = lax.broadcasted_iota(jnp.int32, (ey, ez), 0)

    def hop(i, t):
        ok, where = reach(LAT[i], -1)
        copy = pltpu.make_async_remote_copy(
            src_ref=leaving(i, t),
            dst_ref=landing(i, t),
            send_sem=send_sem.at[t, i - 1],
            recv_sem=recv_sem.at[t, i - 1],
            device_id=where,
            device_id_type=MESH,
        )
        return ok, copy

    def pack_layer(t, x, tiles, packs):
        packs = list(packs)
        for sign in (1, -1):
            h = side(sign)
            if x == (0 if sign == 1 else ex - 1):
                for k, i in enumerate(group(0, sign)):
                    xs[t, h, k] = tiles(i)
            edge = 0 if sign == 1 else ey - 1
            for k, i in enumerate(group(1, sign)):
                ys[t, h, k, x : x + 1, :] = tiles(i)[edge : edge + 1, :]
            edge = 0 if sign == 1 else ez - 1
            for k, i in enumerate(group(2, sign)):
                at = k * ex + x
                moved = tiles(i)
                if (at - edge) % ez:
                    moved = pltpu.roll(moved, (at - edge) % ez, 1)
                packs[h] = jnp.where(lane == at, moved, packs[h])
        return tuple(packs)

    def send_all(t, packs):
        zs[t, 0] = packs[0]
        zs[t, 1] = packs[1]
        for i in sorted(live, key=lambda i: (LAT[i][0] == 0, -sum(map(abs, LAT[i])))):
            ok, copy = hop(i, t)
            pl.when(ok)(copy.start)

    def receive(t, along_x):
        for i in live:
            if (LAT[i][0] != 0) == along_x:
                ok = reach(LAT[i], 1)[0]
                pl.when(ok)(hop(i, t)[1].wait_recv)

    def shifted_columns(t):
        moved = {}
        for i in range(15, 19):
            cy, cz = LAT[i][1], LAT[i][2]
            pack = zr[t, side(cz)]
            src, last = (0, ey - 1) if cy == 1 else (ey - 1, 0)
            corner = er[t, i - 7, src : src + 1, :]
            pack = pltpu.roll(pack, (-cy) % ey, 0)
            moved[i] = jnp.where(row == last, corner, pack)
        return moved

    def pulled_tile(source, t, i, x, moved):
        cx, cy, cz = LAT[i]
        at = x + cx
        inside = 0 <= at < ex
        tile = source[i, at] if inside else xr[t, side(cx), SLOT[0][i]]
        if cy:
            h = side(cy)
            if inside:
                fill = yr[t, h, SLOT[1][i], at : at + 1, :]
            else:
                src = 0 if cx == 1 else ex - 1
                fill = er[t, i - 7, src : src + 1, :]
            last = ey - 1 if cy == 1 else 0
            tile = jnp.where(row == last, fill, pltpu.roll(tile, (-cy) % ey, 0))
        if cz:
            h = side(cz)
            col = SLOT[2][i] * ex
            if cy:
                pack, col = moved[i], col + x
            elif inside:
                pack, col = zr[t, h], col + at
            else:
                pack, col = er[t, i - 7], col + (0 if cx == 1 else ex - 1)
            last = ez - 1 if cz == 1 else 0
            if (last - col) % ez:
                pack = pltpu.roll(pack, (last - col) % ez, 1)
            tile = jnp.where(lane == last, pack, pltpu.roll(tile, (-cz) % ez, 1))
        return tile

    whole_x = nx * ex
    zero = jnp.zeros((ey, ez), jnp.float32)

    def step(t, source, target, packs):
        cost_sum, square_sum = zero, zero
        receive(t, False)
        moved = shifted_columns(t)
        for x in list(range(1, ex - 1)) + [0, ex - 1]:
            if x == 0:
                receive(t, True)
            g = des[x]
            solid = sol[x] == 1
            fluid = jnp.where(solid, 0.0, 1.0)
            kind = kin[x]
            inlet, outlet = kind == 1, kind == 2
            inner = jnp.logical_not(jnp.logical_or(inlet, outlet))
            below = 1.0 / (0.5 + 0.6 * g)
            damping = (0.1 + g) * below
            slope = 0.44 * (below * below)
            place = (me[0] * ex + x).astype(jnp.float32)
            weight = 1.0 + 2.0 * place / (whole_x - 1)
            f = [fwd[t, i, x] for i in range(19)]
            p = [pulled_tile(source, t, i, x, moved) for i in range(19)]
            out, sens, cost = cell_adjoint(
                f, p, damping, slope, fluid, solid, inner, inlet, outlet, weight
            )
            for i in range(19):
                target[i, x] = out[i]
            cost_sum = cost_sum + cost
            if t == 1:
                sens_ref[x] = sens
                packs = pack_layer(0, x, lambda i: out[i], packs)
            else:
                sens = sens + sens_ref[x]
                sens_ref[x] = sens
                square_sum = square_sum + sens * sens
        return cost_sum, square_sum, packs

    loads[0].wait()
    packs = (zero, zero)
    for x in range(ex):
        packs = pack_layer(1, x, lambda i: adj[i, x], packs)
    pl.semaphore_wait(barrier, count)
    send_all(1, packs)
    for load in loads[1:]:
        load.wait()
    cost_one, _, packs = step(1, adj, mid, (zero, zero))
    send_all(0, packs)
    cost_two, square, _ = step(0, mid, out_ref, None)

    half = ez // 2
    cost = jnp.sum(cost_one + cost_two, axis=0, keepdims=True)
    square = jnp.sum(square, axis=0, keepdims=True)
    cost = cost + pltpu.roll(cost, half, 1)
    square = square + pltpu.roll(square, half, 1)
    first = lax.broadcasted_iota(jnp.int32, (1, ez), 1) < half
    total = jnp.where(first, square, cost)

    sent = []
    for r, (n, peer) in enumerate(zip(sum_groups(sizes), peers)):
        part, got, send, recv = sum_refs[4 * r : 4 * r + 4]
        if n == 1:
            continue
        part[...] = total
        copies = []
        for k in range(1, n):
            copy = pltpu.make_async_remote_copy(
                src_ref=part,
                dst_ref=got.at[pl.ds(k - 1, 1)],
                send_sem=send.at[k - 1],
                recv_sem=recv.at[k - 1],
                device_id=peer(k),
                device_id_type=MESH,
            )
            copy.start()
            copies.append(copy)
        got[pl.ds(n - 1, 1)] = total
        for copy in copies:
            copy.wait_recv()
        total = jnp.sum(got[...], axis=0, keepdims=True)
        sent += copies
    tot_ref[0, 0:1, :] = jnp.where(first, total, 0.0)
    tot_ref[0, 1:2, :] = jnp.where(first, 0.0, total)
    for t in (1, 0):
        for i in live:
            ok, copy = hop(i, t)
            pl.when(ok)(copy.wait_send)
    for copy in sent:
        copy.wait_send()


def sum_rows():
    trace = (WROWS[4] + WROWS[5] + WROWS[6]) / 3
    along = WROWS[4] - trace
    across = (WROWS[5] - WROWS[6]) / 2
    assert np.allclose(WROWS[5], trace - along / 2 + across)
    rows = [WROWS[0], WROWS[1], WROWS[2], WROWS[3]]
    rows += [3 * trace, 3 * along, 3 * across, 3 * WROWS[7], 3 * WROWS[8], 3 * WROWS[9]]
    out = np.stack(rows)[:, :16]
    out[np.abs(out) < 1e-12] = 0.0
    return out


SUM_ROWS = sum_rows()


def plus(a, b):
    if a is None or b is None:
        return b if a is None else a
    return a + b


def minus(a, b):
    if b is None:
        return a
    return -b if a is None else a - b


def times(c, a):
    return None if a is None else c * a


def some_moments(p):
    s = {i: plus(p[i], p[i + 1]) for i in range(1, 19, 2)}
    d = {i: minus(p[i], p[i + 1]) for i in range(1, 19, 2)}
    sxy, sxz, syz = plus(s[7], s[9]), plus(s[11], s[13]), plus(s[15], s[17])
    axis_yz = plus(s[3], s[5])
    axis = plus(s[1], axis_yz)
    exy = plus(sxy, sxz)
    edge = plus(exy, syz)
    m = [None] * 19
    m[0] = plus(plus(p[0], axis), edge)
    m[1] = minus(minus(times(8.0, edge), times(11.0, axis)), times(30.0, p[0]))
    m[2] = plus(minus(edge, times(4.0, axis)), times(12.0, p[0]))
    a = minus(times(2.0, s[1]), axis_yz)
    b = minus(exy, times(2.0, syz))
    m[9] = plus(a, b)
    m[10] = minus(b, times(2.0, a))
    a = minus(s[3], s[5])
    b = minus(sxy, sxz)
    m[11] = plus(a, b)
    m[12] = minus(b, times(2.0, a))
    m[13] = minus(s[7], s[9])
    m[14] = minus(s[15], s[17])
    m[15] = minus(s[11], s[13])
    xa, xb = plus(d[7], d[9]), plus(d[11], d[13])
    ya, yb = minus(d[7], d[9]), plus(d[15], d[17])
    za, zb = minus(d[11], d[13]), minus(d[15], d[17])
    for k, axis_d, u, v in ((3, d[1], xa, xb), (5, d[3], ya, yb), (7, d[5], za, zb)):
        e = plus(u, v)
        m[k] = plus(axis_d, e)
        m[k + 1] = minus(e, times(4.0, axis_d))
    m[16] = minus(xa, xb)
    m[17] = minus(yb, ya)
    m[18] = minus(za, zb)
    return m


def cell_state(f, g, fluid, inlet, outlet, weight):
    s, d = flux_sums(f)
    rho = f[0]
    for i in s:
        rho = rho + s[i]
    fx = d[1] + (d[7] + d[9]) + (d[11] + d[13])
    fy = d[3] + (d[7] - d[9]) + (d[15] + d[17])
    fz = d[5] + (d[11] - d[13]) + (d[15] - d[17])
    below = 1.0 / (0.5 + 0.6 * g)
    damping = (0.1 + g) * below
    slope = 0.44 * (below * below)
    inv = 1.0 / rho
    b = [fx * inv, fy * inv, fz * inv]
    u = [c * damping for c in b]
    uu = u[0] * u[0] + u[1] * u[1] + u[2] * u[2]
    wr = weight * rho
    v = [jnp.where(inlet, c, a) for a, c in zip(u, (inflow_speed, 0.0, 0.0))]
    scale = jnp.where(inlet, 0.0, jnp.where(outlet, 3.0, 3.0 * rho))
    half = (0.5 * weight) * uu
    state = v + [wr * c for c in u] + b + [scale, damping * inv, half, fluid * slope]
    return state, fluid * (rho * half)


def cell_sums(m, state, inner, outlet):
    vx, vy, vz, wx, wy, wz, bx, by, bz, scale, di, half, slope = state
    n = [None] * 19
    for k in range(16):
        rate = float(np.float32(RATES[k]))
        n[k] = m[k] * jnp.where(inner, rate, 1.0) if np.any(SUM_ROWS[:, k]) else None
    s0, sx, sy, sz, trace, along, across, xy, yz, xz = [combine(r, n) for r in SUM_ROWS]
    xx = trace + along
    side_on = trace - 0.5 * along
    yy, zz = side_on + across, side_on - across
    ax = sx + (xx * vx + xy * vy + xz * vz) - s0 * vx
    ay = sy + (xy * vx + yy * vy + yz * vz) - s0 * vy
    az = sz + (xz * vx + yz * vy + zz * vz) - s0 * vz
    along_v = (ax + sx) * vx + (ay + sy) * vy + (az + sz) * vz
    rho_bar = jnp.where(outlet, 0.0, s0 + 1.5 * along_v) + half
    ux_bar, uy_bar, uz_bar = scale * ax + wx, scale * ay + wy, scale * az + wz
    d_bar = ux_bar * bx + uy_bar * by + uz_bar * bz
    extra = [rho_bar - d_bar * di, ux_bar * di, uy_bar * di, uz_bar * di]
    return extra, d_bar * slope


def cell_out(p, m, extra, inner, solid):
    z = [None] * 19
    for k in range(19):
        coef = float(np.float32((1.0 - RATES[k]) / NORMS[k]))
        z[k] = jnp.where(inner, coef * m[k], 0.0)
    for k, e in zip((0, 3, 5, 7), extra):
        z[k] = z[k] + e
    out = rebuild(z)
    return [jnp.where(solid, p[opposite_index[i]], out[i]) for i in range(19)]


def near(sizes, cells):
    nx, ny, nz = sizes
    ex, ey, _ = cells
    return ny == 2 and nz == 2 and nx * ny * nz <= 64 and ex == ey and ey % 8 == 0


def rounds(nx):
    return max((nx - 1) // 2, 0)


def end_rows(n, ey, faces):
    return 2 * (7 * ey + faces * (6 * ey + 1)) + 2 * (n - 1)


def fast_kernel(
    sizes,
    adj_hbm,
    fwd_hbm,
    des_hbm,
    sol_hbm,
    kind_hbm,
    out_ref,
    sens_ref,
    tot_ref,
    adj,
    fwd,
    des,
    marks,
    mid,
    pre,
    mom,
    xs,
    xe,
    ys,
    zs,
    xr,
    yr,
    zr,
    er,
    part,
    size_loads,
    size_sends,
    load_sem,
    send_sem,
    side_sem,
    face_sem,
    sum_sem,
    round_sem,
):
    ex, ey, ez = des.shape
    nx, ny, nz = sizes
    mx, my, mz = (lax.axis_index(name) for name in AXES)
    oy, oz = 1 - my, 1 - mz
    has = {1: mx < nx - 1, -1: mx > 0}
    far = {2: mx < nx - 2, -2: mx > 1}

    loads = [
        pltpu.make_async_copy(adj_hbm, adj, load_sem.at[0]),
        pltpu.make_async_copy(fwd_hbm, fwd, load_sem.at[1]),
        pltpu.make_async_copy(des_hbm, des, load_sem.at[1]),
        pltpu.make_async_copy(sol_hbm, marks.at[0], load_sem.at[1]),
        pltpu.make_async_copy(kind_hbm, marks.at[1], load_sem.at[1]),
    ]
    loads[0].start()

    barrier = pltpu.get_barrier_semaphore()

    def greet(x, y, z):
        pl.semaphore_signal(
            barrier, inc=1, device_id={"gx": x, "gy": y, "gz": z}, device_id_type=MESH
        )

    for y, z in ((my, oz), (oy, oz), (my, mz), (oy, mz)):
        for s in (1, -1):
            pl.when(has[s])(functools.partial(greet, mx + s, y, z))
    for y, z in ((my, oz), (oy, oz), (oy, mz)):
        greet(mx, y, z)
    for s in (2, -2):

        @pl.when(far[s])
        def _():
            greet(mx + s, my, mz)

    far_count = far[2].astype(jnp.int32) + far[-2].astype(jnp.int32)
    count = 3 + 4 * (has[1].astype(jnp.int32) + has[-1].astype(jnp.int32)) + far_count
    for load in loads[1:]:
        load.start()

    def tell(j):
        for s in (2, -2):

            @pl.when(far[s])
            def _():
                pl.semaphore_signal(
                    round_sem.at[j],
                    inc=1,
                    device_id={"gx": mx + s, "gy": my, "gz": mz},
                    device_id_type=MESH,
                )

    def hear(j):
        pl.semaphore_wait(round_sem.at[j], far_count)

    def relay(j):
        if j < rounds(nx):
            if j > 0:
                hear(j - 1)
            tell(j)

    def clear(ref):
        ref[...] = jnp.zeros(ref.shape, jnp.float32)

    for t in (0, 1):
        clear(yr.at[t, oy])
        clear(zr.at[t, oz])
        clear(er.at[t, oy, mz])
        clear(er.at[t, my, oz])
        clear(er.at[t, oy, oz])
    for s in (1, -1):

        @pl.when(jnp.logical_not(has[s]))
        def _():
            clear(xr.at[side(s)])

    lane = lax.broadcasted_iota(jnp.int32, (ey, ez), 1)
    row = lax.broadcasted_iota(jnp.int32, (ey, ez), 0)
    low_z = jnp.broadcast_to(mz == 1, (ey, ez))
    slot_lane = jnp.where(low_z, lane, jnp.where(lane == ez - 1, 0, lane + 1))
    match_y = [jnp.broadcast_to(my == h, (1, ez)) for h in (0, 1)]
    match_z = [jnp.broadcast_to(mz == h, (ey, ez)) for h in (0, 1)]

    def push(src, dst, sent, came, x, y, z):
        return pltpu.make_async_remote_copy(
            src_ref=src,
            dst_ref=dst,
            send_sem=sent,
            recv_sem=came,
            device_id={"gx": x, "gy": y, "gz": z},
            device_id_type=MESH,
        )

    def x_sends(t, turn):
        h = lax.rem(mx + turn, 2)
        sent, came, at = send_sem, face_sem.at[t], mx - 1 + 2 * h
        face, last = 5 * ey, 6 * ey
        tilted = pl.multiple_of((3 + jnp.where(h == 0, oz, mz)) * ey, 8)
        edge = xs.at[t, h, pl.ds(tilted, ey)]
        copies = [
            push(edge, xr.at[h, t, pl.ds(face, ey)], sent, came, at, my, oz),
            push(xs.at[t, h], xr.at[h, t, pl.ds(0, face)], sent, came, at, my, mz),
            push(xe.at[t, h, oy], xr.at[h, t, pl.ds(last, 1)], sent, came, at, oy, mz),
        ]
        return jnp.where(h == 0, mx > 0, mx < nx - 1), copies

    def side_sends(t):
        sent, came = send_sem, side_sem.at[t]
        return [
            push(zs.at[t], zr.at[t, oz], sent, came, mx, my, oz),
            push(zs.at[t], er.at[t, oy, oz], sent, came, mx, oy, oz),
            push(ys.at[t, oy], yr.at[t, oy], sent, came, mx, oy, mz),
        ]

    shifted = (1,)

    def store_face(t, x, tiles):
        for sign in (1, -1):
            h = side(sign)
            if x != (0 if sign == 1 else ex - 1):
                continue
            for k, i in enumerate(group(0, sign)):
                cy, cz = LAT[i][1:]
                sent = pltpu.roll(tiles(i), (-cz) % ez, 1) if cz and t in shifted else tiles(i)
                xs[t, h, k * ey : (k + 1) * ey, :] = sent
                if cy:
                    cut = 0 if cy == 1 else ey - 1
                    xe[t, h, side(cy)] = tiles(i)[cut : cut + 1, :]

    def pack_sides(t, x, tiles, pack):
        for sign in (1, -1):
            h = side(sign)
            edge = 0 if sign == 1 else ey - 1
            for k, i in enumerate(group(1, sign)):
                ys[t, h, k, x : x + 1, :] = tiles(i)[edge : edge + 1, :]
        for k, (i, j) in enumerate(zip(group(2, 1), group(2, -1))):
            at = k * ex + x
            moved = jnp.where(low_z, tiles(i), tiles(j))
            if at % ez:
                moved = pltpu.roll(moved, at % ez, 1)
            pack = jnp.where(slot_lane == at, moved, pack)
        return pack

    def send_faces(t):
        for turn in (0, 1):
            ok, copies = x_sends(t, turn)

            @pl.when(ok)
            def _():
                for copy in copies:
                    copy.start()

    def send_sides(t, pack):
        zs[t] = pack
        for copy in side_sends(t):
            copy.start()

    def await_bytes(ref, sem):
        pltpu.make_async_copy(ref, ref, sem).wait()

    def receive_sides(t):
        await_bytes(xr.at[0, t], side_sem.at[t])

    both = jnp.logical_and(has[1], has[-1])

    def receive_faces(t):
        rows = pl.ds(0, 6 * ey + 1)

        @pl.when(both)
        def _():
            await_bytes(xr.at[:, t, rows], face_sem.at[t])

        if nx > 1:

            @pl.when(jnp.logical_not(both))
            def _():
                await_bytes(xr.at[0, t, rows], face_sem.at[t])

    def shifted_columns(t):
        moved = {}
        for i in range(15, 19):
            cy, cz = LAT[i][1], LAT[i][2]
            pack = zr[t, side(cz)]
            src, last = (0, ey - 1) if cy == 1 else (ey - 1, 0)
            corner = er[t, side(cy), side(cz), src : src + 1, :]
            pack = pltpu.roll(pack, (-cy) % ey, 0)
            moved[i] = jnp.where(row == last, corner, pack)
        return moved

    def pulled_tile(source, t, i, x, moved):
        cx, cy, cz = LAT[i]
        at = x + cx
        inside = 0 <= at < ex
        if inside:
            tile = source[i, at]
        else:
            k = SLOT[0][i] * ey
            tile = xr[side(cx), t, k : k + ey, :]
        src = 0 if cx == 1 else ex - 1
        if cy:
            h = side(cy)
            if inside:
                fill = yr[t, h, SLOT[1][i], at : at + 1, :]
            else:
                fill = xr[side(cx), t, 6 * ey : 6 * ey + 1, :]
                fill = jnp.where(match_y[h], fill, 0.0)
            last = ey - 1 if cy == 1 else 0
            tile = jnp.where(row == last, fill, pltpu.roll(tile, (-cy) % ey, 0))
        if cz:
            h = side(cz)
            last = ez - 1 if cz == 1 else 0
            if not inside:
                pack = xr[side(cx), t, 5 * ey : 6 * ey, :]
                pack = jnp.where(match_z[h], pack, 0.0)
                if t in shifted:
                    return jnp.where(lane == last, pack, tile)
                tile = jnp.where(lane == ez - 1 - last, pack, tile)
                return pltpu.roll(tile, (-cz) % ez, 1)
            col = SLOT[2][i] * ex - h
            if cy:
                pack, col = moved[i], col + x
            else:
                pack, col = zr[t, h], col + at
            if (last - col) % ez:
                pack = pltpu.roll(pack, (last - col) % ez, 1)
            tile = jnp.where(lane == last, pack, pltpu.roll(tile, (-cz) % ez, 1))
        return tile

    whole_x = nx * ex
    zero = jnp.zeros((ey, ez), jnp.float32)

    def marked(x):
        kind = marks[1, x]
        return kind == 0, kind == 1, kind == 2, marks[0, x] == 1

    def prepare(t):
        total = zero
        for x in range(ex):
            _, inlet, outlet, solid = marked(x)
            fluid = jnp.where(solid, 0.0, 1.0)
            place = (mx * ex + x).astype(jnp.float32)
            weight = 1.0 + 2.0 * place / (whole_x - 1)
            f = [fwd[t, i, x] for i in range(19)]
            state, cost = cell_state(f, des[x], fluid, inlet, outlet, weight)
            for q, value in enumerate(state):
                pre[q, x] = value
            total = total + cost
        return total

    def is_late(i, x):
        return not 0 <= x + LAT[i][0] < ex

    def sums_of(m, x):
        inner, _, outlet, _ = marked(x)
        return cell_sums(m, [pre[q, x] for q in range(13)], inner, outlet)

    edges = sorted({0, ex - 1})
    inner_planes = range(1, ex - 1)

    def pull(t, source, done):
        receive_sides(t)
        if t == 1:
            relay(1)
        moved = shifted_columns(t)
        for x in inner_planes:
            p = [pulled_tile(source, t, i, x, moved) for i in range(19)]
            done(x, p, some_moments(p))
        early = {}
        for x in edges:
            p = [
                None if is_late(i, x) else pulled_tile(source, t, i, x, moved)
                for i in range(19)
            ]
            early[x] = p, some_moments(p)
        with jax.named_scope(f"faces {t}"):
            receive_faces(t)
        for x in edges:
            p, m = early[x]
            late = [
                pulled_tile(source, t, i, x, moved) if is_late(i, x) else None
                for i in range(19)
            ]
            p = [b if a is None else a for a, b in zip(p, late)]
            done(x, p, [plus(a, b) for a, b in zip(m, some_moments(late))])

    with jax.named_scope("load"):
        loads[0].wait()
    for x in edges:
        store_face(1, x, lambda i: adj[i, x])
    with jax.named_scope("greeted"):
        pl.semaphore_wait(barrier, count)
    with jax.named_scope("send 1"):
        send_faces(1)
    pack = zero
    for x in range(ex):
        pack = pack_sides(1, x, lambda i: adj[i, x], pack)
    with jax.named_scope("sides 1"):
        send_sides(1, pack)
        relay(0)
    await_bytes(size_loads, load_sem.at[1])
    cost = prepare(1)
    packs = [zero]
    kept = {}

    def keep(x, out, sens):
        for i in range(19):
            mid[i, x] = out[i]
        sens_ref[x] = sens
        packs[0] = pack_sides(0, x, lambda i: out[i], packs[0])

    def first_done(x, p, m):
        inner, _, _, solid = marked(x)
        extra, sens = sums_of(m, x)
        out = cell_out(p, m, extra, inner, solid)
        if x in edges:
            store_face(0, x, lambda i: out[i])
            kept[x] = out, sens
        else:
            keep(x, out, sens)

    with jax.named_scope("step 1"):
        pull(1, adj, first_done)
    with jax.named_scope("send 0"):
        send_faces(0)
    for x, (out, sens) in kept.items():
        keep(x, out, sens)
    with jax.named_scope("sides 0"):
        send_sides(0, packs[0])
    for j in range(2, rounds(nx)):
        relay(j)
    cost = cost + prepare(0)
    squares = [zero]

    def second_done(x, p, m):
        extra, sens = sums_of(m, x)
        sens = sens + sens_ref[x]
        sens_ref[x] = sens
        squares[0] = squares[0] + sens * sens
        for i in range(19):
            adj[i, x] = p[i]
        for k, value in enumerate(m + extra):
            mom[k, x] = value

    with jax.named_scope("step 0"):
        pull(0, mid, second_done)
    part[0:1, :] = jnp.sum(squares[0], axis=0, keepdims=True)
    part[1:2, :] = jnp.sum(cost, axis=0, keepdims=True)

    with jax.named_scope("heard"):
        if rounds(nx):
            hear(rounds(nx) - 1)
    n = nx * ny * nz

    def sum_send(k, x, y, z):
        return push(part, tot_ref.at[k - 1], send_sem, sum_sem, x, y, z)

    with jax.named_scope("send sums"):
        for px in range(nx):
            dx = jnp.where(px < mx, px - mx + nx, px - mx)
            for dy, dz in ((0, 1), (1, 1), (0, 0), (1, 0)):
                k = (dx * ny + dy) * nz + dz
                y, z = (oy if dy else my), (oz if dz else mz)
                if dy or dz:
                    sum_send(k, px, y, z).start()
                else:
                    pl.when(px != mx)(sum_send(k, px, y, z).start)
    tot_ref[n - 1] = part[...]
    with jax.named_scope("out"):
        for x in range(ex):
            inner, _, _, solid = marked(x)
            m = [mom[k, x] for k in range(23)]
            out = cell_out([adj[i, x] for i in range(19)], m[:19], m[19:], inner, solid)
            for i in range(19):
                out_ref[i, x] = out[i]
    with jax.named_scope("sums"):
        await_bytes(tot_ref.at[pl.ds(0, n - 1)], sum_sem)
    with jax.named_scope("drain"):

        @pl.when(both)
        def _():
            await_bytes(size_sends, send_sem)

        @pl.when(jnp.logical_not(both))
        def _():
            await_bytes(size_sends.at[pl.ds(0, end_rows(n, ey, nx > 1))], send_sem)


def hand_on(
    cells,
    adj_in,
    sens_in,
    sums_in,
    adj_out,
    sens_out,
    obj_out,
    rms_out,
    sens,
    obj,
    rms,
    sem,
):
    moves = [(adj_in, adj_out), (sens, sens_out), (obj, obj_out), (rms, rms_out)]
    copies = [pltpu.make_async_copy(a, b, sem.at[k]) for k, (a, b) in enumerate(moves)]
    copies[0].start()
    total = jnp.sum(jnp.sum(sums_in[...], axis=0), axis=1, keepdims=True) / cells
    root = jnp.sqrt(total[0:1] + 1e-06)
    scale = jnp.broadcast_to(1.0 / root, sens.shape[1:])
    for x in range(sens.shape[0]):
        sens[x] = sens_in[x] * scale
    copies[1].start()
    obj[0] = total[1, 0]
    rms[0] = root[0, 0]
    copies[2].start()
    copies[3].start()
    for copy in copies:
        copy.wait()


def body(sizes, adjoint_in, forward_states, design, solid_mask, boundary_kind):
    ex, ey, ez = design.shape
    nx, ny, nz = sizes
    any_spec = pl.BlockSpec(memory_space=pltpu.HBM)
    vmem_spec = pl.BlockSpec(memory_space=pltpu.VMEM)
    f32 = jnp.float32
    operands = (adjoint_in, forward_states, design, solid_mask, boundary_kind)
    operands = [pltpu.with_memory_space_constraint(a, pltpu.HBM) for a in operands]
    if near(sizes, design.shape):
        n = nx * ny * nz
        entries = n
        count = adjoint_in.shape[0]
        run = fast_kernel
        scratch = [
            pltpu.VMEM(adjoint_in.shape, f32),
            pltpu.VMEM(forward_states.shape, f32),
            pltpu.VMEM(design.shape, f32),
            pltpu.VMEM((2, *design.shape), jnp.int32),
            pltpu.VMEM(adjoint_in.shape, f32),
            pltpu.VMEM((13, *design.shape), f32),
            pltpu.VMEM((23, *design.shape), f32),
            pltpu.VMEM((2, 2, 5 * ey, ez), f32),
            pltpu.VMEM((2, 2, 2, 1, ez), f32),
            pltpu.VMEM((2, 2, 5, ex, ez), f32),
            pltpu.VMEM((2, ey, ez), f32),
            pltpu.VMEM((2, 2, 7 * ey, ez), f32),
            pltpu.VMEM((2, 2, 5, ex, ez), f32),
            pltpu.VMEM((2, 2, ey, ez), f32),
            pltpu.VMEM((2, 2, 2, ey, ez), f32),
            pltpu.VMEM((2, ez), f32),
            pltpu.VMEM((2 * count + 3, *design.shape), f32),
            pltpu.VMEM((end_rows(n, ey, 2), ez), f32),
            pltpu.SemaphoreType.DMA((2,)),
            pltpu.SemaphoreType.DMA,
            pltpu.SemaphoreType.DMA((2,)),
            pltpu.SemaphoreType.DMA((2,)),
            pltpu.SemaphoreType.DMA,
            pltpu.SemaphoreType.REGULAR((max(rounds(nx), 1),)),
        ]
    else:
        entries = 1
        run = general_kernel
        sum_scratch = []
        for n in sum_groups(sizes):
            sum_scratch += [
                pltpu.VMEM((1, ez), f32),
                pltpu.VMEM((n, ez), f32),
                pltpu.SemaphoreType.DMA((max(n - 1, 1),)),
                pltpu.SemaphoreType.DMA((max(n - 1, 1),)),
            ]
        scratch = [
            pltpu.VMEM(adjoint_in.shape, f32),
            pltpu.VMEM(forward_states.shape, f32),
            pltpu.VMEM(design.shape, f32),
            pltpu.VMEM(design.shape, jnp.int32),
            pltpu.VMEM(design.shape, jnp.int32),
            pltpu.VMEM(adjoint_in.shape, f32),
            pltpu.VMEM((2, 2, 5, ey, ez), f32),
            pltpu.VMEM((2, 2, 5, ex, ez), f32),
            pltpu.VMEM((2, 2, ey, ez), f32),
            pltpu.VMEM((2, 2, 5, ey, ez), f32),
            pltpu.VMEM((2, 2, 5, ex, ez), f32),
            pltpu.VMEM((2, 2, ey, ez), f32),
            pltpu.VMEM((2, 12, ey, ez), f32),
            pltpu.SemaphoreType.DMA((6,)),
            pltpu.SemaphoreType.DMA,
            pltpu.SemaphoreType.DMA((2, 18)),
            pltpu.SemaphoreType.DMA((2, 18)),
            *sum_scratch,
        ]
    adjoint, sens, tot = pl.pallas_call(
        functools.partial(run, sizes),
        out_shape=(
            jax.ShapeDtypeStruct(adjoint_in.shape, f32),
            jax.ShapeDtypeStruct(design.shape, f32),
            jax.ShapeDtypeStruct((entries, 2, ez), f32),
        ),
        in_specs=[any_spec] * 5,
        out_specs=(vmem_spec, vmem_spec, vmem_spec),
        scratch_shapes=scratch,
        compiler_params=pltpu.CompilerParams(
            collective_id=0, has_side_effects=True, vmem_limit_bytes=VMEM_LIMIT
        ),
    )(*operands)
    adjoint, sens, objective, rms = pl.pallas_call(
        functools.partial(hand_on, nx * ex * ny * ey * nz * ez),
        out_shape=(
            jax.ShapeDtypeStruct(adjoint_in.shape, f32),
            jax.ShapeDtypeStruct(design.shape, f32),
            jax.ShapeDtypeStruct((1,), f32),
            jax.ShapeDtypeStruct((1,), f32),
        ),
        in_specs=[vmem_spec] * 3,
        out_specs=(any_spec, any_spec, any_spec, any_spec),
        scratch_shapes=[
            pltpu.VMEM(design.shape, f32),
            pltpu.SMEM((1,), f32),
            pltpu.SMEM((1,), f32),
            pltpu.SemaphoreType.DMA((4,)),
        ],
        compiler_params=pltpu.CompilerParams(vmem_limit_bytes=VMEM_LIMIT),
    )(adjoint, sens, tot)
    return adjoint, sens, objective.reshape(()), rms.reshape(())


def solution(mesh):
    placed = (
        P(None, "gx", "gy", "gz"),
        P(None, None, "gx", "gy", "gz"),
        P("gx", "gy", "gz"),
        P("gx", "gy", "gz"),
        P("gx", "gy", "gz"),
    )
    return jax.shard_map(
        functools.partial(body, tuple(int(mesh.shape[name]) for name in AXES)),
        mesh=mesh,
        in_specs=placed,
        out_specs=(P(None, "gx", "gy", "gz"), P("gx", "gy", "gz"), P(), P()),
        check_vma=False,
    )
```

```python
import functools

import jax
import jax.numpy as jnp
import numpy as np
from jax import lax
from jax.experimental import pallas as pl
from jax.experimental.pallas import tpu as pltpu
from jax.sharding import PartitionSpec as P

MESH = pl.DeviceIdType.MESH
lattice_table = np.array(
    [
        [0, 0, 0],
        [1, 0, 0],
        [-1, 0, 0],
        [0, 1, 0],
        [0, -1, 0],
        [0, 0, 1],
        [0, 0, -1],
        [1, 1, 0],
        [-1, -1, 0],
        [1, -1, 0],
        [-1, 1, 0],
        [1, 0, 1],
        [-1, 0, -1],
        [1, 0, -1],
        [-1, 0, 1],
        [0, 1, 1],
        [0, -1, -1],
        [0, 1, -1],
        [0, -1, 1],
    ],
    dtype=np.int32,
)
LAT = [tuple(int(v) for v in row) for row in lattice_table]
WEIGHTS = np.array([1.0 / 3] + [1.0 / 18] * 6 + [1.0 / 36] * 12, dtype=np.float64)
opposite_index = [0, 2, 1, 4, 3, 6, 5, 8, 7, 10, 9, 12, 11, 14, 13, 16, 15, 18, 17]
inflow_speed = 0.08
AXES = ("gx", "gy", "gz")
VMEM_LIMIT = 16000 * 1024


def moment_rows():
    c = lattice_table.astype(np.float64)
    cx, cy, cz = c[:, 0], c[:, 1], c[:, 2]
    csq = cx * cx + cy * cy + cz * cz
    return np.stack(
        [
            np.ones(19),
            19 * csq - 30,
            (21 * csq * csq - 53 * csq + 24) / 2,
            cx,
            (5 * csq - 9) * cx,
            cy,
            (5 * csq - 9) * cy,
            cz,
            (5 * csq - 9) * cz,
            3 * cx * cx - csq,
            (3 * csq - 5) * (3 * cx * cx - csq),
            cy * cy - cz * cz,
            (3 * csq - 5) * (cy * cy - cz * cz),
            cx * cy,
            cy * cz,
            cx * cz,
            (cy * cy - cz * cz) * cx,
            (cz * cz - cx * cx) * cy,
            (cx * cx - cy * cy) * cz,
        ]
    )


ROWS = moment_rows()
NORMS = np.sum(ROWS * ROWS, axis=1)
SHEAR = 1.0 / 0.6
RATES = [0, 1.19, 1.4, 0, 1.2, 0, 1.2, 0, 1.2, SHEAR, 1.4, SHEAR, 1.4, SHEAR, SHEAR, SHEAR]
RATES = np.array(RATES + [1.98, 1.98, 1.98], dtype=np.float64)


def weighted_rows():
    c = lattice_table.astype(np.float64)
    pairs = [(0, 0), (1, 1), (2, 2), (0, 1), (1, 2), (0, 2)]
    rows = [WEIGHTS] + [WEIGHTS * c[:, a] for a in range(3)]
    rows += [WEIGHTS * c[:, a] * c[:, b] for a, b in pairs]
    out = np.stack(rows) @ (ROWS / NORMS[:, None]).T
    out[np.abs(out) < 1e-12] = 0.0
    return out


WROWS = weighted_rows()


def group(column, sign):
    return [i for i in range(19) if LAT[i][column] == sign]


SLOT = [{i: k for s in (1, -1) for k, i in enumerate(group(col, s))} for col in range(3)]


def side(sign):
    return 0 if sign == 1 else 1


def combine(coefs, terms):
    total = None
    for coef, term in zip(coefs, terms):
        if coef == 0.0:
            continue
        part = term if coef == 1.0 else float(np.float32(coef)) * term
        total = part if total is None else total + part
    return total


def flux_sums(f):
    s = {i: f[i] + f[i + 1] for i in range(1, 19, 2)}
    d = {i: f[i] - f[i + 1] for i in range(1, 19, 2)}
    return s, d


def moments(p):
    s, d = flux_sums(p)
    sxy, sxz, syz = s[7] + s[9], s[11] + s[13], s[15] + s[17]
    axis_yz = s[3] + s[5]
    axis = s[1] + axis_yz
    exy = sxy + sxz
    edge = exy + syz
    m = [None] * 19
    m[0] = p[0] + axis + edge
    m[1] = 8.0 * edge - 11.0 * axis - 30.0 * p[0]
    m[2] = edge - 4.0 * axis + 12.0 * p[0]
    a = 2.0 * s[1] - axis_yz
    b = exy - 2.0 * syz
    m[9] = a + b
    m[10] = b - 2.0 * a
    a = s[3] - s[5]
    b = sxy - sxz
    m[11] = a + b
    m[12] = b - 2.0 * a
    m[13] = s[7] - s[9]
    m[14] = s[15] - s[17]
    m[15] = s[11] - s[13]
    xa, xb = d[7] + d[9], d[11] + d[13]
    ya, yb = d[7] - d[9], d[15] + d[17]
    za, zb = d[11] - d[13], d[15] - d[17]
    for k, axis_d, u, v in ((3, d[1], xa, xb), (5, d[3], ya, yb), (7, d[5], za, zb)):
        e = u + v
        m[k] = axis_d + e
        m[k + 1] = e - 4.0 * axis_d
    m[16] = xa - xb
    m[17] = yb - ya
    m[18] = za - zb
    return m


def rebuild(z):
    out = [None] * 19
    out[0] = z[0] - 30.0 * z[1] + 12.0 * z[2]
    axis = z[0] - 11.0 * z[1] - 4.0 * z[2]
    edge = z[0] + 8.0 * z[1] + z[2]
    px = z[9] - 2.0 * z[10]
    pw = z[11] - 2.0 * z[12]
    qx = z[9] + z[10]
    qw = z[11] + z[12]
    ayz = axis - px
    eyz = edge - 2.0 * qx
    exx = edge + qx
    exy, exz = exx + qw, exx - qw
    jx, jy, jz = z[3] + z[4], z[5] + z[6], z[7] + z[8]
    x1, x2 = jx + z[16], jx - z[16]
    y1, y2 = jy - z[17], jy + z[17]
    z1, z2 = jz + z[18], jz - z[18]
    even = {
        1: axis + 2.0 * px,
        3: ayz + pw,
        5: ayz - pw,
        7: exy + z[13],
        9: exy - z[13],
        11: exz + z[15],
        13: exz - z[15],
        15: eyz + z[14],
        17: eyz - z[14],
    }
    odd = {
        1: z[3] - 4.0 * z[4],
        3: z[5] - 4.0 * z[6],
        5: z[7] - 4.0 * z[8],
        7: x1 + y1,
        9: x1 - y1,
        11: x2 + z1,
        13: x2 - z1,
        15: y2 + z2,
        17: y2 - z2,
    }
    for i in even:
        out[i] = even[i] + odd[i]
        out[i + 1] = even[i] - odd[i]
    return out


def cell_adjoint(f, p, damping, slope, fluid, solid, inner, inlet, outlet, weight):
    s, d = flux_sums(f)
    rho = f[0]
    for i in s:
        rho = rho + s[i]
    fx = d[1] + (d[7] + d[9]) + (d[11] + d[13])
    fy = d[3] + (d[7] - d[9]) + (d[15] + d[17])
    fz = d[5] + (d[11] - d[13]) + (d[15] - d[17])
    inv = 1.0 / rho
    bx, by, bz = fx * inv, fy * inv, fz * inv
    ux, uy, uz = bx * damping, by * damping, bz * damping
    uu = ux * ux + uy * uy + uz * uz
    m = moments(p)
    n = [None] * 19
    for k in range(16):
        rate = float(np.float32(RATES[k]))
        n[k] = m[k] * jnp.where(inner, rate, 1.0) if np.any(WROWS[:, k]) else None
    s0, sx, sy, sz, xx, yy, zz, xy, yz, xz = [
        combine(WROWS[r, :16], n) for r in range(10)
    ]
    vx = jnp.where(inlet, inflow_speed, ux)
    vy = jnp.where(inlet, 0.0, uy)
    vz = jnp.where(inlet, 0.0, uz)
    gx = xx * vx + xy * vy + xz * vz
    gy = xy * vx + yy * vy + yz * vz
    gz = xz * vx + yz * vy + zz * vz
    vv = vx * vx + vy * vy + vz * vz
    rho_bar = (
        s0 * (1.0 - 1.5 * vv)
        + 3.0 * (sx * vx + sy * vy + sz * vz)
        + 4.5 * (gx * vx + gy * vy + gz * vz)
    )
    rho_bar = jnp.where(outlet, 0.0, rho_bar) + (0.5 * weight) * uu
    scale = jnp.where(inlet, 0.0, jnp.where(outlet, 1.0, rho))
    wr = weight * rho
    ux_bar = scale * (3.0 * sx + 9.0 * gx - 3.0 * s0 * vx) + wr * ux
    uy_bar = scale * (3.0 * sy + 9.0 * gy - 3.0 * s0 * vy) + wr * uy
    uz_bar = scale * (3.0 * sz + 9.0 * gz - 3.0 * s0 * vz) + wr * uz
    d_bar = ux_bar * bx + uy_bar * by + uz_bar * bz
    di = damping * inv
    rho_bar = rho_bar - d_bar * di
    z = [None] * 19
    for k in range(19):
        coef = (1.0 - RATES[k]) / NORMS[k]
        z[k] = jnp.where(inner, float(np.float32(coef)) * m[k], 0.0)
    z[0] = z[0] + rho_bar
    z[3] = z[3] + ux_bar * di
    z[5] = z[5] + uy_bar * di
    z[7] = z[7] + uz_bar * di
    out = rebuild(z)
    out = [jnp.where(solid, p[opposite_index[i]], out[i]) for i in range(19)]
    sens = fluid * (d_bar * slope)
    cost = fluid * (0.5 * wr * uu)
    return out, sens, cost


def sum_groups(sizes):
    nx, ny, nz = sizes
    return [nx * ny * nz] if nx * ny * nz <= 64 else [nx, ny * nz]


def general_kernel(
    sizes,
    adj_hbm,
    fwd_hbm,
    des_hbm,
    sol_hbm,
    kind_hbm,
    out_ref,
    sens_ref,
    tot_ref,
    adj,
    fwd,
    des,
    sol,
    kin,
    mid,
    xs,
    ys,
    zs,
    xr,
    yr,
    zr,
    er,
    load_sem,
    store_sem,
    send_sem,
    recv_sem,
    *sum_refs,
):
    ex, ey, ez = des.shape
    me = tuple(lax.axis_index(name) for name in AXES)
    nx, ny, nz = sizes

    loads = [
        pltpu.make_async_copy(adj_hbm, adj, load_sem.at[0]),
        pltpu.make_async_copy(fwd_hbm.at[1], fwd.at[1], load_sem.at[1]),
        pltpu.make_async_copy(des_hbm, des, load_sem.at[2]),
        pltpu.make_async_copy(sol_hbm, sol, load_sem.at[3]),
        pltpu.make_async_copy(kind_hbm, kin, load_sem.at[4]),
        pltpu.make_async_copy(fwd_hbm.at[0], fwd.at[0], load_sem.at[5]),
    ]
    for load in loads:
        load.start()

    def reach(offset, sign):
        ok = None
        where = {}
        for a in range(3):
            c = sign * offset[a]
            where[AXES[a]] = me[a] + c if c else me[a]
            if c == 1:
                test = me[a] < sizes[a] - 1
            elif c == -1:
                test = me[a] > 0
            else:
                continue
            ok = test if ok is None else jnp.logical_and(ok, test)
        return ok, where

    live = [
        i
        for i in range(1, 19)
        if all(sizes[a] > 1 or LAT[i][a] == 0 for a in range(3))
    ]

    def all_peer(k):
        rank = lax.rem((me[0] * ny + me[1]) * nz + me[2] + k, nx * ny * nz)
        return {
            "gx": rank // (ny * nz),
            "gy": lax.rem(rank // nz, ny),
            "gz": lax.rem(rank, nz),
        }

    def x_peer(k):
        return {"gx": lax.rem(me[0] + k, nx), "gy": me[1], "gz": me[2]}

    def yz_peer(k):
        rank = lax.rem(me[1] * nz + me[2] + k, ny * nz)
        return {"gx": me[0], "gy": rank // nz, "gz": lax.rem(rank, nz)}

    if len(sum_groups(sizes)) == 1:
        peers = [all_peer]
    else:
        peers = [x_peer, yz_peer]

    barrier = pltpu.get_barrier_semaphore()
    count = jnp.int32(sum(n - 1 for n in sum_groups(sizes)))
    for n, peer in zip(sum_groups(sizes), peers):
        for k in range(1, n):
            pl.semaphore_signal(barrier, inc=1, device_id=peer(k), device_id_type=MESH)
    if len(peers) > 1:
        for i in live:
            ok, where = reach(LAT[i], -1)

            @pl.when(ok)
            def _():
                pl.semaphore_signal(barrier, inc=1, device_id=where, device_id_type=MESH)

            count = count + reach(LAT[i], 1)[0].astype(jnp.int32)

    def landing(i, t):
        if i < 3:
            return xr.at[t, i - 1]
        if i < 5:
            return yr.at[t, i - 3]
        if i < 7:
            return zr.at[t, i - 5]
        return er.at[t, i - 7]

    def leaving(i, t):
        c = LAT[i]
        if i < 3:
            return xs.at[t, i - 1]
        if i < 5:
            return ys.at[t, i - 3]
        if i < 7:
            return zs.at[t, i - 5]
        if c[2] == 0:
            return ys.at[t, side(c[1]), SLOT[1][i]]
        return zs.at[t, side(c[2])]

    for i in range(1, 19):
        if i in live:

            @pl.when(jnp.logical_not(reach(LAT[i], 1)[0]))
            def _():
                for t in (0, 1):
                    ref = landing(i, t)
                    ref[...] = jnp.zeros(ref.shape, jnp.float32)

        else:
            for t in (0, 1):
                ref = landing(i, t)
                ref[...] = jnp.zeros(ref.shape, jnp.float32)

    lane = lax.broadcasted_iota(jnp.int32, (ey, ez), 1)
    row = lax.broadcasted_iota(jnp.int32, (ey, ez), 0)

    def hop(i, t):
        ok, where = reach(LAT[i], -1)
        copy = pltpu.make_async_remote_copy(
            src_ref=leaving(i, t),
            dst_ref=landing(i, t),
            send_sem=send_sem.at[t, i - 1],
            recv_sem=recv_sem.at[t, i - 1],
            device_id=where,
            device_id_type=MESH,
        )
        return ok, copy

    def pack_layer(t, x, tiles, packs):
        packs = list(packs)
        for sign in (1, -1):
            h = side(sign)
            if x == (0 if sign == 1 else ex - 1):
                for k, i in enumerate(group(0, sign)):
                    xs[t, h, k] = tiles(i)
            edge = 0 if sign == 1 else ey - 1
            for k, i in enumerate(group(1, sign)):
                ys[t, h, k, x : x + 1, :] = tiles(i)[edge : edge + 1, :]
            edge = 0 if sign == 1 else ez - 1
            for k, i in enumerate(group(2, sign)):
                at = k * ex + x
                moved = tiles(i)
                if (at - edge) % ez:
                    moved = pltpu.roll(moved, (at - edge) % ez, 1)
                packs[h] = jnp.where(lane == at, moved, packs[h])
        return tuple(packs)

    def send_all(t, packs):
        zs[t, 0] = packs[0]
        zs[t, 1] = packs[1]
        for i in sorted(live, key=lambda i: (LAT[i][0] == 0, -sum(map(abs, LAT[i])))):
            ok, copy = hop(i, t)
            pl.when(ok)(copy.start)

    def receive(t, along_x):
        for i in live:
            if (LAT[i][0] != 0) == along_x:
                ok = reach(LAT[i], 1)[0]
                pl.when(ok)(hop(i, t)[1].wait_recv)

    def shifted_columns(t):
        moved = {}
        for i in range(15, 19):
            cy, cz = LAT[i][1], LAT[i][2]
            pack = zr[t, side(cz)]
            src, last = (0, ey - 1) if cy == 1 else (ey - 1, 0)
            corner = er[t, i - 7, src : src + 1, :]
            pack = pltpu.roll(pack, (-cy) % ey, 0)
            moved[i] = jnp.where(row == last, corner, pack)
        return moved

    def pulled_tile(source, t, i, x, moved):
        cx, cy, cz = LAT[i]
        at = x + cx
        inside = 0 <= at < ex
        tile = source[i, at] if inside else xr[t, side(cx), SLOT[0][i]]
        if cy:
            h = side(cy)
            if inside:
                fill = yr[t, h, SLOT[1][i], at : at + 1, :]
            else:
                src = 0 if cx == 1 else ex - 1
                fill = er[t, i - 7, src : src + 1, :]
            last = ey - 1 if cy == 1 else 0
            tile = jnp.where(row == last, fill, pltpu.roll(tile, (-cy) % ey, 0))
        if cz:
            h = side(cz)
            col = SLOT[2][i] * ex
            if cy:
                pack, col = moved[i], col + x
            elif inside:
                pack, col = zr[t, h], col + at
            else:
                pack, col = er[t, i - 7], col + (0 if cx == 1 else ex - 1)
            last = ez - 1 if cz == 1 else 0
            if (last - col) % ez:
                pack = pltpu.roll(pack, (last - col) % ez, 1)
            tile = jnp.where(lane == last, pack, pltpu.roll(tile, (-cz) % ez, 1))
        return tile

    whole_x = nx * ex
    zero = jnp.zeros((ey, ez), jnp.float32)

    def step(t, source, target, packs):
        cost_sum, square_sum = zero, zero
        receive(t, False)
        moved = shifted_columns(t)
        for x in list(range(1, ex - 1)) + [0, ex - 1]:
            if x == 0:
                receive(t, True)
            g = des[x]
            solid = sol[x] == 1
            fluid = jnp.where(solid, 0.0, 1.0)
            kind = kin[x]
            inlet, outlet = kind == 1, kind == 2
            inner = jnp.logical_not(jnp.logical_or(inlet, outlet))
            below = 1.0 / (0.5 + 0.6 * g)
            damping = (0.1 + g) * below
            slope = 0.44 * (below * below)
            place = (me[0] * ex + x).astype(jnp.float32)
            weight = 1.0 + 2.0 * place / (whole_x - 1)
            f = [fwd[t, i, x] for i in range(19)]
            p = [pulled_tile(source, t, i, x, moved) for i in range(19)]
            out, sens, cost = cell_adjoint(
                f, p, damping, slope, fluid, solid, inner, inlet, outlet, weight
            )
            for i in range(19):
                target[i, x] = out[i]
            cost_sum = cost_sum + cost
            if t == 1:
                sens_ref[x] = sens
                packs = pack_layer(0, x, lambda i: out[i], packs)
            else:
                sens = sens + sens_ref[x]
                sens_ref[x] = sens
                square_sum = square_sum + sens * sens
        return cost_sum, square_sum, packs

    loads[0].wait()
    packs = (zero, zero)
    for x in range(ex):
        packs = pack_layer(1, x, lambda i: adj[i, x], packs)
    pl.semaphore_wait(barrier, count)
    send_all(1, packs)
    for load in loads[1:]:
        load.wait()
    cost_one, _, packs = step(1, adj, mid, (zero, zero))
    send_all(0, packs)
    cost_two, square, _ = step(0, mid, out_ref, None)

    half = ez // 2
    cost = jnp.sum(cost_one + cost_two, axis=0, keepdims=True)
    square = jnp.sum(square, axis=0, keepdims=True)
    cost = cost + pltpu.roll(cost, half, 1)
    square = square + pltpu.roll(square, half, 1)
    first = lax.broadcasted_iota(jnp.int32, (1, ez), 1) < half
    total = jnp.where(first, square, cost)

    sent = []
    for r, (n, peer) in enumerate(zip(sum_groups(sizes), peers)):
        part, got, send, recv = sum_refs[4 * r : 4 * r + 4]
        if n == 1:
            continue
        part[...] = total
        copies = []
        for k in range(1, n):
            copy = pltpu.make_async_remote_copy(
                src_ref=part,
                dst_ref=got.at[pl.ds(k - 1, 1)],
                send_sem=send.at[k - 1],
                recv_sem=recv.at[k - 1],
                device_id=peer(k),
                device_id_type=MESH,
            )
            copy.start()
            copies.append(copy)
        got[pl.ds(n - 1, 1)] = total
        for copy in copies:
            copy.wait_recv()
        total = jnp.sum(got[...], axis=0, keepdims=True)
        sent += copies
    tot_ref[0, 0:1, :] = jnp.where(first, total, 0.0)
    tot_ref[0, 1:2, :] = jnp.where(first, 0.0, total)
    for t in (1, 0):
        for i in live:
            ok, copy = hop(i, t)
            pl.when(ok)(copy.wait_send)
    for copy in sent:
        copy.wait_send()


def sum_rows():
    trace = (WROWS[4] + WROWS[5] + WROWS[6]) / 3
    along = WROWS[4] - trace
    across = (WROWS[5] - WROWS[6]) / 2
    assert np.allclose(WROWS[5], trace - along / 2 + across)
    rows = [WROWS[0], WROWS[1], WROWS[2], WROWS[3]]
    rows += [3 * trace, 3 * along, 3 * across, 3 * WROWS[7], 3 * WROWS[8], 3 * WROWS[9]]
    out = np.stack(rows)[:, :16]
    out[np.abs(out) < 1e-12] = 0.0
    return out


SUM_ROWS = sum_rows()


def plus(a, b):
    if a is None or b is None:
        return b if a is None else a
    return a + b


def minus(a, b):
    if b is None:
        return a
    return -b if a is None else a - b


def times(c, a):
    return None if a is None else c * a


def some_moments(p):
    s = {i: plus(p[i], p[i + 1]) for i in range(1, 19, 2)}
    d = {i: minus(p[i], p[i + 1]) for i in range(1, 19, 2)}
    sxy, sxz, syz = plus(s[7], s[9]), plus(s[11], s[13]), plus(s[15], s[17])
    axis_yz = plus(s[3], s[5])
    axis = plus(s[1], axis_yz)
    exy = plus(sxy, sxz)
    edge = plus(exy, syz)
    m = [None] * 19
    m[0] = plus(plus(p[0], axis), edge)
    m[1] = minus(minus(times(8.0, edge), times(11.0, axis)), times(30.0, p[0]))
    m[2] = plus(minus(edge, times(4.0, axis)), times(12.0, p[0]))
    a = minus(times(2.0, s[1]), axis_yz)
    b = minus(exy, times(2.0, syz))
    m[9] = plus(a, b)
    m[10] = minus(b, times(2.0, a))
    a = minus(s[3], s[5])
    b = minus(sxy, sxz)
    m[11] = plus(a, b)
    m[12] = minus(b, times(2.0, a))
    m[13] = minus(s[7], s[9])
    m[14] = minus(s[15], s[17])
    m[15] = minus(s[11], s[13])
    xa, xb = plus(d[7], d[9]), plus(d[11], d[13])
    ya, yb = minus(d[7], d[9]), plus(d[15], d[17])
    za, zb = minus(d[11], d[13]), minus(d[15], d[17])
    for k, axis_d, u, v in ((3, d[1], xa, xb), (5, d[3], ya, yb), (7, d[5], za, zb)):
        e = plus(u, v)
        m[k] = plus(axis_d, e)
        m[k + 1] = minus(e, times(4.0, axis_d))
    m[16] = minus(xa, xb)
    m[17] = minus(yb, ya)
    m[18] = minus(za, zb)
    return m


def cell_state(f, g, fluid, inlet, outlet, weight):
    s, d = flux_sums(f)
    rho = f[0]
    for i in s:
        rho = rho + s[i]
    fx = d[1] + (d[7] + d[9]) + (d[11] + d[13])
    fy = d[3] + (d[7] - d[9]) + (d[15] + d[17])
    fz = d[5] + (d[11] - d[13]) + (d[15] - d[17])
    below = 1.0 / (0.5 + 0.6 * g)
    damping = (0.1 + g) * below
    slope = 0.44 * (below * below)
    inv = 1.0 / rho
    b = [fx * inv, fy * inv, fz * inv]
    u = [c * damping for c in b]
    uu = u[0] * u[0] + u[1] * u[1] + u[2] * u[2]
    wr = weight * rho
    v = [jnp.where(inlet, c, a) for a, c in zip(u, (inflow_speed, 0.0, 0.0))]
    scale = jnp.where(inlet, 0.0, jnp.where(outlet, 3.0, 3.0 * rho))
    half = (0.5 * weight) * uu
    state = v + [wr * c for c in u] + b + [scale, damping * inv, half, fluid * slope]
    return state, fluid * (rho * half)


def cell_sums(m, state, inner, outlet):
    vx, vy, vz, wx, wy, wz, bx, by, bz, scale, di, half, slope = state
    n = [None] * 19
    for k in range(16):
        rate = float(np.float32(RATES[k]))
        n[k] = m[k] * jnp.where(inner, rate, 1.0) if np.any(SUM_ROWS[:, k]) else None
    s0, sx, sy, sz, trace, along, across, xy, yz, xz = [combine(r, n) for r in SUM_ROWS]
    xx = trace + along
    side_on = trace - 0.5 * along
    yy, zz = side_on + across, side_on - across
    ax = sx + (xx * vx + xy * vy + xz * vz) - s0 * vx
    ay = sy + (xy * vx + yy * vy + yz * vz) - s0 * vy
    az = sz + (xz * vx + yz * vy + zz * vz) - s0 * vz
    along_v = (ax + sx) * vx + (ay + sy) * vy + (az + sz) * vz
    rho_bar = jnp.where(outlet, 0.0, s0 + 1.5 * along_v) + half
    ux_bar, uy_bar, uz_bar = scale * ax + wx, scale * ay + wy, scale * az + wz
    d_bar = ux_bar * bx + uy_bar * by + uz_bar * bz
    extra = [rho_bar - d_bar * di, ux_bar * di, uy_bar * di, uz_bar * di]
    return extra, d_bar * slope


def cell_out(p, m, extra, inner, solid):
    z = [None] * 19
    for k in range(19):
        coef = float(np.float32((1.0 - RATES[k]) / NORMS[k]))
        z[k] = jnp.where(inner, coef * m[k], 0.0)
    for k, e in zip((0, 3, 5, 7), extra):
        z[k] = z[k] + e
    out = rebuild(z)
    return [jnp.where(solid, p[opposite_index[i]], out[i]) for i in range(19)]


def near(sizes, cells):
    nx, ny, nz = sizes
    ex, ey, _ = cells
    return ny == 2 and nz == 2 and nx * ny * nz <= 64 and ex == ey and ey % 8 == 0


def rounds(nx):
    return max((nx - 1) // 2, 0)


def end_rows(n, ey, faces):
    return 2 * (7 * ey + faces * (6 * ey + 1)) + 2 * (n - 1)


def fast_kernel(
    sizes,
    adj_hbm,
    fwd_hbm,
    des_hbm,
    sol_hbm,
    kind_hbm,
    out_ref,
    sens_ref,
    tot_ref,
    adj,
    fwd,
    des,
    marks,
    mid,
    pre,
    mom,
    xs,
    xe,
    ys,
    zs,
    xr,
    yr,
    zr,
    er,
    part,
    size_loads,
    size_sends,
    load_sem,
    send_sem,
    side_sem,
    face_sem,
    sum_sem,
    round_sem,
):
    ex, ey, ez = des.shape
    nx, ny, nz = sizes
    mx, my, mz = (lax.axis_index(name) for name in AXES)
    oy, oz = 1 - my, 1 - mz
    has = {1: mx < nx - 1, -1: mx > 0}
    far = {2: mx < nx - 2, -2: mx > 1}

    loads = [
        pltpu.make_async_copy(adj_hbm, adj, load_sem.at[0]),
        pltpu.make_async_copy(fwd_hbm, fwd, load_sem.at[1]),
        pltpu.make_async_copy(des_hbm, des, load_sem.at[1]),
        pltpu.make_async_copy(sol_hbm, marks.at[0], load_sem.at[1]),
        pltpu.make_async_copy(kind_hbm, marks.at[1], load_sem.at[1]),
    ]
    loads[0].start()

    barrier = pltpu.get_barrier_semaphore()

    def greet(x, y, z):
        pl.semaphore_signal(
            barrier, inc=1, device_id={"gx": x, "gy": y, "gz": z}, device_id_type=MESH
        )

    for y, z in ((my, oz), (oy, oz), (my, mz), (oy, mz)):
        for s in (1, -1):
            pl.when(has[s])(functools.partial(greet, mx + s, y, z))
    for y, z in ((my, oz), (oy, oz), (oy, mz)):
        greet(mx, y, z)
    for s in (2, -2):

        @pl.when(far[s])
        def _():
            greet(mx + s, my, mz)

    far_count = far[2].astype(jnp.int32) + far[-2].astype(jnp.int32)
    count = 3 + 4 * (has[1].astype(jnp.int32) + has[-1].astype(jnp.int32)) + far_count
    for load in loads[1:]:
        load.start()

    def tell(j):
        for s in (2, -2):

            @pl.when(far[s])
            def _():
                pl.semaphore_signal(
                    round_sem.at[j],
                    inc=1,
                    device_id={"gx": mx + s, "gy": my, "gz": mz},
                    device_id_type=MESH,
                )

    def hear(j):
        pl.semaphore_wait(round_sem.at[j], far_count)

    def relay(j):
        if j < rounds(nx):
            if j > 0:
                hear(j - 1)
            tell(j)

    def clear(ref):
        ref[...] = jnp.zeros(ref.shape, jnp.float32)

    for t in (0, 1):
        clear(yr.at[t, oy])
        clear(zr.at[t, oz])
        clear(er.at[t, oy, mz])
        clear(er.at[t, my, oz])
        clear(er.at[t, oy, oz])
    for s in (1, -1):

        @pl.when(jnp.logical_not(has[s]))
        def _():
            clear(xr.at[side(s)])

    lane = lax.broadcasted_iota(jnp.int32, (ey, ez), 1)
    row = lax.broadcasted_iota(jnp.int32, (ey, ez), 0)
    low_z = jnp.broadcast_to(mz == 1, (ey, ez))
    slot_lane = jnp.where(low_z, lane, jnp.where(lane == ez - 1, 0, lane + 1))
    match_y = [jnp.broadcast_to(my == h, (1, ez)) for h in (0, 1)]
    match_z = [jnp.broadcast_to(mz == h, (ey, ez)) for h in (0, 1)]

    def push(src, dst, sent, came, x, y, z):
        return pltpu.make_async_remote_copy(
            src_ref=src,
            dst_ref=dst,
            send_sem=sent,
            recv_sem=came,
            device_id={"gx": x, "gy": y, "gz": z},
            device_id_type=MESH,
        )

    def x_sends(t, turn):
        h = lax.rem(mx + turn, 2)
        sent, came, at = send_sem, face_sem.at[t], mx - 1 + 2 * h
        face, last = 5 * ey, 6 * ey
        tilted = pl.multiple_of((3 + jnp.where(h == 0, oz, mz)) * ey, 8)
        edge = xs.at[t, h, pl.ds(tilted, ey)]
        copies = [
            push(edge, xr.at[h, t, pl.ds(face, ey)], sent, came, at, my, oz),
            push(xs.at[t, h], xr.at[h, t, pl.ds(0, face)], sent, came, at, my, mz),
            push(xe.at[t, h, oy], xr.at[h, t, pl.ds(last, 1)], sent, came, at, oy, mz),
        ]
        return jnp.where(h == 0, mx > 0, mx < nx - 1), copies

    def side_sends(t):
        sent, came = send_sem, side_sem.at[t]
        return [
            push(zs.at[t], zr.at[t, oz], sent, came, mx, my, oz),
            push(zs.at[t], er.at[t, oy, oz], sent, came, mx, oy, oz),
            push(ys.at[t, oy], yr.at[t, oy], sent, came, mx, oy, mz),
        ]

    shifted = (1,)

    def store_face(t, x, tiles):
        for sign in (1, -1):
            h = side(sign)
            if x != (0 if sign == 1 else ex - 1):
                continue
            for k, i in enumerate(group(0, sign)):
                cy, cz = LAT[i][1:]
                sent = pltpu.roll(tiles(i), (-cz) % ez, 1) if cz and t in shifted else tiles(i)
                xs[t, h, k * ey : (k + 1) * ey, :] = sent
                if cy:
                    cut = 0 if cy == 1 else ey - 1
                    xe[t, h, side(cy)] = tiles(i)[cut : cut + 1, :]

    def pack_sides(t, x, tiles, pack):
        for sign in (1, -1):
            h = side(sign)
            edge = 0 if sign == 1 else ey - 1
            for k, i in enumerate(group(1, sign)):
                ys[t, h, k, x : x + 1, :] = tiles(i)[edge : edge + 1, :]
        for k, (i, j) in enumerate(zip(group(2, 1), group(2, -1))):
            at = k * ex + x
            moved = jnp.where(low_z, tiles(i), tiles(j))
            if at % ez:
                moved = pltpu.roll(moved, at % ez, 1)
            pack = jnp.where(slot_lane == at, moved, pack)
        return pack

    def send_faces(t):
        for k, turn in ((0, 0), (0, 1), (2, 0), (2, 1), (1, 0), (1, 1)):
            ok, copies = x_sends(t, turn)
            pl.when(ok)(copies[k].start)

    def send_sides(t, pack):
        zs[t] = pack
        for copy in side_sends(t):
            copy.start()

    def await_bytes(ref, sem):
        pltpu.make_async_copy(ref, ref, sem).wait()

    def receive_sides(t):
        await_bytes(xr.at[0, t], side_sem.at[t])

    both = jnp.logical_and(has[1], has[-1])

    def receive_faces(t):
        rows = pl.ds(0, 6 * ey + 1)

        @pl.when(both)
        def _():
            await_bytes(xr.at[:, t, rows], face_sem.at[t])

        if nx > 1:

            @pl.when(jnp.logical_not(both))
            def _():
                await_bytes(xr.at[0, t, rows], face_sem.at[t])

    def shifted_columns(t):
        moved = {}
        for i in range(15, 19):
            cy, cz = LAT[i][1], LAT[i][2]
            pack = zr[t, side(cz)]
            src, last = (0, ey - 1) if cy == 1 else (ey - 1, 0)
            corner = er[t, side(cy), side(cz), src : src + 1, :]
            pack = pltpu.roll(pack, (-cy) % ey, 0)
            moved[i] = jnp.where(row == last, corner, pack)
        return moved

    def pulled_tile(source, t, i, x, moved):
        cx, cy, cz = LAT[i]
        at = x + cx
        inside = 0 <= at < ex
        if inside:
            tile = source[i, at]
        else:
            k = SLOT[0][i] * ey
            tile = xr[side(cx), t, k : k + ey, :]
        src = 0 if cx == 1 else ex - 1
        if cy:
            h = side(cy)
            if inside:
                fill = yr[t, h, SLOT[1][i], at : at + 1, :]
            else:
                fill = xr[side(cx), t, 6 * ey : 6 * ey + 1, :]
                fill = jnp.where(match_y[h], fill, 0.0)
            last = ey - 1 if cy == 1 else 0
            tile = jnp.where(row == last, fill, pltpu.roll(tile, (-cy) % ey, 0))
        if cz:
            h = side(cz)
            last = ez - 1 if cz == 1 else 0
            if not inside:
                pack = xr[side(cx), t, 5 * ey : 6 * ey, :]
                pack = jnp.where(match_z[h], pack, 0.0)
                if t in shifted:
                    return jnp.where(lane == last, pack, tile)
                tile = jnp.where(lane == ez - 1 - last, pack, tile)
                return pltpu.roll(tile, (-cz) % ez, 1)
            col = SLOT[2][i] * ex - h
            if cy:
                pack, col = moved[i], col + x
            else:
                pack, col = zr[t, h], col + at
            if (last - col) % ez:
                pack = pltpu.roll(pack, (last - col) % ez, 1)
            tile = jnp.where(lane == last, pack, pltpu.roll(tile, (-cz) % ez, 1))
        return tile

    whole_x = nx * ex
    zero = jnp.zeros((ey, ez), jnp.float32)

    def marked(x):
        kind = marks[1, x]
        return kind == 0, kind == 1, kind == 2, marks[0, x] == 1

    def prepare(t):
        total = zero
        for x in range(ex):
            _, inlet, outlet, solid = marked(x)
            fluid = jnp.where(solid, 0.0, 1.0)
            place = (mx * ex + x).astype(jnp.float32)
            weight = 1.0 + 2.0 * place / (whole_x - 1)
            f = [fwd[t, i, x] for i in range(19)]
            state, cost = cell_state(f, des[x], fluid, inlet, outlet, weight)
            for q, value in enumerate(state):
                pre[q, x] = value
            total = total + cost
        return total

    def is_late(i, x):
        return not 0 <= x + LAT[i][0] < ex

    def sums_of(m, x):
        inner, _, outlet, _ = marked(x)
        return cell_sums(m, [pre[q, x] for q in range(13)], inner, outlet)

    edges = sorted({0, ex - 1})
    inner_planes = range(1, ex - 1)

    def pull(t, source, done):
        receive_sides(t)
        if t == 1:
            relay(1)
        moved = shifted_columns(t)
        for x in inner_planes:
            p = [pulled_tile(source, t, i, x, moved) for i in range(19)]
            done(x, p, some_moments(p))
        early = {}
        for x in edges:
            p = [
                None if is_late(i, x) else pulled_tile(source, t, i, x, moved)
                for i in range(19)
            ]
            early[x] = p, some_moments(p)
        with jax.named_scope(f"faces {t}"):
            receive_faces(t)
        for x in edges:
            p, m = early[x]
            late = [
                pulled_tile(source, t, i, x, moved) if is_late(i, x) else None
                for i in range(19)
            ]
            p = [b if a is None else a for a, b in zip(p, late)]
            done(x, p, [plus(a, b) for a, b in zip(m, some_moments(late))])

    with jax.named_scope("load"):
        loads[0].wait()
    for x in edges:
        store_face(1, x, lambda i: adj[i, x])
    with jax.named_scope("greeted"):
        pl.semaphore_wait(barrier, count)
    with jax.named_scope("send 1"):
        send_faces(1)
    pack = zero
    for x in range(ex):
        pack = pack_sides(1, x, lambda i: adj[i, x], pack)
    with jax.named_scope("sides 1"):
        send_sides(1, pack)
        relay(0)
    await_bytes(size_loads, load_sem.at[1])
    cost = prepare(1)
    packs = [zero]
    kept = {}

    def keep(x, out, sens):
        for i in range(19):
            mid[i, x] = out[i]
        sens_ref[x] = sens
        packs[0] = pack_sides(0, x, lambda i: out[i], packs[0])

    def first_done(x, p, m):
        inner, _, _, solid = marked(x)
        extra, sens = sums_of(m, x)
        out = cell_out(p, m, extra, inner, solid)
        if x in edges:
            store_face(0, x, lambda i: out[i])
            kept[x] = out, sens
        else:
            keep(x, out, sens)

    with jax.named_scope("step 1"):
        pull(1, adj, first_done)
    with jax.named_scope("send 0"):
        send_faces(0)
    for x, (out, sens) in kept.items():
        keep(x, out, sens)
    with jax.named_scope("sides 0"):
        send_sides(0, packs[0])
    for j in range(2, rounds(nx)):
        relay(j)
    cost = cost + prepare(0)
    squares = [zero]

    def second_done(x, p, m):
        extra, sens = sums_of(m, x)
        sens = sens + sens_ref[x]
        sens_ref[x] = sens
        squares[0] = squares[0] + sens * sens
        for i in range(19):
            adj[i, x] = p[i]
        for k, value in enumerate(m + extra):
            mom[k, x] = value

    with jax.named_scope("step 0"):
        pull(0, mid, second_done)
    part[0:1, :] = jnp.sum(squares[0], axis=0, keepdims=True)
    part[1:2, :] = jnp.sum(cost, axis=0, keepdims=True)

    with jax.named_scope("heard"):
        if rounds(nx):
            hear(rounds(nx) - 1)
    n = nx * ny * nz

    def sum_send(k, x, y, z):
        return push(part, tot_ref.at[k - 1], send_sem, sum_sem, x, y, z)

    with jax.named_scope("send sums"):
        for px in range(nx):
            dx = jnp.where(px < mx, px - mx + nx, px - mx)
            for dy, dz in ((0, 1), (1, 1), (0, 0), (1, 0)):
                k = (dx * ny + dy) * nz + dz
                y, z = (oy if dy else my), (oz if dz else mz)
                if dy or dz:
                    sum_send(k, px, y, z).start()
                else:
                    pl.when(px != mx)(sum_send(k, px, y, z).start)
    tot_ref[n - 1] = part[...]
    with jax.named_scope("out"):
        for x in range(ex):
            inner, _, _, solid = marked(x)
            m = [mom[k, x] for k in range(23)]
            out = cell_out([adj[i, x] for i in range(19)], m[:19], m[19:], inner, solid)
            for i in range(19):
                out_ref[i, x] = out[i]
    with jax.named_scope("sums"):
        await_bytes(tot_ref.at[pl.ds(0, n - 1)], sum_sem)
    with jax.named_scope("drain"):

        @pl.when(both)
        def _():
            await_bytes(size_sends, send_sem)

        @pl.when(jnp.logical_not(both))
        def _():
            await_bytes(size_sends.at[pl.ds(0, end_rows(n, ey, nx > 1))], send_sem)


def hand_on(
    cells,
    adj_in,
    sens_in,
    sums_in,
    adj_out,
    sens_out,
    obj_out,
    rms_out,
    sens,
    obj,
    rms,
    sem,
):
    moves = [(adj_in, adj_out), (sens, sens_out), (obj, obj_out), (rms, rms_out)]
    copies = [pltpu.make_async_copy(a, b, sem.at[k]) for k, (a, b) in enumerate(moves)]
    copies[0].start()
    total = jnp.sum(jnp.sum(sums_in[...], axis=0), axis=1, keepdims=True) / cells
    root = jnp.sqrt(total[0:1] + 1e-06)
    scale = jnp.broadcast_to(1.0 / root, sens.shape[1:])
    for x in range(sens.shape[0]):
        sens[x] = sens_in[x] * scale
    copies[1].start()
    obj[0] = total[1, 0]
    rms[0] = root[0, 0]
    copies[2].start()
    copies[3].start()
    for copy in copies:
        copy.wait()


def body(sizes, adjoint_in, forward_states, design, solid_mask, boundary_kind):
    ex, ey, ez = design.shape
    nx, ny, nz = sizes
    any_spec = pl.BlockSpec(memory_space=pltpu.HBM)
    vmem_spec = pl.BlockSpec(memory_space=pltpu.VMEM)
    f32 = jnp.float32
    operands = (adjoint_in, forward_states, design, solid_mask, boundary_kind)
    operands = [pltpu.with_memory_space_constraint(a, pltpu.HBM) for a in operands]
    if near(sizes, design.shape):
        n = nx * ny * nz
        entries = n
        count = adjoint_in.shape[0]
        run = fast_kernel
        scratch = [
            pltpu.VMEM(adjoint_in.shape, f32),
            pltpu.VMEM(forward_states.shape, f32),
            pltpu.VMEM(design.shape, f32),
            pltpu.VMEM((2, *design.shape), jnp.int32),
            pltpu.VMEM(adjoint_in.shape, f32),
            pltpu.VMEM((13, *design.shape), f32),
            pltpu.VMEM((23, *design.shape), f32),
            pltpu.VMEM((2, 2, 5 * ey, ez), f32),
            pltpu.VMEM((2, 2, 2, 1, ez), f32),
            pltpu.VMEM((2, 2, 5, ex, ez), f32),
            pltpu.VMEM((2, ey, ez), f32),
            pltpu.VMEM((2, 2, 7 * ey, ez), f32),
            pltpu.VMEM((2, 2, 5, ex, ez), f32),
            pltpu.VMEM((2, 2, ey, ez), f32),
            pltpu.VMEM((2, 2, 2, ey, ez), f32),
            pltpu.VMEM((2, ez), f32),
            pltpu.VMEM((2 * count + 3, *design.shape), f32),
            pltpu.VMEM((end_rows(n, ey, 2), ez), f32),
            pltpu.SemaphoreType.DMA((2,)),
            pltpu.SemaphoreType.DMA,
            pltpu.SemaphoreType.DMA((2,)),
            pltpu.SemaphoreType.DMA((2,)),
            pltpu.SemaphoreType.DMA,
            pltpu.SemaphoreType.REGULAR((max(rounds(nx), 1),)),
        ]
    else:
        entries = 1
        run = general_kernel
        sum_scratch = []
        for n in sum_groups(sizes):
            sum_scratch += [
                pltpu.VMEM((1, ez), f32),
                pltpu.VMEM((n, ez), f32),
                pltpu.SemaphoreType.DMA((max(n - 1, 1),)),
                pltpu.SemaphoreType.DMA((max(n - 1, 1),)),
            ]
        scratch = [
            pltpu.VMEM(adjoint_in.shape, f32),
            pltpu.VMEM(forward_states.shape, f32),
            pltpu.VMEM(design.shape, f32),
            pltpu.VMEM(design.shape, jnp.int32),
            pltpu.VMEM(design.shape, jnp.int32),
            pltpu.VMEM(adjoint_in.shape, f32),
            pltpu.VMEM((2, 2, 5, ey, ez), f32),
            pltpu.VMEM((2, 2, 5, ex, ez), f32),
            pltpu.VMEM((2, 2, ey, ez), f32),
            pltpu.VMEM((2, 2, 5, ey, ez), f32),
            pltpu.VMEM((2, 2, 5, ex, ez), f32),
            pltpu.VMEM((2, 2, ey, ez), f32),
            pltpu.VMEM((2, 12, ey, ez), f32),
            pltpu.SemaphoreType.DMA((6,)),
            pltpu.SemaphoreType.DMA,
            pltpu.SemaphoreType.DMA((2, 18)),
            pltpu.SemaphoreType.DMA((2, 18)),
            *sum_scratch,
        ]
    adjoint, sens, tot = pl.pallas_call(
        functools.partial(run, sizes),
        out_shape=(
            jax.ShapeDtypeStruct(adjoint_in.shape, f32),
            jax.ShapeDtypeStruct(design.shape, f32),
            jax.ShapeDtypeStruct((entries, 2, ez), f32),
        ),
        in_specs=[any_spec] * 5,
        out_specs=(vmem_spec, vmem_spec, vmem_spec),
        scratch_shapes=scratch,
        compiler_params=pltpu.CompilerParams(
            collective_id=0, has_side_effects=True, vmem_limit_bytes=VMEM_LIMIT
        ),
    )(*operands)
    adjoint, sens, objective, rms = pl.pallas_call(
        functools.partial(hand_on, nx * ex * ny * ey * nz * ez),
        out_shape=(
            jax.ShapeDtypeStruct(adjoint_in.shape, f32),
            jax.ShapeDtypeStruct(design.shape, f32),
            jax.ShapeDtypeStruct((1,), f32),
            jax.ShapeDtypeStruct((1,), f32),
        ),
        in_specs=[vmem_spec] * 3,
        out_specs=(any_spec, any_spec, any_spec, any_spec),
        scratch_shapes=[
            pltpu.VMEM(design.shape, f32),
            pltpu.SMEM((1,), f32),
            pltpu.SMEM((1,), f32),
            pltpu.SemaphoreType.DMA((4,)),
        ],
        compiler_params=pltpu.CompilerParams(vmem_limit_bytes=VMEM_LIMIT),
    )(adjoint, sens, tot)
    return adjoint, sens, objective.reshape(()), rms.reshape(())


def solution(mesh):
    placed = (
        P(None, "gx", "gy", "gz"),
        P(None, None, "gx", "gy", "gz"),
        P("gx", "gy", "gz"),
        P("gx", "gy", "gz"),
        P("gx", "gy", "gz"),
    )
    return jax.shard_map(
        functools.partial(body, tuple(int(mesh.shape[name]) for name in AXES)),
        mesh=mesh,
        in_specs=placed,
        out_specs=(P(None, "gx", "gy", "gz"), P("gx", "gy", "gz"), P(), P()),
        check_vma=False,
    )
```
